32 devices in a mesh: groups: 2 (over y), batch: 8 (over z, x), mp: 2 (over core).
Axes of the slice: x: 2, y: 2, z: 4, core: 2. Of those that a mesh axis runs over, the one named last changes fastest.
Arguments:
- hidden: bfloat16 [32, 1280], P(('groups', 'batch')), parts along dimension 0, may hold values from -6 to 6
- token_qkv: bfloat16 [3, 32, 1280], P(None, ('groups', 'batch'), 'mp'), parts along dimension 1, may hold values from -6 to 6
- self_cache: bfloat16 [2, 32, 128, 1280], P(None, ('groups', 'batch'), None, 'mp'), parts along dimension 1, may hold values from -6 to 6
- cross_kv: bfloat16 [2, 32, 64, 1280], P(None, ('groups', 'batch'), None, 'mp'), parts along dimension 1, may hold values from -6 to 6
- cache_len: int32 [32], P(('groups', 'batch')), parts along dimension 0, may hold values from 1 to 127
- finished: int32 [32], P(('groups', 'batch')), parts along dimension 0, may hold values 0 or 1
- new_slot: int32 [32], P(('groups', 'batch')), parts along dimension 0, may hold values from 0 to 15, as said below
- out_proj: bfloat16 [1280, 1280], P('mp'), may hold values from -0.15625 to 0.15625
- ln_gain: float32 [1280], replicated, may hold values from 0.5 to 1.5
- ln_bias: float32 [1280], replicated, may hold values from -3 to 3
- query_proj: bfloat16 [1280, 1280], P(None, 'mp'), may hold values from -3 to 3
Outputs:
- moved_cache: bfloat16 [2, 32, 128, 1280], P(None, ('groups', 'batch'), None, 'mp'), parts along dimension 1
- moved_out: bfloat16 [32, 1280], P(('groups', 'batch'), 'mp'), parts along dimension 0
The draws below stay inside these ranges and needn't reach their ends.
There are 2 independent parts, one for each index of `groups`. The reference program is written for one: setup_inputs(seed, part) draws one part's arguments, and reference() takes and returns one part's arrays. A program takes and returns all parts, laid end to end along the dimension named above; an argument that names none is the same for every part. Nothing has to cross between parts.
Inputs may be any that keep to these rules, and one draw needn't show every extreme that they name: A permutation of the spans' slots. Span c's new owner new_slot[c] // 2 lies within 3 devices of its present one c // 2, counting the device order as a loop; of one device's spans at most one moves by any given signed distance.
All inputs are finite; a program needn't handle non-finite values. No bound on the sum of `finished` on one device may be relied on, other than what follows from the above.
Results may differ from the reference program's by a relative error of at most 0.015.
Values may be sent and summed in bfloat16 or wider, within the bound.
A program may use at most 64 MiB of HBM per device.

```python
import jax
import jax.numpy as jnp
from jax import lax

D = 1280
HEADS = 20
HEAD_DIM = 64
CH_DEV = 2
ENC = 64
SLOTS = 128
SPANS = 16


def swap_round(key, table, stride, period):
    devices, width = table.shape
    keys = jax.random.split(key, 4)
    phase = jax.random.randint(keys[0], (), 0, period)
    left_slot = jax.random.randint(keys[1], (devices,), 0, width)
    right_slot = jax.random.randint(keys[2], (devices,), 0, width)
    coin = jax.random.randint(keys[3], (devices,), 0, 2)
    index = jnp.arange(devices, dtype=jnp.int32)
    is_left = (index - phase) % period < stride
    partner = jnp.where(is_left, (index + stride) % devices, (index - stride) % devices)
    leader = jnp.where(is_left, index, partner)
    mine = jnp.where(is_left, left_slot[leader], right_slot[leader])
    theirs = jnp.where(is_left, right_slot[leader], left_slot[leader])
    swapping = coin[leader] == 1
    incoming = table[partner, theirs]
    column = jnp.arange(width, dtype=jnp.int32)[None, :] == mine[:, None]
    return jnp.where(column & swapping[:, None], incoming[:, None], table)


def draw_new_slot(key, part):
    devices = SPANS // CH_DEV
    table = jnp.arange(SPANS, dtype=jnp.int32).reshape(devices, CH_DEV)
    table = swap_round(jax.random.fold_in(key, 11), table, 1, 2)
    table = swap_round(jax.random.fold_in(key, 12), table, 2, 4)
    return jnp.zeros((SPANS,), jnp.int32).at[table.reshape(-1)].set(jnp.arange(SPANS, dtype=jnp.int32))


def rough_noise(key, shape):
    return jax.random.truncated_normal(key, -6.0, 6.0, shape, jnp.float32)


def fixed_pattern():
    dims = jnp.arange(HEAD_DIM, dtype=jnp.int32)
    return jnp.where((dims * 37 + 11) % 8 < 4, 1.0, -1.0).astype(jnp.float32)


def self_plan(key):
    keys = jax.random.split(jax.random.fold_in(key, 71), 7)
    span_index = jnp.arange(SPANS, dtype=jnp.int32)[:, None]
    head_index = jnp.arange(HEADS, dtype=jnp.int32)[None, :]
    first_span = jax.random.randint(keys[0], (), 0, SPANS)
    first_head = jax.random.randint(keys[1], (), 0, HEADS)
    forced = (span_index == first_span) & (head_index == first_head)
    planted = (jax.random.randint(keys[2], (SPANS, HEADS), 0, 16) == 0) | forced
    signs = (2 * jax.random.randint(keys[3], (SPANS, HEADS, HEAD_DIM), 0, 2) - 1).astype(jnp.float32)
    query_steps = jnp.where(forced, 185, jax.random.randint(keys[4], (SPANS, HEADS), 112, 186))
    key_steps = jnp.where(forced, 185, jax.random.randint(keys[5], (SPANS, HEADS), 144, 186))
    own_first = jax.random.randint(keys[6], (SPANS, HEADS), 0, 2) == 1
    higher = key_steps.astype(jnp.float32) / 32.0
    lower = (key_steps - 2).astype(jnp.float32) / 32.0
    query_scale = query_steps.astype(jnp.float32) / 32.0
    own_scale = jnp.where(own_first, higher, lower)
    cached_scale = jnp.where(own_first, lower, higher)
    return (planted, signs, query_scale, own_scale, cached_scale)


def draw_token_qkv(key, part):
    base = rough_noise(jax.random.fold_in(key, 1), (3, SPANS, HEADS, HEAD_DIM))
    planted, signs, query_scale, own_scale, cached_scale = self_plan(key)
    mask = planted[:, :, None]
    query_part = jnp.where(mask, query_scale[:, :, None] * signs, base[0])
    key_part = jnp.where(mask, own_scale[:, :, None] * signs, base[1])
    stacked = jnp.stack([query_part, key_part, base[2]])
    return stacked.reshape(3, SPANS, D).astype(jnp.bfloat16)


def draw_self_cache(key, part):
    base = rough_noise(jax.random.fold_in(key, 2), (2, SPANS, SLOTS, HEADS, HEAD_DIM))
    planted, signs, query_scale, own_scale, cached_scale = self_plan(key)
    first_keys = jnp.where(planted[:, :, None], cached_scale[:, :, None] * signs, base[0, :, 0])
    base = base.at[0, :, 0].set(first_keys)
    return base.reshape(2, SPANS, SLOTS, D).astype(jnp.bfloat16)


def draw_cross_kv(key, part):
    base = rough_noise(jax.random.fold_in(key, 3), (2, SPANS, ENC, HEADS, HEAD_DIM))
    keys = jax.random.split(jax.random.fold_in(key, 73), 5)
    span_index = jnp.arange(SPANS, dtype=jnp.int32)
    forced_span = jax.random.randint(keys[0], (), 0, SPANS)
    planted = (jax.random.randint(keys[1], (SPANS,), 0, 8) == 0) | (span_index == forced_span)
    first_frame = jax.random.randint(keys[2], (SPANS,), 0, ENC)
    second_frame = (first_frame + 1 + jax.random.randint(keys[3], (SPANS,), 0, ENC - 1)) % ENC
    key_steps = jnp.where(span_index == forced_span, 184, jax.random.randint(keys[4], (SPANS,), 96, 186))
    higher = key_steps.astype(jnp.float32) / 32.0
    lower = (key_steps - 2).astype(jnp.float32) / 32.0
    frame = jnp.arange(ENC, dtype=jnp.int32)[None, :]
    at_first = frame == first_frame[:, None]
    at_second = frame == second_frame[:, None]
    scale = jnp.where(at_first, higher[:, None], jnp.where(at_second, lower[:, None], 0.0))
    use = planted[:, None] & (at_first | at_second)
    pattern = fixed_pattern()
    key_part = jnp.where(use[:, :, None, None], scale[:, :, None, None] * pattern[None, None, None, :], base[0])
    stacked = jnp.stack([key_part, base[1]])
    return stacked.reshape(2, SPANS, ENC, D).astype(jnp.bfloat16)


def bias_plan(key):
    keys = jax.random.split(jax.random.fold_in(key, 91), 3)
    bias = 0.5 * jax.random.truncated_normal(keys[0], -6.0, 6.0, (D,), jnp.float32)
    head_index = jnp.arange(HEADS, dtype=jnp.int32)
    chosen_head = jax.random.randint(keys[1], (), 0, HEADS)
    heads_on = (jax.random.randint(keys[2], (HEADS,), 0, 4) == 0) | (head_index == chosen_head)
    return (bias, heads_on)


def draw_ln_bias(key, part):
    bias, heads_on = bias_plan(key)
    return bias


def draw_query_proj(key, part):
    bias, heads_on = bias_plan(key)
    weight_key = jax.random.fold_in(key, 92)
    weight = jax.random.truncated_normal(weight_key, -6.0, 6.0, (D, D), jnp.float32) * D ** (-0.5)
    direction = 5.0 * jnp.where(heads_on[:, None], fixed_pattern()[None, :], 0.0).reshape(D)
    norm_sq = jnp.maximum(jnp.sum(bias * bias), D / 8.0)
    weight = weight + (bias / norm_sq)[:, None] * direction[None, :]
    return weight.astype(jnp.bfloat16)


def set_ends(drawn, own_key, low, high):
    extent = drawn.shape
    place = [jax.random.randint(jax.random.fold_in(own_key, axis), (), 0, extent[axis]) for axis in range(len(extent))]
    drawn = drawn.at[tuple(place)].set(low)
    longest = extent.index(max(extent))
    place[longest] = (place[longest] + 1) % extent[longest]
    return drawn.at[tuple(place)].set(high)


def shard_levels(key, shape, shards, low, top_value):
    factor_of, own = 1.0, jax.random.fold_in(key, 6)
    for dim, shards_of in shards:
        heights = jnp.exp(jax.random.uniform(jax.random.fold_in(own, dim), (shards_of,), jnp.float32, low / len(shards), top_value / len(shards)))
        factor_of = factor_of * jnp.repeat(heights, shape[dim] // shards_of).reshape([-1 if axis == dim else 1 for axis in range(len(shape))])
    return factor_of


def noise(key, extent, deviation, reach, shards=(), kind=jnp.bfloat16):
    values = deviation * jax.random.normal(key, extent, jnp.float32)
    if shards:
        values = values * shard_levels(key, extent, shards, -0.22, 0.18)
    return jnp.clip(values, -reach, reach).astype(kind)


def setup_inputs(seed: int = 0, part: int = 0) -> dict:
    seeds = jax.random.split(jax.random.key(seed), 12)
    part_splits = jax.random.split(jax.random.fold_in(seeds[11], part), 12)
    return {
        "hidden": noise(part_splits[0], (SPANS, D), 1.0, 6.0, ((0, 8),)),
        "token_qkv": draw_token_qkv(jax.random.fold_in(jax.random.fold_in(seeds[11], part), 71), part),
        "self_cache": draw_self_cache(jax.random.fold_in(jax.random.fold_in(seeds[11], part), 71), part),
        "cross_kv": draw_cross_kv(jax.random.fold_in(jax.random.fold_in(seeds[11], part), 71), part),
        "cache_len": set_ends(jax.random.randint(part_splits[4], (SPANS,), 1, SLOTS), jax.random.fold_in(part_splits[4], 1), 1, SLOTS - 1).astype(jnp.int32),
        "finished": set_ends((jax.random.randint(part_splits[5], (SPANS,), 0, 4) < 1).astype(jnp.int32), jax.random.fold_in(part_splits[5], 1), 0, 1),
        "new_slot": draw_new_slot(jax.random.fold_in(jax.random.fold_in(seeds[11], part), 71), part),
        "out_proj": noise(seeds[7], (D, D), D ** -0.5, 0.15625, ((0, 2),)),
        "ln_gain": jnp.clip(1.0 + 0.1 * jax.random.normal(seeds[8], (D,), jnp.float32), 0.5, 1.5),
        "ln_bias": draw_ln_bias(jax.random.fold_in(seeds[11], 71), part),
        "query_proj": draw_query_proj(jax.random.fold_in(seeds[11], 71), part),
    }


def reference(hidden, token_qkv, self_cache, cross_kv, cache_len, finished, new_slot, out_proj, ln_gain, ln_bias, query_proj):
    head_count = D // HEAD_DIM
    factor = HEAD_DIM ** (-0.5)
    new_query = token_qkv[0].astype(jnp.float32).reshape(SPANS, head_count, HEAD_DIM)
    new_key = token_qkv[1].astype(jnp.float32).reshape(SPANS, head_count, HEAD_DIM)
    new_value = token_qkv[2].astype(jnp.float32).reshape(SPANS, head_count, HEAD_DIM)
    cache_keys = self_cache[0].astype(jnp.float32).reshape(SPANS, SLOTS, head_count, HEAD_DIM)
    cache_values = self_cache[1].astype(jnp.float32).reshape(SPANS, SLOTS, head_count, HEAD_DIM)
    scores = jnp.einsum('chd,cthd->cht', new_query, cache_keys) * factor
    position = jnp.arange(SLOTS, dtype=jnp.int32)
    usable = position[None, None, :] < cache_len[:, None, None]
    scores = jnp.where(usable, scores, -1e+30)
    own_score = lax.optimization_barrier(jnp.sum(new_query * new_key, axis=-1)) * factor
    highest = jnp.maximum(lax.optimization_barrier(jnp.max(scores, axis=-1)), own_score)
    cache_weight = jnp.where(usable, jnp.exp(scores - highest[..., None]), 0.0)
    own_weight = jnp.exp(own_score - highest)
    total = lax.optimization_barrier(jnp.sum(cache_weight, axis=-1)) + own_weight
    cache_weight = (cache_weight / total[..., None]).astype(jnp.bfloat16)
    own_weight = (own_weight / total).astype(jnp.bfloat16)
    context = jnp.einsum('cht,cthd->chd', cache_weight.astype(jnp.float32), cache_values)
    context = context + own_weight.astype(jnp.float32)[..., None] * new_value
    context = context.astype(jnp.bfloat16).reshape(SPANS, D)
    resid = hidden.astype(jnp.float32) + jnp.dot(context, out_proj, preferred_element_type=jnp.float32)
    centre = lax.optimization_barrier(jnp.mean(resid, axis=-1, keepdims=True))
    spread = lax.optimization_barrier(jnp.mean((resid - centre) ** 2, axis=-1, keepdims=True))
    normed = ((resid - centre) * lax.rsqrt(spread + 1e-05) * ln_gain + ln_bias).astype(jnp.bfloat16)
    cross_query = jnp.dot(normed, query_proj, preferred_element_type=jnp.float32).astype(jnp.bfloat16)
    cross_query = cross_query.astype(jnp.float32).reshape(SPANS, head_count, HEAD_DIM)
    cross_keys = cross_kv[0].astype(jnp.float32).reshape(SPANS, ENC, head_count, HEAD_DIM)
    cross_values = cross_kv[1].astype(jnp.float32).reshape(SPANS, ENC, head_count, HEAD_DIM)
    cross_scores = jnp.einsum('chd,cthd->cht', cross_query, cross_keys) * factor
    cross_high = lax.optimization_barrier(jnp.max(cross_scores, axis=-1, keepdims=True))
    cross_exp = jnp.exp(cross_scores - cross_high)
    cross_weight = (cross_exp / lax.optimization_barrier(jnp.sum(cross_exp, axis=-1, keepdims=True))).astype(jnp.bfloat16)
    cross_context = jnp.einsum('cht,cthd->chd', cross_weight.astype(jnp.float32), cross_values).reshape(SPANS, D)
    alive = finished == 0
    decoded = jnp.where(alive[:, None], cross_context, 0.0).astype(jnp.bfloat16)
    slot_pos = position[None, :, None]
    length = cache_len[:, None, None]

    def extend(older, fresh):
        grown = jnp.where(slot_pos < length, older, jnp.where(slot_pos == length, fresh[:, None, :], jnp.zeros_like(older)))
        return jnp.where(alive[:, None, None], grown, jnp.zeros_like(older))
    updated = jnp.stack([extend(self_cache[0], token_qkv[1]), extend(self_cache[1], token_qkv[2])])
    moved_cache = jnp.zeros_like(self_cache).at[:, new_slot].set(updated)
    moved_out = jnp.zeros((SPANS, D), jnp.bfloat16).at[new_slot].set(decoded)
    return (moved_cache, moved_out)
```

```python
import functools

import jax
import jax.numpy as jnp
from jax import lax
from jax.experimental import pallas as pl
from jax.experimental.pallas import tpu as pltpu
from jax.sharding import PartitionSpec as P

HEAD_DIM = 64
REACH = 3
MESH = pl.DeviceIdType.MESH
DISTANCES = [3, -3, 2, -2, 1, -1]
ROWS = 16
WHOLE = 6
JOINED = 14
AHEAD = 5
LAG = 3
BEHIND = 3
LINES = 11


def attend(query, keys, values, length, own):
    slots, width = keys.shape
    heads = width // HEAD_DIM
    rows = -(-heads // 16) * 16
    row = lax.broadcasted_iota(jnp.int32, (rows, width), 0)
    column = lax.broadcasted_iota(jnp.int32, (rows, width), 1)
    low = row * HEAD_DIM
    mine = (column >= low) & (column < low + HEAD_DIM)
    spread = jnp.where(mine, query.astype(jnp.float32), 0.0)
    factor = HEAD_DIM ** (-0.5)
    scores = (
        lax.dot_general(
            spread.astype(jnp.bfloat16),
            keys,
            (((1,), (1,)), ((), ())),
            preferred_element_type=jnp.float32,
        )
        * factor
    )
    if length is not None:
        usable = lax.broadcasted_iota(jnp.int32, (rows, slots), 1) < length
        scores = jnp.where(usable, scores, -1e30)
    highest = jnp.max(scores, axis=-1, keepdims=True)
    if own is not None:
        new_key, new_value = own
        own_score = jnp.sum(spread * new_key.astype(jnp.float32), axis=-1, keepdims=True) * factor
        highest = jnp.maximum(highest, own_score)
    weight = jnp.exp(scores - highest)
    if length is not None:
        weight = jnp.where(usable, weight, 0.0)
    total = jnp.sum(weight, axis=-1, keepdims=True)
    if own is not None:
        own_weight = jnp.exp(own_score - highest)
        total = total + own_weight
    weight = (weight / total).astype(jnp.bfloat16)
    mixed = jnp.dot(weight, values, preferred_element_type=jnp.float32)
    if own is not None:
        own_weight = (own_weight / total).astype(jnp.bfloat16).astype(jnp.float32)
        mixed = mixed + own_weight * new_value.astype(jnp.float32)
    return jnp.sum(jnp.where(mine, mixed, 0.0), axis=0, keepdims=True)


def kernel(
    count,
    cores,
    cache_len,
    finished,
    new_slot,
    hidden,
    token_qkv,
    self_cache,
    ln_gain,
    ln_bias,
    cross_hbm,
    out_proj_hbm,
    query_proj_hbm,
    moved_cache,
    moved_out,
    cross,
    out_proj,
    query_proj,
    updated,
    parcel,
    arrived,
    mark,
    mark_in,
    line,
    line_in,
    part,
    part_in,
    load_sem,
    cache_sems,
    mark_sems,
    line_sems,
    part_sems,
):
    spans, width = hidden.shape
    slots, local = self_cache.shape[2:]
    me = lax.axis_index("batch")
    core = lax.axis_index("mp")
    loads = [
        pltpu.make_async_copy(source, target, load_sem.at[i])
        for i, (source, target) in enumerate(
            [(out_proj_hbm, out_proj), (query_proj_hbm, query_proj), (cross_hbm, cross)]
        )
    ]
    for load in loads:
        load.start()

    barrier = pltpu.get_barrier_semaphore()
    targets = [lax.rem(me + distance + count, count) for distance in DISTANCES]
    for target in targets:
        pl.semaphore_signal(barrier, inc=1, device_id={"batch": target}, device_id_type=MESH)
    others = [lax.rem(core + k, cores) for k in range(1, cores)]
    for other in others:
        pl.semaphore_signal(barrier, inc=1, device_id={"mp": other}, device_id_type=MESH)

    half = count // 2
    alive, offset, place = [], [], []
    for c in range(spans):
        slot = new_slot[c]
        owner = lax.div(slot, spans)
        offset.append(lax.rem(owner - me + half + count, count) - half)
        place.append(lax.rem(slot, spans))
        alive.append(jnp.where(finished[c] == 0, 1, 0))

    position = lax.broadcasted_iota(jnp.int32, (slots, local), 0)
    for c in range(spans):
        length = cache_len[c]
        older = jnp.where(position < length * alive[c], 1.0, 0.0).astype(jnp.bfloat16)
        fresh = jnp.where(position == jnp.where(alive[c] == 1, length, -1), 1.0, 0.0).astype(
            jnp.bfloat16
        )
        for a in range(2):
            updated[a, c] = self_cache[a, c] * older + token_qkv[1 + a, c : c + 1, :] * fresh

    def flag(value, shape):
        return jnp.full(shape, jnp.where(value, 1.0, 0.0), jnp.float32).astype(jnp.bfloat16)

    marker_row = lax.broadcasted_iota(jnp.int32, mark.shape[1:], 0)
    for i, distance in enumerate(DISTANCES):
        marker = jnp.zeros(mark.shape[1:], jnp.float32)
        for c in range(spans):
            at = jnp.where(offset[c] == distance, place[c], -1)
            marker = jnp.where(marker_row == at, 1.0, marker)
        mark[i] = marker.astype(jnp.bfloat16)

    def send(source, target, sems, i, distance):
        return pltpu.make_async_remote_copy(
            src_ref=source,
            dst_ref=target,
            send_sem=sems.at[0, i],
            recv_sem=sems.at[1, i],
            device_id={"batch": targets[i]},
            device_id_type=MESH,
        )

    pl.semaphore_wait(barrier, len(targets) + len(others))
    mark_copies, cache_copies = [], []
    for i, distance in enumerate(DISTANCES):
        copy = send(mark.at[i], mark_in.at[i], mark_sems, i, distance)
        copy.start()
        mark_copies.append(copy)
    for i, distance in enumerate(DISTANCES):
        for a in range(2):
            total = updated[a, 0] * flag(offset[0] == distance, (1, local))
            for c in range(1, spans):
                total = total + updated[a, c] * flag(offset[c] == distance, (1, local))
            parcel[i, a] = total
        copy = send(parcel.at[i], arrived.at[i], cache_sems, i, distance)
        copy.start()
        cache_copies.append(copy)

    for l in range(spans):
        for a in range(2):
            total = updated[a, 0] * flag((offset[0] == 0) & (place[0] == l), (1, local))
            for c in range(1, spans):
                keep = flag((offset[c] == 0) & (place[c] == l), (1, local))
                total = total + updated[a, c] * keep
            moved_cache[a, l] = total

    contexts = []
    for c in range(spans):
        query, key, value = (token_qkv[k, c : c + 1, :] for k in range(3))
        contexts.append(
            attend(query, self_cache[0, c], self_cache[1, c], cache_len[c], (key, value))
        )
    pad = part.shape[0] - spans
    context = jnp.concatenate(contexts + [jnp.zeros((pad, local), jnp.float32)], 0)
    context = context.astype(jnp.bfloat16)
    loads[0].wait()
    part[...] = jnp.dot(context, out_proj[...], preferred_element_type=jnp.float32)
    part_copies = []
    for k, other in enumerate(others):
        copy = pltpu.make_async_remote_copy(
            src_ref=part,
            dst_ref=part_in.at[k],
            send_sem=part_sems.at[0, k],
            recv_sem=part_sems.at[1, k],
            device_id={"mp": other},
            device_id_type=MESH,
        )
        copy.start()
        part_copies.append(copy)
    loads[1].wait()
    loads[2].wait()
    for copy in part_copies:
        copy.wait()
    summed = part[...]
    for k in range(len(others)):
        summed = summed + part_in[k]
    resid = hidden[...].astype(jnp.float32) + summed[:spans]
    centre = jnp.mean(resid, axis=-1, keepdims=True)
    spread = jnp.mean((resid - centre) ** 2, axis=-1, keepdims=True)
    gain = ln_gain[...].reshape(1, width)
    bias = ln_bias[...].reshape(1, width)
    normed = (resid - centre) * lax.rsqrt(spread + 1e-05) * gain + bias
    normed = jnp.concatenate([normed, jnp.zeros((pad, width), jnp.float32)], 0)
    query = jnp.dot(
        normed.astype(jnp.bfloat16), query_proj[...], preferred_element_type=jnp.float32
    ).astype(jnp.bfloat16).astype(jnp.float32)
    decoded = []
    for c in range(spans):
        mixed = attend(query[c : c + 1], cross[0, c], cross[1, c], None, None)
        decoded.append(mixed * jnp.where(alive[c] == 1, 1.0, 0.0))

    line_copies = []
    blank = jnp.zeros((line.shape[1] - 1, local), jnp.float32)
    for i, distance in enumerate(DISTANCES):
        row = jnp.zeros((1, local), jnp.float32)
        for c in range(spans):
            row = row + decoded[c] * jnp.where(offset[c] == distance, 1.0, 0.0)
        line[i] = jnp.concatenate([row, blank], 0).astype(jnp.bfloat16)
        copy = send(line.at[i], line_in.at[i], line_sems, i, distance)
        copy.start()
        line_copies.append(copy)

    rows = []
    for l in range(spans):
        row = jnp.zeros((1, local), jnp.float32)
        for c in range(spans):
            keep = (offset[c] == 0) & (place[c] == l)
            row = row + decoded[c] * jnp.where(keep, 1.0, 0.0)
        rows.append(row)
    for i in range(len(DISTANCES)):
        mark_copies[i].wait()
        cache_copies[i].wait()
        for l in range(spans):
            taken = mark_in[i, l : l + 1, :]
            for a in range(2):
                moved_cache[a, l] = moved_cache[a, l] + arrived[i, a] * taken
    for i in range(len(DISTANCES)):
        line_copies[i].wait()
        for l in range(spans):
            taken = mark_in[i, l : l + 1, :].astype(jnp.float32)
            rows[l] = rows[l] + line_in[i, 0:1, :].astype(jnp.float32) * taken
    moved_out[...] = jnp.concatenate(rows, 0).astype(jnp.bfloat16)


def relay_kernel(
    count,
    cores,
    cache_len_hbm,
    finished_hbm,
    new_slot_hbm,
    hidden_hbm,
    token_qkv_hbm,
    cache_hbm,
    ln_gain_hbm,
    ln_bias_hbm,
    cross_hbm,
    out_proj_hbm,
    query_proj_hbm,
    moved_cache,
    moved_out,
    cache_len,
    finished,
    new_slot,
    hidden,
    token_qkv,
    ln_gain,
    ln_bias,
    self_cache,
    cross,
    out_proj,
    query_proj,
    own,
    raw_in,
    cross_out,
    cross_in,
    kept,
    final_out,
    final_in,
    final_far,
    pick,
    label,
    label_in,
    line,
    line_in,
    line_kept,
    line_out,
    line_cross,
    line_last,
    line_final,
    part,
    part_in,
    load_sem,
    raw_send,
    raw_recv,
    hop_sems,
    label_send,
    label_recv,
    line_send,
    line_recv,
    line_hops,
    part_sems,
    pass_sems,
):
    spans, width = hidden.shape
    slots, local = self_cache.shape[2:]
    steps, _, rows_per, _ = own.shape
    per = steps // 2
    me = lax.axis_index("batch")
    core = lax.axis_index("mp")
    level, column = lax.div(me, 2), lax.rem(me, 2)
    inner = (level == 1) | (level == REACH - 1)
    outer = jnp.logical_not(inner)
    barrier = pltpu.get_barrier_semaphore()

    def greet(where):
        pl.semaphore_signal(barrier, inc=1, device_id=where, device_id_type=MESH)

    mate_level = jnp.where(level == 0, 1, jnp.where(level == 1, 0, jnp.where(level == 2, 3, 2)))
    mate = mate_level * 2 + column
    mate_aside = mate_level * 2 + 1 - column
    aside = level * 2 + 1 - column
    across = (REACH - level) * 2 + column
    beyond = (REACH - mate_level) * 2 + column
    others = [lax.rem(core + k, cores) for k in range(1, cores)]
    for node in (mate, beyond, aside):
        greet({"batch": node})

    @pl.when(inner)
    def _():
        greet({"batch": across})

    for other in others:
        greet({"mp": other})
    loads = [
        pltpu.make_async_copy(source, target, load_sem.at[i])
        for i, (source, target) in enumerate(
            [
                (out_proj_hbm, out_proj),
                (query_proj_hbm, query_proj),
                (cross_hbm, cross),
                (cache_hbm.at[0], self_cache.at[0]),
                (cache_hbm.at[1], self_cache.at[1]),
                (cache_len_hbm, cache_len),
                (finished_hbm, finished),
                (new_slot_hbm, new_slot),
                (hidden_hbm, hidden),
                (token_qkv_hbm, token_qkv),
                (ln_gain_hbm, ln_gain),
                (ln_bias_hbm, ln_bias),
            ]
        )
    ]
    for i in [3, *range(5, len(loads)), 4, 0, 1, 2]:
        loads[i].start()
    for load in loads[5:]:
        load.wait()

    alive = [jnp.where(finished[c] == 0, 1, 0) for c in range(spans)]

    def to(node, source, target, sent, received):
        return pltpu.make_async_remote_copy(
            src_ref=source,
            dst_ref=target,
            send_sem=sent,
            recv_sem=received,
            device_id={"batch": node},
            device_id_type=MESH,
        )

    def raw_copy(node, lane, way, k):
        return to(node, own.at[k], raw_in.at[way, k], raw_send.at[lane, k], raw_recv.at[way, k])

    def pass_copy(k):
        return to(across, raw_in.at[0, k], raw_in.at[2, k], pass_sems.at[k], raw_recv.at[2, k])

    def outer_pass_copy(k):
        return to(mate, raw_in.at[1, k], raw_in.at[1, k], pass_sems.at[k], raw_recv.at[1, k])

    def far_copy(k):
        return to(
            beyond,
            cross_out.at[k, pl.ds(spans, spans)],
            final_far.at[k],
            hop_sems.at[0, k],
            hop_sems.at[1, k],
        )

    def turn_copy(k):
        return to(
            mate,
            cross_out.at[k, pl.ds(spans, spans)],
            raw_in.at[2, k],
            hop_sems.at[0, k],
            raw_recv.at[2, k],
        )

    def turned_copy(k):
        return to(aside, raw_in.at[2, k], final_far.at[k], pass_sems.at[k], hop_sems.at[1, k])

    def cross_copy(k, node, count):
        return to(
            node,
            cross_out.at[k, pl.ds(0, count)],
            cross_in.at[k, pl.ds(0, count)],
            hop_sems.at[2, k],
            hop_sems.at[3, k],
        )

    def final_copy(k):
        return to(mate, final_out.at[k], final_in.at[k], hop_sems.at[4, k], hop_sems.at[5, k])

    def label_copy(node, lane, way):
        return to(node, label, label_in.at[way], label_send.at[lane], label_recv.at[way])

    def line_copy(node, lane, way):
        return to(node, line, line_in.at[way], line_send.at[lane], line_recv.at[way])

    def label_pass_copy(node, here, there):
        return to(node, label_in.at[here], label_in.at[there], label_send.at[2], label_recv.at[there])

    def line_pass_copy():
        return to(mate, line_in.at[1], line_in.at[1], line_send.at[2], line_recv.at[1])

    def line_cross_copy():
        return to(across, line_out, line_cross, line_hops.at[0], line_hops.at[1])

    def line_final_copy():
        return to(mate, line_last, line_final, line_hops.at[2], line_hops.at[3])

    label_row = lax.broadcasted_iota(jnp.int32, label.shape, 0)
    labels = jnp.zeros(label.shape, jnp.int32)
    for c in range(spans):
        labels = jnp.where(label_row == c, new_slot[c], labels)
    label[...] = labels.astype(jnp.float32)

    @pl.when(inner)
    def _():
        pl.semaphore_wait(barrier, 4 + len(others))

    @pl.when(outer)
    def _():
        pl.semaphore_wait(barrier, 3 + len(others))

    position = lax.broadcasted_iota(jnp.int32, (rows_per, local), 0)
    ends = [cache_len[c] * alive[c] for c in range(spans)]
    fresh_at = [jnp.where(alive[c] == 1, cache_len[c], -1) for c in range(spans)]

    def grow(k, _):
        a, r = lax.div(k, per), lax.rem(k, per)
        start = pl.multiple_of(r * rows_per, rows_per)
        at = position + start
        for c in range(spans):
            older = jnp.where(at < ends[c], 1.0, 0.0).astype(jnp.bfloat16)
            fresh = jnp.where(at == fresh_at[c], 1.0, 0.0).astype(jnp.bfloat16)
            new = jnp.where(a == 0, token_qkv[1, c : c + 1, :].astype(jnp.float32),
                            token_qkv[2, c : c + 1, :].astype(jnp.float32)).astype(jnp.bfloat16)
            own[k, c] = self_cache[a, c, pl.ds(start, rows_per), :] * older + new * fresh

        return 0

    def pass_whole(k, _):
        grow(k, 0)

        @pl.when(outer)
        def _():
            raw_copy(mate, 0, 0, k).start()

        @pl.when(inner)
        def _():
            raw_copy(across, 0, 1, k).start()

        return 0

    def pass_on(k, _):
        @pl.when(outer)
        def _():
            raw_copy(aside, 1, 1, k).start()

        @pl.when(inner)
        def _():
            raw_copy(aside, 0, 2, k).start()

        return 0

    @pl.when(outer)
    def _():
        label_copy(mate, 0, 0).start()
        label_copy(aside, 1, 1).start()

    @pl.when(inner)
    def _():
        label_copy(aside, 0, 2).start()
        label_copy(across, 1, 3).start()

    loads[3].wait()
    lax.fori_loop(0, WHOLE, pass_whole, 0)
    lax.fori_loop(WHOLE, per, grow, 0)
    loads[4].wait()
    lax.fori_loop(per, steps, grow, 0)

    @pl.when(inner)
    def _():
        lax.fori_loop(WHOLE, WHOLE + AHEAD, pass_on, 0)

    @pl.when(outer)
    def _():
        lax.fori_loop(WHOLE, steps, pass_on, 0)


    def self_part():
        contexts = []
        for c in range(spans):
            query, key, value = (token_qkv[k, c : c + 1, :] for k in range(3))
            contexts.append(
                attend(query, self_cache[0, c], self_cache[1, c], cache_len[c], (key, value))
            )
        context = jnp.concatenate(contexts + [jnp.zeros((pad, local), jnp.float32)], 0)
        context = context.astype(jnp.bfloat16)
        loads[0].wait()
        part[...] = jnp.dot(context, out_proj[...], preferred_element_type=jnp.float32)

    def part_copy(k):
        return pltpu.make_async_remote_copy(
            src_ref=part,
            dst_ref=part_in.at[k],
            send_sem=part_sems.at[0, k],
            recv_sem=part_sems.at[1, k],
            device_id={"mp": others[k]},
            device_id_type=MESH,
        )

    pad = part.shape[0] - spans
    self_part()
    for k in range(len(others)):
        part_copy(k).start()

    @pl.when(outer)
    def _():
        label_copy(mate, 0, 1).wait_recv()
        label_pass_copy(mate, 1, 1).start()

    @pl.when(inner)
    def _():
        label_copy(mate, 0, 0).wait_recv()
        label_pass_copy(across, 0, 4).start()

    def choose(p, ways, nodes):
        for s, source in enumerate([label] + [label_in.at[way] for way in ways]):
            for c in range(spans):
                held = jnp.broadcast_to(source[c : c + 1, 0:1], (rows_per, local))
                for d, node in enumerate(nodes):
                    for l in range(spans):
                        wanted = jnp.full((rows_per, local), node * spans + l, jnp.int32)
                        pick[p, s * spans + c, d * spans + l] = jnp.where(
                            held == wanted.astype(jnp.float32), 1.0, 0.0
                        ).astype(jnp.bfloat16)

    def gather(k, p, cross_done, final_done):
        blocks = [own[k, c] for c in range(spans)]
        for way in range(3):
            blocks += [raw_in[way, k, c] for c in range(spans)]

        def gathered(d):
            total = blocks[0] * pick[p, 0, d]
            for s in range(1, len(blocks)):
                total = total + blocks[s] * pick[p, s, d]
            return total

        for d in range(spans, 2 * spans):
            cross_out[k, d] = gathered(2 * spans + d)
        for d in range(spans):
            cross_out[k, d] = gathered(2 * spans + d)
        cross_done()
        for d in range(spans):
            final_out[k, d] = gathered(spans + d)
        final_done()
        for d in range(spans):
            kept[k, d] = gathered(d)

    def merge_whole(k, _):
        for way in (1, 2):
            raw_copy(mate, 0, way, k).wait_recv()

        def cross_done():
            turn_copy(k).start()
            cross_copy(k, aside, spans).start()

        gather(k, 1, cross_done, lambda: final_copy(k).start())
        return 0

    def merge_joined(k, _):
        for way in range(3):
            raw_copy(mate, 0, way, k).wait_recv()
        gather(k, 0, lambda: cross_copy(k, across, 2 * spans).start(), lambda: None)
        return 0

    def merge(k, _):
        for way in range(3):
            raw_copy(mate, 0, way, k).wait_recv()

        def cross_done():
            far_copy(k).start()
            cross_copy(k, across, spans).start()

        gather(k, 0, cross_done, lambda: final_copy(k).start())
        return 0

    def settle(k):
        a, r = lax.div(k, per), lax.rem(k, per)
        start = pl.multiple_of(r * rows_per, rows_per)
        for l in range(spans):
            moved_cache[a, l, pl.ds(start, rows_per), :] = kept[k, l] + cross_in[k, l]

    def finish(k, _):
        cross_copy(k, across, spans).wait_recv()
        settle(k)
        return 0

    def finish_joined(k, _):
        cross_copy(k, across, 2 * spans).wait_recv()
        for l in range(spans):
            final_out[k, l] = final_out[k, l] + cross_in[k, spans + l]
        final_copy(k).start()
        settle(k)
        return 0

    loads[1].wait()
    loads[2].wait()
    for k in range(len(others)):
        part_copy(k).wait()
    summed = part[...]
    for k in range(len(others)):
        summed = summed + part_in[k]
    resid = hidden[...].astype(jnp.float32) + summed[:spans]
    centre = jnp.mean(resid, axis=-1, keepdims=True)
    spread = jnp.mean((resid - centre) ** 2, axis=-1, keepdims=True)
    gain = ln_gain[...].reshape(1, width)
    bias = ln_bias[...].reshape(1, width)
    normed = (resid - centre) * lax.rsqrt(spread + 1e-05) * gain + bias
    normed = jnp.concatenate([normed, jnp.zeros((pad, width), jnp.float32)], 0)
    query = jnp.dot(
        normed.astype(jnp.bfloat16), query_proj[...], preferred_element_type=jnp.float32
    ).astype(jnp.bfloat16).astype(jnp.float32)

    decoded = []
    for c in range(spans):
        mixed = attend(query[c : c + 1], cross[0, c], cross[1, c], None, None)
        decoded.append(mixed * jnp.where(alive[c] == 1, 1.0, 0.0))

    line[...] = jnp.concatenate(decoded, 0).astype(jnp.bfloat16)

    @pl.when(outer)
    def _():
        line_copy(mate, 0, 0).start()
        line_copy(aside, 1, 1).start()

    @pl.when(inner)
    def _():
        line_copy(aside, 0, 2).start()

    def turn(k, _):
        turn_copy(k).wait_recv()
        turned_copy(k).start()
        return 0

    def outer_forward(k, _):
        raw_copy(mate, 0, 0, k).start()
        raw_copy(mate, 0, 1, k).wait_recv()
        outer_pass_copy(k).start()
        return 0

    @pl.when(outer)
    def _():
        lax.fori_loop(WHOLE, WHOLE + AHEAD, outer_forward, 0)
        line_copy(mate, 0, 1).wait_recv()
        line_pass_copy().start()
        lax.fori_loop(WHOLE + AHEAD, steps, outer_forward, 0)
        lax.fori_loop(0, WHOLE, turn, 0)

    @pl.when(inner)
    def _():
        lax.fori_loop(WHOLE + AHEAD, steps, pass_on, 0)

    def forward(k, _):
        raw_copy(mate, 0, 0, k).wait_recv()
        pass_copy(k).start()
        return 0

    def gather_lines():
        for way in range(3):
            line_copy(mate, 0, way).wait_recv()
        blocks = []
        for held in [line] + [line_in.at[way] for way in range(3)]:
            blocks += [held[c : c + 1, :].astype(jnp.float32) for c in range(spans)]
        rows = []
        for d in range(4 * spans):
            total = blocks[0] * pick[0, 0, d, 0:1, :].astype(jnp.float32)
            for s in range(1, len(blocks)):
                total = total + blocks[s] * pick[0, s, d, 0:1, :].astype(jnp.float32)
            rows.append(total)
        line_out[...] = jnp.concatenate(rows[2 * spans :], 0).astype(jnp.bfloat16)
        line_cross_copy().start()
        line_kept[...] = jnp.concatenate(rows[: 2 * spans], 0)

    def send_lines():
        line_cross_copy().wait_recv()
        total = line_kept[...] + line_cross[...].astype(jnp.float32)
        line_last[...] = total[spans:].astype(jnp.bfloat16)
        line_final_copy().start()
        moved_out[...] = total[:spans].astype(jnp.bfloat16)

    def run(groups):
        while groups:
            ops, starts = [op for op, _ in groups[0]], [k for _, k in groups[0]]
            size = 1
            while size < len(groups) and groups[size] == [(op, k + size) for op, k in groups[0]]:
                size += 1

            def step(i, _, ops=ops, starts=starts):
                for op, k in zip(ops, starts):
                    op(i + k, 0)
                return 0

            if size > 1:
                lax.fori_loop(0, size, step, 0)
            else:
                step(0, 0)
            groups = groups[size:]

    def groups(low, high):
        found = []
        for k in range(low, high):
            group = []
            if k < steps:
                group.append((merge_joined if k < JOINED else merge, k))
            if WHOLE <= k - LAG < JOINED:
                group.append((finish_joined, k - LAG))
            if k < WHOLE + BEHIND:
                group.append((merge_whole, k - BEHIND))
            found.append(group)
        return found

    @pl.when(inner)
    def _():
        lax.fori_loop(0, WHOLE, forward, 0)
        for way in range(1, 5):
            label_copy(mate, 0, way).wait_recv()
        choose(1, (0, 3, 4), (me, mate, aside, mate_aside))
        choose(0, (0, 1, 2), (me, mate, across, beyond))
        run([[(merge_whole, k)] for k in range(WHOLE - BEHIND)])
        run(groups(WHOLE, LINES))
        gather_lines()
        run(groups(LINES, steps + LAG))
        send_lines()

    def place(k, value):
        a, r = lax.div(k, per), lax.rem(k, per)
        start = pl.multiple_of(r * rows_per, rows_per)
        for l in range(spans):
            moved_cache[a, l, pl.ds(start, rows_per), :] = value(l)

    def land(k, _):
        final_copy(k).wait_recv()
        far_copy(k).wait_recv()
        place(k, lambda l: final_in[k, l] + final_far[k, l])
        return 0

    def land_joined(k, _):
        final_copy(k).wait_recv()
        place(k, lambda l: final_in[k, l])
        return 0

    def outer_sent(k, _):
        raw_copy(mate, 0, 0, k).wait_send()
        return 0

    def outer_aside_sent(k, _):
        raw_copy(aside, 1, 1, k).wait_send()
        outer_pass_copy(k).wait_send()
        return 0

    def turned_sent(k, _):
        turned_copy(k).wait_send()
        return 0

    def inner_sent(k, _):
        raw_copy(aside, 0, 2, k).wait_send()
        final_copy(k).wait_send()
        return 0

    def cross_sent(k, _):
        far_copy(k).wait_send()
        cross_copy(k, across, spans).wait_send()
        return 0

    def joined_sent(k, _):
        cross_copy(k, across, 2 * spans).wait_send()
        return 0

    def pass_sent(k, _):
        pass_copy(k).wait_send()
        return 0

    @pl.when(inner)
    def _():
        lax.fori_loop(0, WHOLE, finish, 0)
        lax.fori_loop(JOINED, steps, finish, 0)
        label_copy(aside, 0, 2).wait_send()
        label_copy(across, 1, 3).wait_send()
        label_pass_copy(across, 0, 4).wait_send()
        line_copy(aside, 0, 2).wait_send()
        line_cross_copy().wait_send()
        line_final_copy().wait_send()
        lax.fori_loop(0, steps, inner_sent, 0)
        lax.fori_loop(0, WHOLE, pass_sent, 0)
        lax.fori_loop(0, WHOLE, cross_sent, 0)
        lax.fori_loop(WHOLE, JOINED, joined_sent, 0)
        lax.fori_loop(JOINED, steps, cross_sent, 0)

    @pl.when(outer)
    def _():
        lax.fori_loop(0, WHOLE, land, 0)
        lax.fori_loop(WHOLE, JOINED, land_joined, 0)
        lax.fori_loop(JOINED, steps, land, 0)
        label_copy(mate, 0, 0).wait_send()
        label_copy(aside, 1, 1).wait_send()
        label_pass_copy(mate, 1, 1).wait_send()
        line_copy(mate, 0, 0).wait_send()
        line_copy(aside, 1, 1).wait_send()
        line_pass_copy().wait_send()
        line_final_copy().wait_recv()
        moved_out[...] = line_final[...]
        lax.fori_loop(0, steps, outer_sent, 0)
        lax.fori_loop(WHOLE, steps, outer_aside_sent, 0)
        lax.fori_loop(0, WHOLE, turned_sent, 0)


def body(
    hidden,
    token_qkv,
    self_cache,
    cross_kv,
    cache_len,
    finished,
    new_slot,
    out_proj,
    ln_gain,
    ln_bias,
    query_proj,
):
    count, cores = lax.axis_size("batch"), lax.axis_size("mp")
    spans, width = hidden.shape
    slots, local = self_cache.shape[2:]
    moves = len(DISTANCES)
    smem = pl.BlockSpec(memory_space=pltpu.SMEM)
    vmem = pl.BlockSpec(memory_space=pltpu.VMEM)
    away = pl.BlockSpec(memory_space=pl.ANY)
    bf16, f32 = jnp.bfloat16, jnp.float32
    operands = (
        cache_len,
        finished,
        new_slot,
        hidden,
        token_qkv,
        self_cache,
        ln_gain,
        ln_bias,
        cross_kv,
        out_proj,
        query_proj,
    )
    parcels = pltpu.VMEM((moves, 2, slots, local), bf16)
    tiles = pltpu.VMEM((moves, 16, local), bf16)
    dma = pltpu.SemaphoreType.DMA
    inputs = [pltpu.VMEM(array.shape, bf16) for array in (cross_kv, out_proj, query_proj)]
    parts = [pltpu.VMEM((8, width), f32), pltpu.VMEM((cores - 1, 8, width), f32)]
    steps = 2 * slots // ROWS
    if count == 2 * (REACH + 1):
        function, specs = relay_kernel, [away] * 8

        def blocks(*lead):
            return pltpu.VMEM(lead + (ROWS, local), bf16)

        small = [pltpu.SMEM((spans,), jnp.int32)] * 3 + [
            pltpu.VMEM(hidden.shape, bf16),
            pltpu.VMEM(token_qkv.shape, bf16),
            pltpu.VMEM(ln_gain.shape, f32),
            pltpu.VMEM(ln_bias.shape, f32),
        ]
        scratch = small + [pltpu.VMEM(self_cache.shape, bf16)] + inputs + [
            blocks(steps, spans),
            blocks(3, steps, spans),
            blocks(steps, 2 * spans),
            blocks(steps, 2 * spans),
            blocks(steps, spans),
            blocks(steps, spans),
            blocks(steps, spans),
            blocks(steps, spans),
            blocks(2, 4 * spans, 4 * spans),
            pltpu.VMEM((8, 128), f32),
            pltpu.VMEM((5, 8, 128), f32),
            pltpu.VMEM((spans, local), bf16),
            pltpu.VMEM((3, spans, local), bf16),
            pltpu.VMEM((2 * spans, local), f32),
            pltpu.VMEM((2 * spans, local), bf16),
            pltpu.VMEM((2 * spans, local), bf16),
            pltpu.VMEM((spans, local), bf16),
            pltpu.VMEM((spans, local), bf16),
            *parts,
            dma((12,)),
            dma((2, steps)),
            dma((3, steps)),
            dma((6, steps)),
            dma((3,)),
            dma((5,)),
            dma((3,)),
            dma((3,)),
            dma((4,)),
            dma((2, cores - 1)),
            dma((steps,)),
        ]
    else:
        function, specs = kernel, [smem] * 3 + [vmem] * 5
        scratch = inputs + [
            pltpu.VMEM(self_cache.shape, bf16),
            parcels,
            parcels,
            tiles,
            tiles,
            tiles,
            tiles,
            *parts,
            dma((3,)),
            dma((2, moves)),
            dma((2, moves)),
            dma((2, moves)),
            dma((2, cores - 1)),
        ]
    return pl.pallas_call(
        functools.partial(function, count, cores),
        out_shape=(
            pltpu.VMEM(self_cache.shape, bf16),
            pltpu.VMEM((spans, local), bf16),
        ),
        in_specs=specs + [away] * 3,
        out_specs=(vmem, vmem),
        scratch_shapes=scratch,
        compiler_params=pltpu.CompilerParams(collective_id=0, has_side_effects=True),
    )(*operands)


def solution(mesh):
    placed = (
        P(("groups", "batch"), None),
        P(None, ("groups", "batch"), "mp"),
        P(None, ("groups", "batch"), None, "mp"),
        P(None, ("groups", "batch"), None, "mp"),
        P(("groups", "batch")),
        P(("groups", "batch")),
        P(("groups", "batch")),
        P("mp", None),
        P(),
        P(),
        P(None, "mp"),
    )
    return jax.shard_map(
        body,
        mesh=mesh,
        in_specs=placed,
        out_specs=(P(None, ("groups", "batch"), None, "mp"), P(("groups", "batch"), "mp")),
        check_vma=False,
    )
```

```python
import functools

import jax
import jax.numpy as jnp
from jax import lax
from jax.experimental import pallas as pl
from jax.experimental.pallas import tpu as pltpu
from jax.sharding import PartitionSpec as P

HEAD_DIM = 64
REACH = 3
MESH = pl.DeviceIdType.MESH
DISTANCES = [3, -3, 2, -2, 1, -1]
ROWS = 16
WHOLE = 6
JOINED = 14
AHEAD = 5
LAG = 3
BEHIND = 3
LINES = 11


def attend(query, keys, values, length, own):
    slots, width = keys.shape
    heads = width // HEAD_DIM
    rows = -(-heads // 16) * 16
    row = lax.broadcasted_iota(jnp.int32, (rows, width), 0)
    column = lax.broadcasted_iota(jnp.int32, (rows, width), 1)
    low = row * HEAD_DIM
    mine = (column >= low) & (column < low + HEAD_DIM)
    spread = jnp.where(mine, query.astype(jnp.float32), 0.0)
    factor = HEAD_DIM ** (-0.5)
    scores = (
        lax.dot_general(
            spread.astype(jnp.bfloat16),
            keys,
            (((1,), (1,)), ((), ())),
            preferred_element_type=jnp.float32,
        )
        * factor
    )
    if length is not None:
        usable = lax.broadcasted_iota(jnp.int32, (rows, slots), 1) < length
        scores = jnp.where(usable, scores, -1e30)
    highest = jnp.max(scores, axis=-1, keepdims=True)
    if own is not None:
        new_key, new_value = own
        own_score = jnp.sum(spread * new_key.astype(jnp.float32), axis=-1, keepdims=True) * factor
        highest = jnp.maximum(highest, own_score)
    weight = jnp.exp(scores - highest)
    if length is not None:
        weight = jnp.where(usable, weight, 0.0)
    total = jnp.sum(weight, axis=-1, keepdims=True)
    if own is not None:
        own_weight = jnp.exp(own_score - highest)
        total = total + own_weight
    weight = (weight / total).astype(jnp.bfloat16)
    mixed = jnp.dot(weight, values, preferred_element_type=jnp.float32)
    if own is not None:
        own_weight = (own_weight / total).astype(jnp.bfloat16).astype(jnp.float32)
        mixed = mixed + own_weight * new_value.astype(jnp.float32)
    return jnp.sum(jnp.where(mine, mixed, 0.0), axis=0, keepdims=True)


def kernel(
    count,
    cores,
    cache_len,
    finished,
    new_slot,
    hidden,
    token_qkv,
    self_cache,
    ln_gain,
    ln_bias,
    cross_hbm,
    out_proj_hbm,
    query_proj_hbm,
    moved_cache,
    moved_out,
    cross,
    out_proj,
    query_proj,
    updated,
    parcel,
    arrived,
    mark,
    mark_in,
    line,
    line_in,
    part,
    part_in,
    load_sem,
    cache_sems,
    mark_sems,
    line_sems,
    part_sems,
):
    spans, width = hidden.shape
    slots, local = self_cache.shape[2:]
    me = lax.axis_index("batch")
    core = lax.axis_index("mp")
    loads = [
        pltpu.make_async_copy(source, target, load_sem.at[i])
        for i, (source, target) in enumerate(
            [(out_proj_hbm, out_proj), (query_proj_hbm, query_proj), (cross_hbm, cross)]
        )
    ]
    for load in loads:
        load.start()

    barrier = pltpu.get_barrier_semaphore()
    targets = [lax.rem(me + distance + count, count) for distance in DISTANCES]
    for target in targets:
        pl.semaphore_signal(barrier, inc=1, device_id={"batch": target}, device_id_type=MESH)
    others = [lax.rem(core + k, cores) for k in range(1, cores)]
    for other in others:
        pl.semaphore_signal(barrier, inc=1, device_id={"mp": other}, device_id_type=MESH)

    half = count // 2
    alive, offset, place = [], [], []
    for c in range(spans):
        slot = new_slot[c]
        owner = lax.div(slot, spans)
        offset.append(lax.rem(owner - me + half + count, count) - half)
        place.append(lax.rem(slot, spans))
        alive.append(jnp.where(finished[c] == 0, 1, 0))

    position = lax.broadcasted_iota(jnp.int32, (slots, local), 0)
    for c in range(spans):
        length = cache_len[c]
        older = jnp.where(position < length * alive[c], 1.0, 0.0).astype(jnp.bfloat16)
        fresh = jnp.where(position == jnp.where(alive[c] == 1, length, -1), 1.0, 0.0).astype(
            jnp.bfloat16
        )
        for a in range(2):
            updated[a, c] = self_cache[a, c] * older + token_qkv[1 + a, c : c + 1, :] * fresh

    def flag(value, shape):
        return jnp.full(shape, jnp.where(value, 1.0, 0.0), jnp.float32).astype(jnp.bfloat16)

    marker_row = lax.broadcasted_iota(jnp.int32, mark.shape[1:], 0)
    for i, distance in enumerate(DISTANCES):
        marker = jnp.zeros(mark.shape[1:], jnp.float32)
        for c in range(spans):
            at = jnp.where(offset[c] == distance, place[c], -1)
            marker = jnp.where(marker_row == at, 1.0, marker)
        mark[i] = marker.astype(jnp.bfloat16)

    def send(source, target, sems, i, distance):
        return pltpu.make_async_remote_copy(
            src_ref=source,
            dst_ref=target,
            send_sem=sems.at[0, i],
            recv_sem=sems.at[1, i],
            device_id={"batch": targets[i]},
            device_id_type=MESH,
        )

    pl.semaphore_wait(barrier, len(targets) + len(others))
    mark_copies, cache_copies = [], []
    for i, distance in enumerate(DISTANCES):
        copy = send(mark.at[i], mark_in.at[i], mark_sems, i, distance)
        copy.start()
        mark_copies.append(copy)
    for i, distance in enumerate(DISTANCES):
        for a in range(2):
            total = updated[a, 0] * flag(offset[0] == distance, (1, local))
            for c in range(1, spans):
                total = total + updated[a, c] * flag(offset[c] == distance, (1, local))
            parcel[i, a] = total
        copy = send(parcel.at[i], arrived.at[i], cache_sems, i, distance)
        copy.start()
        cache_copies.append(copy)

    for l in range(spans):
        for a in range(2):
            total = updated[a, 0] * flag((offset[0] == 0) & (place[0] == l), (1, local))
            for c in range(1, spans):
                keep = flag((offset[c] == 0) & (place[c] == l), (1, local))
                total = total + updated[a, c] * keep
            moved_cache[a, l] = total

    contexts = []
    for c in range(spans):
        query, key, value = (token_qkv[k, c : c + 1, :] for k in range(3))
        contexts.append(
            attend(query, self_cache[0, c], self_cache[1, c], cache_len[c], (key, value))
        )
    pad = part.shape[0] - spans
    context = jnp.concatenate(contexts + [jnp.zeros((pad, local), jnp.float32)], 0)
    context = context.astype(jnp.bfloat16)
    loads[0].wait()
    part[...] = jnp.dot(context, out_proj[...], preferred_element_type=jnp.float32)
    part_copies = []
    for k, other in enumerate(others):
        copy = pltpu.make_async_remote_copy(
            src_ref=part,
            dst_ref=part_in.at[k],
            send_sem=part_sems.at[0, k],
            recv_sem=part_sems.at[1, k],
            device_id={"mp": other},
            device_id_type=MESH,
        )
        copy.start()
        part_copies.append(copy)
    loads[1].wait()
    loads[2].wait()
    for copy in part_copies:
        copy.wait()
    summed = part[...]
    for k in range(len(others)):
        summed = summed + part_in[k]
    resid = hidden[...].astype(jnp.float32) + summed[:spans]
    centre = jnp.mean(resid, axis=-1, keepdims=True)
    spread = jnp.mean((resid - centre) ** 2, axis=-1, keepdims=True)
    gain = ln_gain[...].reshape(1, width)
    bias = ln_bias[...].reshape(1, width)
    normed = (resid - centre) * lax.rsqrt(spread + 1e-05) * gain + bias
    normed = jnp.concatenate([normed, jnp.zeros((pad, width), jnp.float32)], 0)
    query = jnp.dot(
        normed.astype(jnp.bfloat16), query_proj[...], preferred_element_type=jnp.float32
    ).astype(jnp.bfloat16).astype(jnp.float32)
    decoded = []
    for c in range(spans):
        mixed = attend(query[c : c + 1], cross[0, c], cross[1, c], None, None)
        decoded.append(mixed * jnp.where(alive[c] == 1, 1.0, 0.0))

    line_copies = []
    blank = jnp.zeros((line.shape[1] - 1, local), jnp.float32)
    for i, distance in enumerate(DISTANCES):
        row = jnp.zeros((1, local), jnp.float32)
        for c in range(spans):
            row = row + decoded[c] * jnp.where(offset[c] == distance, 1.0, 0.0)
        line[i] = jnp.concatenate([row, blank], 0).astype(jnp.bfloat16)
        copy = send(line.at[i], line_in.at[i], line_sems, i, distance)
        copy.start()
        line_copies.append(copy)

    rows = []
    for l in range(spans):
        row = jnp.zeros((1, local), jnp.float32)
        for c in range(spans):
            keep = (offset[c] == 0) & (place[c] == l)
            row = row + decoded[c] * jnp.where(keep, 1.0, 0.0)
        rows.append(row)
    for i in range(len(DISTANCES)):
        mark_copies[i].wait()
        cache_copies[i].wait()
        for l in range(spans):
            taken = mark_in[i, l : l + 1, :]
            for a in range(2):
                moved_cache[a, l] = moved_cache[a, l] + arrived[i, a] * taken
    for i in range(len(DISTANCES)):
        line_copies[i].wait()
        for l in range(spans):
            taken = mark_in[i, l : l + 1, :].astype(jnp.float32)
            rows[l] = rows[l] + line_in[i, 0:1, :].astype(jnp.float32) * taken
    moved_out[...] = jnp.concatenate(rows, 0).astype(jnp.bfloat16)


def relay_kernel(
    count,
    cores,
    cache_len_hbm,
    finished_hbm,
    new_slot_hbm,
    hidden_hbm,
    token_qkv_hbm,
    cache_hbm,
    ln_gain_hbm,
    ln_bias_hbm,
    cross_hbm,
    out_proj_hbm,
    query_proj_hbm,
    moved_cache,
    moved_out,
    cache_len,
    finished,
    new_slot,
    hidden,
    token_qkv,
    ln_gain,
    ln_bias,
    self_cache,
    cross,
    out_proj,
    query_proj,
    own,
    raw_in,
    cross_out,
    cross_in,
    kept,
    final_out,
    final_in,
    final_far,
    pick,
    label,
    label_in,
    line,
    line_in,
    line_kept,
    line_out,
    line_cross,
    line_last,
    line_final,
    part,
    part_in,
    load_sem,
    send_sems,
    mate_recv,
    second_recv,
    whole_recv,
    cross_recv,
    final_recv,
    far_recv,
    label_send,
    label_recv,
    line_send,
    line_recv,
    line_hops,
    part_sems,
):
    spans, width = hidden.shape
    slots, local = self_cache.shape[2:]
    steps, _, rows_per, _ = own.shape
    per = steps // 2
    me = lax.axis_index("batch")
    core = lax.axis_index("mp")
    level, column = lax.div(me, 2), lax.rem(me, 2)
    inner = (level == 1) | (level == REACH - 1)
    outer = jnp.logical_not(inner)
    barrier = pltpu.get_barrier_semaphore()

    def greet(where):
        pl.semaphore_signal(barrier, inc=1, device_id=where, device_id_type=MESH)

    mate_level = jnp.where(level == 0, 1, jnp.where(level == 1, 0, jnp.where(level == 2, 3, 2)))
    mate = mate_level * 2 + column
    mate_aside = mate_level * 2 + 1 - column
    aside = level * 2 + 1 - column
    across = (REACH - level) * 2 + column
    beyond = (REACH - mate_level) * 2 + column
    others = [lax.rem(core + k, cores) for k in range(1, cores)]
    for node in (mate, aside):
        greet({"batch": node})

    @pl.when(inner)
    def _():
        greet({"batch": across})

    for other in others:
        greet({"mp": other})
    loads = [
        pltpu.make_async_copy(source, target, load_sem.at[i])
        for i, (source, target) in enumerate(
            [
                (out_proj_hbm, out_proj),
                (query_proj_hbm, query_proj),
                (cross_hbm, cross),
                (cache_hbm.at[0], self_cache.at[0]),
                (cache_hbm.at[1], self_cache.at[1]),
                (cache_len_hbm, cache_len),
                (finished_hbm, finished),
                (new_slot_hbm, new_slot),
                (hidden_hbm, hidden),
                (token_qkv_hbm, token_qkv),
                (ln_gain_hbm, ln_gain),
                (ln_bias_hbm, ln_bias),
            ]
        )
    ]
    for i in [3, *range(5, len(loads)), 4, 0, 1, 2]:
        loads[i].start()
    for load in loads[5:]:
        load.wait()

    alive = [jnp.where(finished[c] == 0, 1, 0) for c in range(spans)]

    def to(node, source, target, sent, received):
        return pltpu.make_async_remote_copy(
            src_ref=source,
            dst_ref=target,
            send_sem=sent,
            recv_sem=received,
            device_id={"batch": node},
            device_id_type=MESH,
        )

    own_send, aside_send, pass_send, far_send, cross_send, joined_send, final_send = (
        send_sems.at[i] for i in range(7)
    )

    def mate_copy(k):
        return to(mate, own.at[k], raw_in.at[0, k], own_send, mate_recv.at[k])

    def across_copy(k):
        return to(across, own.at[k], raw_in.at[1, k], own_send, whole_recv.at[k])

    def aside_copy(k):
        return to(aside, own.at[k], raw_in.at[2, k], aside_send, second_recv.at[k])

    def pass_copy(k):
        return to(across, raw_in.at[0, k], raw_in.at[2, k], pass_send, second_recv.at[k])

    def outer_pass_copy(k):
        return to(mate, raw_in.at[2, k], raw_in.at[1, k], pass_send, mate_recv.at[k])

    def arrive(blocks, sem):
        pltpu.make_async_copy(blocks, blocks, sem).wait()

    def far_copy(k):
        return to(
            beyond,
            cross_out.at[k, pl.ds(spans, spans)],
            final_far.at[k],
            far_send,
            far_recv.at[k - JOINED + WHOLE],
        )

    def turn_copy(k):
        return to(
            mate,
            cross_out.at[k, pl.ds(spans, spans)],
            raw_in.at[2, k],
            far_send,
            second_recv.at[k],
        )

    def turned_copy(k):
        return to(aside, raw_in.at[2, k], final_far.at[k], far_send, far_recv.at[k])

    def cross_copy(k, node, count, sent):
        return to(
            node,
            cross_out.at[k, pl.ds(0, count)],
            cross_in.at[k, pl.ds(0, count)],
            sent,
            cross_recv.at[k],
        )

    def final_copy(k):
        return to(mate, final_out.at[k], final_in.at[k], final_send, final_recv.at[k])

    def label_copy(node, lane, way):
        return to(node, label, label_in.at[way], label_send.at[lane], label_recv.at[way])

    def line_copy(node, lane, way):
        return to(node, line, line_in.at[way], line_send.at[lane], line_recv.at[way])

    def label_pass_copy(node, here, there):
        return to(node, label_in.at[here], label_in.at[there], label_send.at[2], label_recv.at[there])

    def line_pass_copy():
        return to(mate, line_in.at[1], line_in.at[1], line_send.at[2], line_recv.at[1])

    def line_cross_copy():
        return to(across, line_out, line_cross, line_hops.at[0], line_hops.at[1])

    def line_final_copy():
        return to(mate, line_last, line_final, line_hops.at[2], line_hops.at[3])

    label_row = lax.broadcasted_iota(jnp.int32, label.shape, 0)
    labels = jnp.zeros(label.shape, jnp.int32)
    for c in range(spans):
        labels = jnp.where(label_row == c, new_slot[c], labels)
    label[...] = labels.astype(jnp.float32)

    @pl.when(inner)
    def _():
        pl.semaphore_wait(barrier, 3 + len(others))

    @pl.when(outer)
    def _():
        pl.semaphore_wait(barrier, 2 + len(others))

    position = lax.broadcasted_iota(jnp.int32, (rows_per, local), 0)
    ends = [cache_len[c] * alive[c] for c in range(spans)]
    fresh_at = [jnp.where(alive[c] == 1, cache_len[c], -1) for c in range(spans)]

    def grow(k, _):
        a, r = lax.div(k, per), lax.rem(k, per)
        start = pl.multiple_of(r * rows_per, rows_per)
        at = position + start
        for c in range(spans):
            older = jnp.where(at < ends[c], 1.0, 0.0).astype(jnp.bfloat16)
            fresh = jnp.where(at == fresh_at[c], 1.0, 0.0).astype(jnp.bfloat16)
            new = jnp.where(a == 0, token_qkv[1, c : c + 1, :].astype(jnp.float32),
                            token_qkv[2, c : c + 1, :].astype(jnp.float32)).astype(jnp.bfloat16)
            own[k, c] = self_cache[a, c, pl.ds(start, rows_per), :] * older + new * fresh

        return 0

    def pass_whole(k, _):
        grow(k, 0)

        @pl.when(outer)
        def _():
            mate_copy(k).start()

        @pl.when(inner)
        def _():
            across_copy(k).start()

        return 0

    def pass_on(k, _):
        aside_copy(k).start()
        return 0

    @pl.when(outer)
    def _():
        label_copy(mate, 0, 0).start()
        label_copy(aside, 1, 1).start()

    @pl.when(inner)
    def _():
        label_copy(aside, 0, 2).start()
        label_copy(across, 1, 3).start()

    loads[3].wait()
    lax.fori_loop(0, WHOLE, pass_whole, 0)
    lax.fori_loop(WHOLE, per, grow, 0)
    loads[4].wait()
    lax.fori_loop(per, steps, grow, 0)

    @pl.when(inner)
    def _():
        lax.fori_loop(WHOLE, WHOLE + AHEAD, pass_on, 0)

    @pl.when(outer)
    def _():
        lax.fori_loop(WHOLE, steps, pass_on, 0)


    def self_part():
        contexts = []
        for c in range(spans):
            query, key, value = (token_qkv[k, c : c + 1, :] for k in range(3))
            contexts.append(
                attend(query, self_cache[0, c], self_cache[1, c], cache_len[c], (key, value))
            )
        context = jnp.concatenate(contexts + [jnp.zeros((pad, local), jnp.float32)], 0)
        context = context.astype(jnp.bfloat16)
        loads[0].wait()
        part[...] = jnp.dot(context, out_proj[...], preferred_element_type=jnp.float32)

    def part_copy(k):
        return pltpu.make_async_remote_copy(
            src_ref=part,
            dst_ref=part_in.at[k],
            send_sem=part_sems.at[0, k],
            recv_sem=part_sems.at[1, k],
            device_id={"mp": others[k]},
            device_id_type=MESH,
        )

    pad = part.shape[0] - spans
    self_part()
    for k in range(len(others)):
        part_copy(k).start()

    @pl.when(outer)
    def _():
        label_copy(mate, 0, 1).wait_recv()
        label_pass_copy(mate, 1, 1).start()

    @pl.when(inner)
    def _():
        label_copy(mate, 0, 0).wait_recv()
        label_pass_copy(across, 0, 4).start()

    def choose(p, ways, nodes):
        for s, source in enumerate([label] + [label_in.at[way] for way in ways]):
            for c in range(spans):
                held = jnp.broadcast_to(source[c : c + 1, 0:1], (rows_per, local))
                for d, node in enumerate(nodes):
                    for l in range(spans):
                        wanted = jnp.full((rows_per, local), node * spans + l, jnp.int32)
                        pick[p, s * spans + c, d * spans + l] = jnp.where(
                            held == wanted.astype(jnp.float32), 1.0, 0.0
                        ).astype(jnp.bfloat16)

    def gather(k, p, cross_done, final_done):
        blocks = [own[k, c] for c in range(spans)]
        for way in range(3):
            blocks += [raw_in[way, k, c] for c in range(spans)]

        def gathered(d):
            total = blocks[0] * pick[p, 0, d]
            for s in range(1, len(blocks)):
                total = total + blocks[s] * pick[p, s, d]
            return total

        for d in range(spans, 2 * spans):
            cross_out[k, d] = gathered(2 * spans + d)
        for d in range(spans):
            cross_out[k, d] = gathered(2 * spans + d)
        cross_done()
        for d in range(spans):
            final_out[k, d] = gathered(spans + d)
        final_done()
        for d in range(spans):
            kept[k, d] = gathered(d)

    def gathered_in(k):
        arrive(raw_in.at[pl.ds(0, 2), k], mate_recv.at[k])
        aside_copy(k).wait_recv()

    def merge_whole(k, _):
        across_copy(k).wait_recv()
        pass_copy(k).wait_recv()

        def cross_done():
            turn_copy(k).start()
            cross_copy(k, aside, spans, cross_send).start()

        gather(k, 1, cross_done, lambda: final_copy(k).start())
        return 0

    def merge_joined(k, _):
        gathered_in(k)
        gather(k, 0, lambda: cross_copy(k, across, 2 * spans, joined_send).start(), lambda: None)
        return 0

    def merge(k, _):
        gathered_in(k)

        def cross_done():
            far_copy(k).start()
            cross_copy(k, across, spans, cross_send).start()

        gather(k, 0, cross_done, lambda: final_copy(k).start())
        return 0

    def settle(k):
        a, r = lax.div(k, per), lax.rem(k, per)
        start = pl.multiple_of(r * rows_per, rows_per)
        for l in range(spans):
            moved_cache[a, l, pl.ds(start, rows_per), :] = kept[k, l] + cross_in[k, l]

    def finish(k, _):
        cross_copy(k, across, spans, cross_send).wait_recv()
        settle(k)
        return 0

    def finish_joined(k, _):
        cross_copy(k, across, 2 * spans, joined_send).wait_recv()
        for l in range(spans):
            final_out[k, l] = final_out[k, l] + cross_in[k, spans + l]
        final_copy(k).start()
        settle(k)
        return 0

    loads[1].wait()
    loads[2].wait()
    for k in range(len(others)):
        part_copy(k).wait()
    summed = part[...]
    for k in range(len(others)):
        summed = summed + part_in[k]
    resid = hidden[...].astype(jnp.float32) + summed[:spans]
    centre = jnp.mean(resid, axis=-1, keepdims=True)
    spread = jnp.mean((resid - centre) ** 2, axis=-1, keepdims=True)
    gain = ln_gain[...].reshape(1, width)
    bias = ln_bias[...].reshape(1, width)
    normed = (resid - centre) * lax.rsqrt(spread + 1e-05) * gain + bias
    normed = jnp.concatenate([normed, jnp.zeros((pad, width), jnp.float32)], 0)
    query = jnp.dot(
        normed.astype(jnp.bfloat16), query_proj[...], preferred_element_type=jnp.float32
    ).astype(jnp.bfloat16).astype(jnp.float32)

    decoded = []
    for c in range(spans):
        mixed = attend(query[c : c + 1], cross[0, c], cross[1, c], None, None)
        decoded.append(mixed * jnp.where(alive[c] == 1, 1.0, 0.0))

    line[...] = jnp.concatenate(decoded, 0).astype(jnp.bfloat16)

    @pl.when(outer)
    def _():
        line_copy(mate, 0, 0).start()
        line_copy(aside, 1, 1).start()

    @pl.when(inner)
    def _():
        line_copy(aside, 0, 2).start()

    def turn(k, _):
        turn_copy(k).wait_recv()
        turned_copy(k).start()
        return 0

    def outer_forward(k, _):
        mate_copy(k).start()
        aside_copy(k).wait_recv()
        outer_pass_copy(k).start()
        return 0

    @pl.when(outer)
    def _():
        lax.fori_loop(WHOLE, WHOLE + AHEAD, outer_forward, 0)
        line_copy(mate, 0, 1).wait_recv()
        line_pass_copy().start()
        lax.fori_loop(WHOLE + AHEAD, steps, outer_forward, 0)
        lax.fori_loop(0, WHOLE, turn, 0)

    @pl.when(inner)
    def _():
        lax.fori_loop(WHOLE + AHEAD, steps, pass_on, 0)

    def forward(k, _):
        mate_copy(k).wait_recv()
        pass_copy(k).start()
        return 0

    def gather_lines():
        for way in range(3):
            line_copy(mate, 0, way).wait_recv()
        blocks = []
        for held in [line] + [line_in.at[way] for way in range(3)]:
            blocks += [held[c : c + 1, :].astype(jnp.float32) for c in range(spans)]
        rows = []
        for d in range(4 * spans):
            total = blocks[0] * pick[0, 0, d, 0:1, :].astype(jnp.float32)
            for s in range(1, len(blocks)):
                total = total + blocks[s] * pick[0, s, d, 0:1, :].astype(jnp.float32)
            rows.append(total)
        line_out[...] = jnp.concatenate(rows[2 * spans :], 0).astype(jnp.bfloat16)
        line_cross_copy().start()
        line_kept[...] = jnp.concatenate(rows[: 2 * spans], 0)

    def send_lines():
        line_cross_copy().wait_recv()
        total = line_kept[...] + line_cross[...].astype(jnp.float32)
        line_last[...] = total[spans:].astype(jnp.bfloat16)
        line_final_copy().start()
        moved_out[...] = total[:spans].astype(jnp.bfloat16)

    def run(groups):
        while groups:
            ops, starts = [op for op, _ in groups[0]], [k for _, k in groups[0]]
            size = 1
            while size < len(groups) and groups[size] == [(op, k + size) for op, k in groups[0]]:
                size += 1

            def step(i, _, ops=ops, starts=starts):
                for op, k in zip(ops, starts):
                    op(i + k, 0)
                return 0

            if size > 1:
                lax.fori_loop(0, size, step, 0)
            else:
                step(0, 0)
            groups = groups[size:]

    def groups(low, high):
        found = []
        for k in range(low, high):
            group = []
            if k < steps:
                group.append((merge_joined if k < JOINED else merge, k))
            if WHOLE <= k - LAG < JOINED:
                group.append((finish_joined, k - LAG))
            if k < WHOLE + BEHIND:
                group.append((merge_whole, k - BEHIND))
            found.append(group)
        return found

    @pl.when(inner)
    def _():
        lax.fori_loop(0, WHOLE, forward, 0)
        for way in range(1, 5):
            label_copy(mate, 0, way).wait_recv()
        choose(1, (0, 3, 4), (me, mate, aside, mate_aside))
        choose(0, (0, 1, 2), (me, mate, across, beyond))
        run([[(merge_whole, k)] for k in range(WHOLE - BEHIND)])
        run(groups(WHOLE, LINES))
        gather_lines()
        run(groups(LINES, steps + LAG))
        send_lines()

    def place(k, value):
        a, r = lax.div(k, per), lax.rem(k, per)
        start = pl.multiple_of(r * rows_per, rows_per)
        for l in range(spans):
            moved_cache[a, l, pl.ds(start, rows_per), :] = value(l)

    def land_whole(k, _):
        final_copy(k).wait_recv()
        turned_copy(k).wait_recv()
        place(k, lambda l: final_in[k, l] + final_far[k, l])
        return 0

    def land(k, _):
        final_copy(k).wait_recv()
        far_copy(k).wait_recv()
        place(k, lambda l: final_in[k, l] + final_far[k, l])
        return 0

    def land_joined(k, _):
        final_copy(k).wait_recv()
        place(k, lambda l: final_in[k, l])
        return 0

    rest, late = steps - WHOLE, steps - JOINED

    @pl.when(inner)
    def _():
        lax.fori_loop(0, WHOLE, finish, 0)
        lax.fori_loop(JOINED, steps, finish, 0)
        label_copy(aside, 0, 2).wait_send()
        label_copy(across, 1, 3).wait_send()
        label_pass_copy(across, 0, 4).wait_send()
        line_copy(aside, 0, 2).wait_send()
        line_cross_copy().wait_send()
        line_final_copy().wait_send()
        arrive(own.at[pl.ds(0, WHOLE)], own_send)
        arrive(own.at[pl.ds(0, rest)], aside_send)
        arrive(own.at[pl.ds(0, WHOLE)], pass_send)
        arrive(own.at[pl.ds(0, WHOLE + late)], far_send)
        arrive(own.at[pl.ds(0, WHOLE + late)], cross_send)
        arrive(cross_out.at[pl.ds(0, JOINED - WHOLE)], joined_send)
        arrive(own, final_send)

    @pl.when(outer)
    def _():
        lax.fori_loop(0, WHOLE, land_whole, 0)
        lax.fori_loop(WHOLE, JOINED, land_joined, 0)
        lax.fori_loop(JOINED, steps, land, 0)
        label_copy(mate, 0, 0).wait_send()
        label_copy(aside, 1, 1).wait_send()
        label_pass_copy(mate, 1, 1).wait_send()
        line_copy(mate, 0, 0).wait_send()
        line_copy(aside, 1, 1).wait_send()
        line_pass_copy().wait_send()
        line_final_copy().wait_recv()
        moved_out[...] = line_final[...]
        arrive(own, own_send)
        arrive(own.at[pl.ds(0, rest)], aside_send)
        arrive(own.at[pl.ds(0, rest)], pass_send)
        arrive(own.at[pl.ds(0, WHOLE)], far_send)


def body(
    hidden,
    token_qkv,
    self_cache,
    cross_kv,
    cache_len,
    finished,
    new_slot,
    out_proj,
    ln_gain,
    ln_bias,
    query_proj,
):
    count, cores = lax.axis_size("batch"), lax.axis_size("mp")
    spans, width = hidden.shape
    slots, local = self_cache.shape[2:]
    moves = len(DISTANCES)
    smem = pl.BlockSpec(memory_space=pltpu.SMEM)
    vmem = pl.BlockSpec(memory_space=pltpu.VMEM)
    away = pl.BlockSpec(memory_space=pl.ANY)
    bf16, f32 = jnp.bfloat16, jnp.float32
    operands = (
        cache_len,
        finished,
        new_slot,
        hidden,
        token_qkv,
        self_cache,
        ln_gain,
        ln_bias,
        cross_kv,
        out_proj,
        query_proj,
    )
    parcels = pltpu.VMEM((moves, 2, slots, local), bf16)
    tiles = pltpu.VMEM((moves, 16, local), bf16)
    dma = pltpu.SemaphoreType.DMA
    inputs = [pltpu.VMEM(array.shape, bf16) for array in (cross_kv, out_proj, query_proj)]
    parts = [pltpu.VMEM((8, width), f32), pltpu.VMEM((cores - 1, 8, width), f32)]
    steps = 2 * slots // ROWS
    if count == 2 * (REACH + 1):
        function, specs = relay_kernel, [away] * 8

        def blocks(*lead):
            return pltpu.VMEM(lead + (ROWS, local), bf16)

        small = [pltpu.SMEM((spans,), jnp.int32)] * 3 + [
            pltpu.VMEM(hidden.shape, bf16),
            pltpu.VMEM(token_qkv.shape, bf16),
            pltpu.VMEM(ln_gain.shape, f32),
            pltpu.VMEM(ln_bias.shape, f32),
        ]
        scratch = small + [pltpu.VMEM(self_cache.shape, bf16)] + inputs + [
            blocks(steps, spans),
            blocks(3, steps, spans),
            blocks(steps, 2 * spans),
            blocks(steps, 2 * spans),
            blocks(steps, spans),
            blocks(steps, spans),
            blocks(steps, spans),
            blocks(steps, spans),
            blocks(2, 4 * spans, 4 * spans),
            pltpu.VMEM((8, 128), f32),
            pltpu.VMEM((5, 8, 128), f32),
            pltpu.VMEM((spans, local), bf16),
            pltpu.VMEM((3, spans, local), bf16),
            pltpu.VMEM((2 * spans, local), f32),
            pltpu.VMEM((2 * spans, local), bf16),
            pltpu.VMEM((2 * spans, local), bf16),
            pltpu.VMEM((spans, local), bf16),
            pltpu.VMEM((spans, local), bf16),
            *parts,
            dma((12,)),
            dma((7,)),
            dma((steps,)),
            dma((steps,)),
            dma((WHOLE,)),
            dma((steps,)),
            dma((steps,)),
            dma((WHOLE + steps - JOINED,)),
            dma((3,)),
            dma((5,)),
            dma((3,)),
            dma((3,)),
            dma((4,)),
            dma((2, cores - 1)),
        ]
    else:
        function, specs = kernel, [smem] * 3 + [vmem] * 5
        scratch = inputs + [
            pltpu.VMEM(self_cache.shape, bf16),
            parcels,
            parcels,
            tiles,
            tiles,
            tiles,
            tiles,
            *parts,
            dma((3,)),
            dma((2, moves)),
            dma((2, moves)),
            dma((2, moves)),
            dma((2, cores - 1)),
        ]
    return pl.pallas_call(
        functools.partial(function, count, cores),
        out_shape=(
            pltpu.VMEM(self_cache.shape, bf16),
            pltpu.VMEM((spans, local), bf16),
        ),
        in_specs=specs + [away] * 3,
        out_specs=(vmem, vmem),
        scratch_shapes=scratch,
        compiler_params=pltpu.CompilerParams(collective_id=0, has_side_effects=True),
    )(*operands)


def solution(mesh):
    placed = (
        P(("groups", "batch"), None),
        P(None, ("groups", "batch"), "mp"),
        P(None, ("groups", "batch"), None, "mp"),
        P(None, ("groups", "batch"), None, "mp"),
        P(("groups", "batch")),
        P(("groups", "batch")),
        P(("groups", "batch")),
        P("mp", None),
        P(),
        P(),
        P(None, "mp"),
    )
    return jax.shard_map(
        body,
        mesh=mesh,
        in_specs=placed,
        out_specs=(P(None, ("groups", "batch"), None, "mp"), P(("groups", "batch"), "mp")),
        check_vma=False,
    )
```

```python
import functools

import jax
import jax.numpy as jnp
from jax import lax
from jax.experimental import pallas as pl
from jax.experimental.pallas import tpu as pltpu
from jax.sharding import PartitionSpec as P

HEAD_DIM = 64
REACH = 3
MESH = pl.DeviceIdType.MESH
DISTANCES = [3, -3, 2, -2, 1, -1]
ROWS = 16
WHOLE = 6
SPLIT = 12
JOINED = 14
AHEAD = 5
LAG = 3
BEHIND = 3
TURNED = 3
WAIT = 4
DEFER = 1
LINES = 11


def attend(query, keys, values, length, own):
    slots, width = keys.shape
    heads = width // HEAD_DIM
    rows = -(-heads // 16) * 16
    row = lax.broadcasted_iota(jnp.int32, (rows, width), 0)
    column = lax.broadcasted_iota(jnp.int32, (rows, width), 1)
    low = row * HEAD_DIM
    mine = (column >= low) & (column < low + HEAD_DIM)
    spread = jnp.where(mine, query.astype(jnp.float32), 0.0)
    factor = HEAD_DIM ** (-0.5)
    scores = (
        lax.dot_general(
            spread.astype(jnp.bfloat16),
            keys,
            (((1,), (1,)), ((), ())),
            preferred_element_type=jnp.float32,
        )
        * factor
    )
    if length is not None:
        usable = lax.broadcasted_iota(jnp.int32, (rows, slots), 1) < length
        scores = jnp.where(usable, scores, -1e30)
    highest = jnp.max(scores, axis=-1, keepdims=True)
    if own is not None:
        new_key, new_value = own
        own_score = jnp.sum(spread * new_key.astype(jnp.float32), axis=-1, keepdims=True) * factor
        highest = jnp.maximum(highest, own_score)
    weight = jnp.exp(scores - highest)
    if length is not None:
        weight = jnp.where(usable, weight, 0.0)
    total = jnp.sum(weight, axis=-1, keepdims=True)
    if own is not None:
        own_weight = jnp.exp(own_score - highest)
        total = total + own_weight
    weight = (weight / total).astype(jnp.bfloat16)
    mixed = jnp.dot(weight, values, preferred_element_type=jnp.float32)
    if own is not None:
        own_weight = (own_weight / total).astype(jnp.bfloat16).astype(jnp.float32)
        mixed = mixed + own_weight * new_value.astype(jnp.float32)
    return jnp.sum(jnp.where(mine, mixed, 0.0), axis=0, keepdims=True)


def kernel(
    count,
    cores,
    cache_len,
    finished,
    new_slot,
    hidden,
    token_qkv,
    self_cache,
    ln_gain,
    ln_bias,
    cross_hbm,
    out_proj_hbm,
    query_proj_hbm,
    moved_cache,
    moved_out,
    cross,
    out_proj,
    query_proj,
    updated,
    parcel,
    arrived,
    mark,
    mark_in,
    line,
    line_in,
    part,
    part_in,
    load_sem,
    cache_sems,
    mark_sems,
    line_sems,
    part_sems,
):
    spans, width = hidden.shape
    slots, local = self_cache.shape[2:]
    me = lax.axis_index("batch")
    core = lax.axis_index("mp")
    loads = [
        pltpu.make_async_copy(source, target, load_sem.at[i])
        for i, (source, target) in enumerate(
            [(out_proj_hbm, out_proj), (query_proj_hbm, query_proj), (cross_hbm, cross)]
        )
    ]
    for load in loads:
        load.start()

    barrier = pltpu.get_barrier_semaphore()
    targets = [lax.rem(me + distance + count, count) for distance in DISTANCES]
    for target in targets:
        pl.semaphore_signal(barrier, inc=1, device_id={"batch": target}, device_id_type=MESH)
    others = [lax.rem(core + k, cores) for k in range(1, cores)]
    for other in others:
        pl.semaphore_signal(barrier, inc=1, device_id={"mp": other}, device_id_type=MESH)

    half = count // 2
    alive, offset, place = [], [], []
    for c in range(spans):
        slot = new_slot[c]
        owner = lax.div(slot, spans)
        offset.append(lax.rem(owner - me + half + count, count) - half)
        place.append(lax.rem(slot, spans))
        alive.append(jnp.where(finished[c] == 0, 1, 0))

    position = lax.broadcasted_iota(jnp.int32, (slots, local), 0)
    for c in range(spans):
        length = cache_len[c]
        older = jnp.where(position < length * alive[c], 1.0, 0.0).astype(jnp.bfloat16)
        fresh = jnp.where(position == jnp.where(alive[c] == 1, length, -1), 1.0, 0.0).astype(
            jnp.bfloat16
        )
        for a in range(2):
            updated[a, c] = self_cache[a, c] * older + token_qkv[1 + a, c : c + 1, :] * fresh

    def flag(value, shape):
        return jnp.full(shape, jnp.where(value, 1.0, 0.0), jnp.float32).astype(jnp.bfloat16)

    marker_row = lax.broadcasted_iota(jnp.int32, mark.shape[1:], 0)
    for i, distance in enumerate(DISTANCES):
        marker = jnp.zeros(mark.shape[1:], jnp.float32)
        for c in range(spans):
            at = jnp.where(offset[c] == distance, place[c], -1)
            marker = jnp.where(marker_row == at, 1.0, marker)
        mark[i] = marker.astype(jnp.bfloat16)

    def send(source, target, sems, i, distance):
        return pltpu.make_async_remote_copy(
            src_ref=source,
            dst_ref=target,
            send_sem=sems.at[0, i],
            recv_sem=sems.at[1, i],
            device_id={"batch": targets[i]},
            device_id_type=MESH,
        )

    pl.semaphore_wait(barrier, len(targets) + len(others))
    mark_copies, cache_copies = [], []
    for i, distance in enumerate(DISTANCES):
        copy = send(mark.at[i], mark_in.at[i], mark_sems, i, distance)
        copy.start()
        mark_copies.append(copy)
    for i, distance in enumerate(DISTANCES):
        for a in range(2):
            total = updated[a, 0] * flag(offset[0] == distance, (1, local))
            for c in range(1, spans):
                total = total + updated[a, c] * flag(offset[c] == distance, (1, local))
            parcel[i, a] = total
        copy = send(parcel.at[i], arrived.at[i], cache_sems, i, distance)
        copy.start()
        cache_copies.append(copy)

    for l in range(spans):
        for a in range(2):
            total = updated[a, 0] * flag((offset[0] == 0) & (place[0] == l), (1, local))
            for c in range(1, spans):
                keep = flag((offset[c] == 0) & (place[c] == l), (1, local))
                total = total + updated[a, c] * keep
            moved_cache[a, l] = total

    contexts = []
    for c in range(spans):
        query, key, value = (token_qkv[k, c : c + 1, :] for k in range(3))
        contexts.append(
            attend(query, self_cache[0, c], self_cache[1, c], cache_len[c], (key, value))
        )
    pad = part.shape[0] - spans
    context = jnp.concatenate(contexts + [jnp.zeros((pad, local), jnp.float32)], 0)
    context = context.astype(jnp.bfloat16)
    loads[0].wait()
    part[...] = jnp.dot(context, out_proj[...], preferred_element_type=jnp.float32)
    part_copies = []
    for k, other in enumerate(others):
        copy = pltpu.make_async_remote_copy(
            src_ref=part,
            dst_ref=part_in.at[k],
            send_sem=part_sems.at[0, k],
            recv_sem=part_sems.at[1, k],
            device_id={"mp": other},
            device_id_type=MESH,
        )
        copy.start()
        part_copies.append(copy)
    loads[1].wait()
    loads[2].wait()
    for copy in part_copies:
        copy.wait()
    summed = part[...]
    for k in range(len(others)):
        summed = summed + part_in[k]
    resid = hidden[...].astype(jnp.float32) + summed[:spans]
    centre = jnp.mean(resid, axis=-1, keepdims=True)
    spread = jnp.mean((resid - centre) ** 2, axis=-1, keepdims=True)
    gain = ln_gain[...].reshape(1, width)
    bias = ln_bias[...].reshape(1, width)
    normed = (resid - centre) * lax.rsqrt(spread + 1e-05) * gain + bias
    normed = jnp.concatenate([normed, jnp.zeros((pad, width), jnp.float32)], 0)
    query = jnp.dot(
        normed.astype(jnp.bfloat16), query_proj[...], preferred_element_type=jnp.float32
    ).astype(jnp.bfloat16).astype(jnp.float32)
    decoded = []
    for c in range(spans):
        mixed = attend(query[c : c + 1], cross[0, c], cross[1, c], None, None)
        decoded.append(mixed * jnp.where(alive[c] == 1, 1.0, 0.0))

    line_copies = []
    blank = jnp.zeros((line.shape[1] - 1, local), jnp.float32)
    for i, distance in enumerate(DISTANCES):
        row = jnp.zeros((1, local), jnp.float32)
        for c in range(spans):
            row = row + decoded[c] * jnp.where(offset[c] == distance, 1.0, 0.0)
        line[i] = jnp.concatenate([row, blank], 0).astype(jnp.bfloat16)
        copy = send(line.at[i], line_in.at[i], line_sems, i, distance)
        copy.start()
        line_copies.append(copy)

    rows = []
    for l in range(spans):
        row = jnp.zeros((1, local), jnp.float32)
        for c in range(spans):
            keep = (offset[c] == 0) & (place[c] == l)
            row = row + decoded[c] * jnp.where(keep, 1.0, 0.0)
        rows.append(row)
    for i in range(len(DISTANCES)):
        mark_copies[i].wait()
        cache_copies[i].wait()
        for l in range(spans):
            taken = mark_in[i, l : l + 1, :]
            for a in range(2):
                moved_cache[a, l] = moved_cache[a, l] + arrived[i, a] * taken
    for i in range(len(DISTANCES)):
        line_copies[i].wait()
        for l in range(spans):
            taken = mark_in[i, l : l + 1, :].astype(jnp.float32)
            rows[l] = rows[l] + line_in[i, 0:1, :].astype(jnp.float32) * taken
    moved_out[...] = jnp.concatenate(rows, 0).astype(jnp.bfloat16)


def relay_kernel(
    count,
    cores,
    cache_len_hbm,
    finished_hbm,
    new_slot_hbm,
    hidden_hbm,
    token_qkv_hbm,
    cache_hbm,
    ln_gain_hbm,
    ln_bias_hbm,
    cross_hbm,
    out_proj_hbm,
    query_proj_hbm,
    moved_cache,
    moved_out,
    cache_len,
    finished,
    new_slot,
    hidden,
    token_qkv,
    ln_gain,
    ln_bias,
    self_cache,
    cross,
    out_proj,
    query_proj,
    own,
    raw_in,
    cross_out,
    cross_in,
    kept,
    final_out,
    final_in,
    final_far,
    pick,
    label,
    label_in,
    line,
    line_in,
    line_kept,
    line_out,
    line_cross,
    line_last,
    line_final,
    part,
    part_in,
    load_sem,
    send_sems,
    mate_recv,
    second_recv,
    whole_recv,
    cross_recv,
    final_recv,
    far_recv,
    half_recv,
    label_send,
    label_recv,
    line_send,
    line_recv,
    line_hops,
    part_sems,
    core_sem,
):
    spans, width = hidden.shape
    slots, local = self_cache.shape[2:]
    steps, _, rows_per, _ = own.shape
    per = steps // 2
    me = lax.axis_index("batch")
    core = lax.axis_index("mp")
    level, column = lax.div(me, 2), lax.rem(me, 2)
    inner = (level == 1) | (level == REACH - 1)
    outer = jnp.logical_not(inner)
    barrier = pltpu.get_barrier_semaphore()

    def greet(where):
        pl.semaphore_signal(barrier, inc=1, device_id=where, device_id_type=MESH)

    mate_level = jnp.where(level == 0, 1, jnp.where(level == 1, 0, jnp.where(level == 2, 3, 2)))
    mate = mate_level * 2 + column
    mate_aside = mate_level * 2 + 1 - column
    aside = level * 2 + 1 - column
    across = (REACH - level) * 2 + column
    beyond = (REACH - mate_level) * 2 + column
    others = [lax.rem(core + k, cores) for k in range(1, cores)]
    for node in (mate, aside):
        greet({"batch": node})

    @pl.when(inner)
    def _():
        greet({"batch": across})

    @pl.when(core == 0)
    def _():
        greet({"mp": 1})

    loads = [
        pltpu.make_async_copy(source, target, load_sem.at[i])
        for i, (source, target) in enumerate(
            [
                (out_proj_hbm, out_proj),
                (query_proj_hbm, query_proj),
                (cross_hbm, cross),
                (cache_hbm.at[0], self_cache.at[0]),
                (cache_hbm.at[1], self_cache.at[1]),
                (cache_len_hbm, cache_len),
                (finished_hbm, finished),
                (new_slot_hbm, new_slot),
                (hidden_hbm, hidden),
                (token_qkv_hbm, token_qkv),
                (ln_gain_hbm, ln_gain),
                (ln_bias_hbm, ln_bias),
            ]
        )
    ]
    for i in [3, *range(5, len(loads)), 4, 0, 1, 2]:
        loads[i].start()
    for load in loads[5:]:
        load.wait()

    alive = [jnp.where(finished[c] == 0, 1, 0) for c in range(spans)]

    def to(node, source, target, sent, received):
        return pltpu.make_async_remote_copy(
            src_ref=source,
            dst_ref=target,
            send_sem=sent,
            recv_sem=received,
            device_id={"batch": node},
            device_id_type=MESH,
        )

    own_send, aside_send, pass_send, far_send, cross_send, joined_send, final_send = (
        send_sems.at[i] for i in range(7)
    )

    def mate_copy(k):
        return to(mate, own.at[k], raw_in.at[0, k], own_send, mate_recv.at[k])

    def across_copy(k):
        return to(across, own.at[k], raw_in.at[1, k], own_send, whole_recv.at[0])

    def aside_copy(k):
        return to(aside, own.at[k], raw_in.at[2, k], aside_send, second_recv.at[k])

    def pass_copy(k):
        return to(across, raw_in.at[0, k], raw_in.at[2, k], pass_send, second_recv.at[k])

    def outer_pass_copy(k):
        return to(mate, raw_in.at[2, k], raw_in.at[1, k], pass_send, mate_recv.at[k])

    def arrive(blocks, sem):
        pltpu.make_async_copy(blocks, blocks, sem).wait()

    def far_copy(k):
        return to(
            beyond,
            cross_out.at[k, pl.ds(spans, spans)],
            final_far.at[k],
            far_send,
            far_recv.at[k - JOINED + 1],
        )

    def half_copy(k):
        return to(
            across,
            cross_out.at[k, pl.ds(spans, spans)],
            cross_in.at[k, pl.ds(spans, spans)],
            far_send,
            half_recv.at[k - SPLIT],
        )

    def turn_copy(k):
        return to(
            mate,
            cross_out.at[k, pl.ds(spans, spans)],
            raw_in.at[2, k],
            far_send,
            second_recv.at[k],
        )

    def turned_copy(k):
        return to(aside, raw_in.at[2, k], final_far.at[k], far_send, far_recv.at[0])

    def cross_copy(k, node, count, sent, slot=None):
        return to(
            node,
            cross_out.at[k, pl.ds(0, count)],
            cross_in.at[k, pl.ds(0, count)],
            sent,
            cross_recv.at[k - TURNED + 1 if slot is None else slot],
        )

    def final_copy(k, slot):
        return to(mate, final_out.at[k], final_in.at[k], final_send, final_recv.at[slot])

    def last_copy(k):
        return final_copy(k, k - SPLIT + 2)

    def label_copy(node, lane, way):
        return to(node, label, label_in.at[way], label_send.at[0], label_recv.at[way])

    def line_copy(node, lane, way):
        return to(node, line, line_in.at[way], line_send.at[0], line_recv.at[way])

    def label_pass_copy(node, here, there):
        return to(node, label_in.at[here], label_in.at[there], label_send.at[0], label_recv.at[there])

    def line_pass_copy():
        return to(mate, line_in.at[1], line_in.at[1], line_send.at[0], line_recv.at[1])

    def line_cross_copy():
        return to(across, line_out, line_cross, line_hops.at[0], line_hops.at[1])

    def line_final_copy():
        return to(mate, line_last, line_final, line_hops.at[2], line_hops.at[3])

    label_row = lax.broadcasted_iota(jnp.int32, label.shape, 0)
    labels = jnp.zeros(label.shape, jnp.int32)
    for c in range(spans):
        labels = jnp.where(label_row == c, new_slot[c], labels)
    label[...] = labels.astype(jnp.float32)

    @pl.when(inner)
    def _():
        pl.semaphore_wait(barrier, 3 + core)

    @pl.when(outer)
    def _():
        pl.semaphore_wait(barrier, 2 + core)

    @pl.when(core == 1)
    def _():
        pl.semaphore_signal(core_sem, inc=1, device_id={"mp": 0}, device_id_type=MESH)

    position = lax.broadcasted_iota(jnp.int32, (rows_per, local), 0)
    ends = [cache_len[c] * alive[c] for c in range(spans)]
    fresh_at = [jnp.where(alive[c] == 1, cache_len[c], -1) for c in range(spans)]

    def grow(k, _):
        a, r = lax.div(k, per), lax.rem(k, per)
        start = pl.multiple_of(r * rows_per, rows_per)
        at = position + start
        for c in range(spans):
            older = jnp.where(at < ends[c], 1.0, 0.0).astype(jnp.bfloat16)
            fresh = jnp.where(at == fresh_at[c], 1.0, 0.0).astype(jnp.bfloat16)
            new = jnp.where(a == 0, token_qkv[1, c : c + 1, :].astype(jnp.float32),
                            token_qkv[2, c : c + 1, :].astype(jnp.float32)).astype(jnp.bfloat16)
            own[k, c] = self_cache[a, c, pl.ds(start, rows_per), :] * older + new * fresh

        return 0

    def pass_whole(k, _):
        grow(k, 0)

        @pl.when(outer)
        def _():
            mate_copy(k).start()

        @pl.when(inner)
        def _():
            across_copy(k).start()

        return 0

    def pass_on(k, _):
        aside_copy(k).start()
        return 0

    @pl.when(outer)
    def _():
        label_copy(mate, 0, 0).start()
        label_copy(aside, 1, 1).start()

    @pl.when(inner)
    def _():
        label_copy(aside, 0, 2).start()
        label_copy(across, 1, 3).start()

    loads[3].wait()
    lax.fori_loop(0, WHOLE, pass_whole, 0)
    lax.fori_loop(WHOLE, per, grow, 0)
    loads[4].wait()
    lax.fori_loop(per, steps, grow, 0)

    @pl.when(inner)
    def _():
        lax.fori_loop(WHOLE, WHOLE + AHEAD, pass_on, 0)

    @pl.when(outer)
    def _():
        lax.fori_loop(WHOLE, steps, pass_on, 0)


    def self_part():
        contexts = []
        for c in range(spans):
            query, key, value = (token_qkv[k, c : c + 1, :] for k in range(3))
            contexts.append(
                attend(query, self_cache[0, c], self_cache[1, c], cache_len[c], (key, value))
            )
        context = jnp.concatenate(contexts + [jnp.zeros((pad, local), jnp.float32)], 0)
        context = context.astype(jnp.bfloat16)
        loads[0].wait()
        part[...] = jnp.dot(context, out_proj[...], preferred_element_type=jnp.float32)

    def part_copy(k):
        return pltpu.make_async_remote_copy(
            src_ref=part,
            dst_ref=part_in.at[k],
            send_sem=part_sems.at[0, k],
            recv_sem=part_sems.at[1, k],
            device_id={"mp": others[k]},
            device_id_type=MESH,
        )

    pad = part.shape[0] - spans
    self_part()

    @pl.when(core == 0)
    def _():
        pl.semaphore_wait(core_sem, 1)

    for k in range(len(others)):
        part_copy(k).start()

    @pl.when(outer)
    def _():
        label_copy(mate, 0, 1).wait_recv()
        label_pass_copy(mate, 1, 1).start()

    @pl.when(inner)
    def _():
        label_copy(mate, 0, 0).wait_recv()
        label_pass_copy(across, 0, 4).start()

    def choose(p, ways, nodes):
        for s, source in enumerate([label] + [label_in.at[way] for way in ways]):
            for c in range(spans):
                held = jnp.broadcast_to(source[c : c + 1, 0:1], (rows_per, local))
                for d, node in enumerate(nodes):
                    for l in range(spans):
                        wanted = jnp.full((rows_per, local), node * spans + l, jnp.int32)
                        pick[p, s * spans + c, d * spans + l] = jnp.where(
                            held == wanted.astype(jnp.float32), 1.0, 0.0
                        ).astype(jnp.bfloat16)

    def gather(k, p, cross_done, final_done):
        blocks = [own[k, c] for c in range(spans)]
        for way in range(3):
            blocks += [raw_in[way, k, c] for c in range(spans)]

        def gathered(d):
            total = blocks[0] * pick[p, 0, d]
            for s in range(1, len(blocks)):
                total = total + blocks[s] * pick[p, s, d]
            return total

        for d in range(spans, 2 * spans):
            cross_out[k, d] = gathered(2 * spans + d)
        for d in range(spans):
            cross_out[k, d] = gathered(2 * spans + d)
        cross_done()
        for d in range(spans):
            final_out[k, d] = gathered(spans + d)
        final_done()
        for d in range(spans):
            kept[k, d] = gathered(d)

    def gathered_in(k):
        arrive(raw_in.at[pl.ds(0, 2), k], mate_recv.at[k])
        aside_copy(k).wait_recv()

    def merge_whole(k, _):
        pass_copy(k).wait_recv()

        def cross_done():
            turn_copy(k).start()
            cross_copy(k, aside, spans, cross_send, 0).start()

        gather(k, 1, cross_done, lambda: final_copy(k, 0).start())
        return 0

    def merge_whole_joined(k, _):
        pass_copy(k).wait_recv()
        gather(k, 1, lambda: cross_copy(k, aside, 2 * spans, joined_send).start(), lambda: None)
        return 0

    def whole(k):
        return (merge_whole if k < TURNED else merge_whole_joined, k)

    def merge_joined(k, _):
        gathered_in(k)
        gather(k, 0, lambda: cross_copy(k, across, 2 * spans, joined_send).start(), lambda: None)
        return 0

    def merge_half(k, _):
        gathered_in(k)
        gather(k, 0, lambda: half_copy(k).start(), lambda: None)
        return 0

    def merge(k, _):
        gathered_in(k)
        gather(k, 0, lambda: far_copy(k).start(), lambda: last_copy(k).start())
        return 0

    def send_rest(k, _):
        cross_copy(k, across, spans, cross_send).start()
        return 0

    def settle(k):
        a, r = lax.div(k, per), lax.rem(k, per)
        start = pl.multiple_of(r * rows_per, rows_per)
        for l in range(spans):
            moved_cache[a, l, pl.ds(start, rows_per), :] = kept[k, l] + cross_in[k, l]

    def finish(k, _):
        cross_copy(k, across, spans, cross_send).wait_recv()
        settle(k)
        return 0

    def hand_on(k, copy):
        for l in range(spans):
            final_out[k, l] = final_out[k, l] + cross_in[k, spans + l]
        copy.start()

    def finish_joined(k, _):
        cross_copy(k, across, 2 * spans, joined_send).wait_recv()
        hand_on(k, final_copy(k, 1))
        settle(k)
        return 0

    def finish_half(k, _):
        half_copy(k).wait_recv()
        hand_on(k, last_copy(k))
        return 0

    loads[1].wait()
    loads[2].wait()
    for k in range(len(others)):
        part_copy(k).wait()
    summed = part[...]
    for k in range(len(others)):
        summed = summed + part_in[k]
    resid = hidden[...].astype(jnp.float32) + summed[:spans]
    centre = jnp.mean(resid, axis=-1, keepdims=True)
    spread = jnp.mean((resid - centre) ** 2, axis=-1, keepdims=True)
    gain = ln_gain[...].reshape(1, width)
    bias = ln_bias[...].reshape(1, width)
    normed = (resid - centre) * lax.rsqrt(spread + 1e-05) * gain + bias
    normed = jnp.concatenate([normed, jnp.zeros((pad, width), jnp.float32)], 0)
    query = jnp.dot(
        normed.astype(jnp.bfloat16), query_proj[...], preferred_element_type=jnp.float32
    ).astype(jnp.bfloat16).astype(jnp.float32)

    decoded = []
    for c in range(spans):
        mixed = attend(query[c : c + 1], cross[0, c], cross[1, c], None, None)
        decoded.append(mixed * jnp.where(alive[c] == 1, 1.0, 0.0))

    line[...] = jnp.concatenate(decoded, 0).astype(jnp.bfloat16)

    @pl.when(outer)
    def _():
        line_copy(mate, 0, 0).start()
        line_copy(aside, 1, 1).start()

    @pl.when(inner)
    def _():
        line_copy(aside, 0, 2).start()

    def turn(k, _):
        turn_copy(k).wait_recv()
        turned_copy(k).start()
        return 0

    def outer_forward(k, _):
        mate_copy(k).start()
        aside_copy(k).wait_recv()
        outer_pass_copy(k).start()
        return 0

    @pl.when(outer)
    def _():
        lax.fori_loop(WHOLE, WHOLE + AHEAD, outer_forward, 0)
        line_copy(mate, 0, 1).wait_recv()
        line_pass_copy().start()
        lax.fori_loop(WHOLE + AHEAD, steps, outer_forward, 0)
        lax.fori_loop(0, TURNED, turn, 0)

    @pl.when(inner)
    def _():
        lax.fori_loop(WHOLE + AHEAD, steps, pass_on, 0)

    def forward(k, _):
        mate_copy(k).wait_recv()
        pass_copy(k).start()
        return 0

    def gather_lines():
        for way in range(3):
            line_copy(mate, 0, way).wait_recv()
        blocks = []
        for held in [line] + [line_in.at[way] for way in range(3)]:
            blocks += [held[c : c + 1, :].astype(jnp.float32) for c in range(spans)]
        rows = []
        for d in range(4 * spans):
            total = blocks[0] * pick[0, 0, d, 0:1, :].astype(jnp.float32)
            for s in range(1, len(blocks)):
                total = total + blocks[s] * pick[0, s, d, 0:1, :].astype(jnp.float32)
            rows.append(total)
        line_out[...] = jnp.concatenate(rows[2 * spans :], 0).astype(jnp.bfloat16)
        line_cross_copy().start()
        line_kept[...] = jnp.concatenate(rows[: 2 * spans], 0)

    def send_lines():
        line_cross_copy().wait_recv()
        total = line_kept[...] + line_cross[...].astype(jnp.float32)
        line_last[...] = total[spans:].astype(jnp.bfloat16)
        line_final_copy().start()
        moved_out[...] = total[:spans].astype(jnp.bfloat16)

    def run(groups):
        while groups:
            ops, starts = [op for op, _ in groups[0]], [k for _, k in groups[0]]
            size = 1
            while size < len(groups) and groups[size] == [(op, k + size) for op, k in groups[0]]:
                size += 1

            def step(i, _, ops=ops, starts=starts):
                for op, k in zip(ops, starts):
                    op(i + k, 0)
                return 0

            if size > 1:
                lax.fori_loop(0, size, step, 0)
            else:
                step(0, 0)
            groups = groups[size:]

    def groups(low, high):
        found = []
        for k in range(low, high):
            group = []
            if k < steps:
                group.append(
                    (merge_joined if k < SPLIT else merge_half if k < JOINED else merge, k)
                )
            if SPLIT <= k - DEFER < steps and k < steps:
                group.append((send_rest, k - DEFER))
            if k == steps - 1:
                group += [(send_rest, j) for j in range(steps - DEFER, steps)]
            if WHOLE <= k - LAG < JOINED:
                group.append((finish_joined if k - LAG < SPLIT else finish_half, k - LAG))
            if k < WHOLE + BEHIND:
                group.append(whole(k - BEHIND))
            if TURNED <= k - WHOLE - WAIT + TURNED < WHOLE:
                group.append((finish_joined, k - WHOLE - WAIT + TURNED))
            found.append(group)
        return found

    @pl.when(inner)
    def _():
        lax.fori_loop(0, WHOLE, forward, 0)
        for way in range(1, 5):
            label_copy(mate, 0, way).wait_recv()
        choose(1, (0, 3, 4), (me, mate, aside, mate_aside))
        choose(0, (0, 1, 2), (me, mate, across, beyond))
        arrive(raw_in.at[1, pl.ds(0, WHOLE)], whole_recv.at[0])
        run([[whole(k)] for k in range(WHOLE - BEHIND)])
        run(groups(WHOLE, LINES))
        gather_lines()
        run(groups(LINES, steps + LAG))
        send_lines()

    def place(k, value):
        a, r = lax.div(k, per), lax.rem(k, per)
        start = pl.multiple_of(r * rows_per, rows_per)
        for l in range(spans):
            moved_cache[a, l, pl.ds(start, rows_per), :] = value(l)

    def land_turned(k, _):
        place(k, lambda l: final_in[k, l] + final_far[k, l])
        return 0

    def land_ready(k, _):
        place(k, lambda l: final_in[k, l])
        return 0

    def land_joined(k, _):
        last_copy(k).wait_recv()
        return land_ready(k, 0)

    def land(k, _):
        last_copy(k).wait_recv()
        far_copy(k).wait_recv()
        return land_turned(k, 0)

    def settle_turned(k, _):
        settle(k)
        return 0

    rest = steps - WHOLE

    @pl.when(inner)
    def _():
        arrive(kept.at[pl.ds(0, TURNED)], cross_recv.at[0])
        lax.fori_loop(0, TURNED, settle_turned, 0)
        lax.fori_loop(SPLIT, steps, finish, 0)
        arrive(label_in.at[pl.ds(0, 3)], label_send.at[0])
        line_copy(aside, 0, 2).wait_send()
        line_cross_copy().wait_send()
        line_final_copy().wait_send()
        arrive(own.at[pl.ds(0, WHOLE)], own_send)
        arrive(own.at[pl.ds(0, rest)], aside_send)
        arrive(own.at[pl.ds(0, WHOLE)], pass_send)
        arrive(own.at[pl.ds(0, TURNED + steps - SPLIT)], far_send)
        arrive(own.at[pl.ds(0, TURNED + steps - SPLIT)], cross_send)
        arrive(cross_out.at[pl.ds(0, SPLIT - TURNED)], joined_send)
        arrive(own, final_send)

    @pl.when(outer)
    def _():
        arrive(final_in.at[pl.ds(0, TURNED)], final_recv.at[0])
        arrive(final_far.at[pl.ds(0, TURNED)], far_recv.at[0])
        lax.fori_loop(0, TURNED, land_turned, 0)
        arrive(final_in.at[pl.ds(TURNED, SPLIT - TURNED)], final_recv.at[1])
        lax.fori_loop(TURNED, SPLIT, land_ready, 0)
        lax.fori_loop(SPLIT, JOINED, land_joined, 0)
        lax.fori_loop(JOINED, steps, land, 0)
        arrive(label_in.at[pl.ds(0, 3)], label_send.at[0])
        arrive(line_in, line_send.at[0])
        line_final_copy().wait_recv()
        moved_out[...] = line_final[...]
        arrive(own, own_send)
        arrive(own.at[pl.ds(0, rest)], aside_send)
        arrive(own.at[pl.ds(0, rest)], pass_send)
        arrive(own.at[pl.ds(0, TURNED)], far_send)


def store_kernel(cache, out, cache_hbm, out_hbm, sems):
    copies = [pltpu.make_async_copy(out, out_hbm, sems.at[0])] + [
        pltpu.make_async_copy(cache.at[a], cache_hbm.at[a], sems.at[1 + a]) for a in range(2)
    ]
    for copy in copies:
        copy.start()
    for copy in copies:
        copy.wait()


def body(
    hidden,
    token_qkv,
    self_cache,
    cross_kv,
    cache_len,
    finished,
    new_slot,
    out_proj,
    ln_gain,
    ln_bias,
    query_proj,
):
    count, cores = lax.axis_size("batch"), lax.axis_size("mp")
    spans, width = hidden.shape
    slots, local = self_cache.shape[2:]
    moves = len(DISTANCES)
    smem = pl.BlockSpec(memory_space=pltpu.SMEM)
    vmem = pl.BlockSpec(memory_space=pltpu.VMEM)
    away = pl.BlockSpec(memory_space=pl.ANY)
    bf16, f32 = jnp.bfloat16, jnp.float32
    operands = (
        cache_len,
        finished,
        new_slot,
        hidden,
        token_qkv,
        self_cache,
        ln_gain,
        ln_bias,
        cross_kv,
        out_proj,
        query_proj,
    )
    parcels = pltpu.VMEM((moves, 2, slots, local), bf16)
    tiles = pltpu.VMEM((moves, 16, local), bf16)
    dma = pltpu.SemaphoreType.DMA
    inputs = [pltpu.VMEM(array.shape, bf16) for array in (cross_kv, out_proj, query_proj)]
    parts = [pltpu.VMEM((8, width), f32), pltpu.VMEM((cores - 1, 8, width), f32)]
    steps = 2 * slots // ROWS
    if count == 2 * (REACH + 1) and cores == 2:
        function, specs = relay_kernel, [away] * 8

        def blocks(*lead):
            return pltpu.VMEM(lead + (ROWS, local), bf16)

        small = [pltpu.SMEM((spans,), jnp.int32)] * 3 + [
            pltpu.VMEM(hidden.shape, bf16),
            pltpu.VMEM(token_qkv.shape, bf16),
            pltpu.VMEM(ln_gain.shape, f32),
            pltpu.VMEM(ln_bias.shape, f32),
        ]
        scratch = small + [pltpu.VMEM(self_cache.shape, bf16)] + inputs + [
            blocks(steps, spans),
            blocks(3, steps, spans),
            blocks(steps, 2 * spans),
            blocks(steps, 2 * spans),
            blocks(steps, spans),
            blocks(steps, spans),
            blocks(steps, spans),
            blocks(steps, spans),
            blocks(2, 4 * spans, 4 * spans),
            pltpu.VMEM((8, 128), f32),
            pltpu.VMEM((5, 8, 128), f32),
            pltpu.VMEM((spans, local), bf16),
            pltpu.VMEM((3, spans, local), bf16),
            pltpu.VMEM((2 * spans, local), f32),
            pltpu.VMEM((2 * spans, local), bf16),
            pltpu.VMEM((2 * spans, local), bf16),
            pltpu.VMEM((spans, local), bf16),
            pltpu.VMEM((spans, local), bf16),
            *parts,
            dma((12,)),
            dma((7,)),
            dma((steps,)),
            dma((steps,)),
            dma((1,)),
            dma((steps - TURNED + 1,)),
            dma((steps - SPLIT + 2,)),
            dma((steps - JOINED + 1,)),
            dma((JOINED - SPLIT,)),
            dma((1,)),
            dma((5,)),
            dma((1,)),
            dma((3,)),
            dma((4,)),
            dma((2, cores - 1)),
            pltpu.SemaphoreType.REGULAR,
        ]
    else:
        function, specs = kernel, [smem] * 3 + [vmem] * 5
        scratch = inputs + [
            pltpu.VMEM(self_cache.shape, bf16),
            parcels,
            parcels,
            tiles,
            tiles,
            tiles,
            tiles,
            *parts,
            dma((3,)),
            dma((2, moves)),
            dma((2, moves)),
            dma((2, moves)),
            dma((2, cores - 1)),
        ]
    moved = pl.pallas_call(
        functools.partial(function, count, cores),
        out_shape=(
            pltpu.VMEM(self_cache.shape, bf16),
            pltpu.VMEM((spans, local), bf16),
        ),
        in_specs=specs + [away] * 3,
        out_specs=(vmem, vmem),
        scratch_shapes=scratch,
        compiler_params=pltpu.CompilerParams(collective_id=0, has_side_effects=True),
    )(*operands)
    return pl.pallas_call(
        store_kernel,
        out_shape=tuple(jax.ShapeDtypeStruct(array.shape, bf16) for array in moved),
        in_specs=[vmem, vmem],
        out_specs=(away, away),
        scratch_shapes=[dma((3,))],
    )(*(pltpu.with_memory_space_constraint(a, pltpu.VMEM) for a in moved))


def solution(mesh):
    placed = (
        P(("groups", "batch"), None),
        P(None, ("groups", "batch"), "mp"),
        P(None, ("groups", "batch"), None, "mp"),
        P(None, ("groups", "batch"), None, "mp"),
        P(("groups", "batch")),
        P(("groups", "batch")),
        P(("groups", "batch")),
        P("mp", None),
        P(),
        P(),
        P(None, "mp"),
    )
    return jax.shard_map(
        body,
        mesh=mesh,
        in_specs=placed,
        out_specs=(P(None, ("groups", "batch"), None, "mp"), P(("groups", "batch"), "mp")),
        check_vma=False,
    )
```

```python
import functools

import jax
import jax.numpy as jnp
from jax import lax
from jax.experimental import pallas as pl
from jax.experimental.pallas import tpu as pltpu
from jax.sharding import PartitionSpec as P

HEAD_DIM = 64
REACH = 3
MESH = pl.DeviceIdType.MESH
DISTANCES = [3, -3, 2, -2, 1, -1]
ROWS = 16
WHOLE = 7
SPLIT = 12
JOINED = 14
AHEAD = 5
LAG = 3
BEHIND = 3
TURNED = 4
WAIT = 4
DEFER = 1
LINES = 12


def attend(query, keys, values, length, own):
    slots, width = keys.shape
    heads = width // HEAD_DIM
    rows = -(-heads // 16) * 16
    row = lax.broadcasted_iota(jnp.int32, (rows, width), 0)
    column = lax.broadcasted_iota(jnp.int32, (rows, width), 1)
    low = row * HEAD_DIM
    mine = (column >= low) & (column < low + HEAD_DIM)
    spread = jnp.where(mine, query.astype(jnp.float32), 0.0)
    factor = HEAD_DIM ** (-0.5)
    scores = (
        lax.dot_general(
            spread.astype(jnp.bfloat16),
            keys,
            (((1,), (1,)), ((), ())),
            preferred_element_type=jnp.float32,
        )
        * factor
    )
    if length is not None:
        usable = lax.broadcasted_iota(jnp.int32, (rows, slots), 1) < length
        scores = jnp.where(usable, scores, -1e30)
    highest = jnp.max(scores, axis=-1, keepdims=True)
    if own is not None:
        new_key, new_value = own
        own_score = jnp.sum(spread * new_key.astype(jnp.float32), axis=-1, keepdims=True) * factor
        highest = jnp.maximum(highest, own_score)
    weight = jnp.exp(scores - highest)
    if length is not None:
        weight = jnp.where(usable, weight, 0.0)
    total = jnp.sum(weight, axis=-1, keepdims=True)
    if own is not None:
        own_weight = jnp.exp(own_score - highest)
        total = total + own_weight
    weight = (weight / total).astype(jnp.bfloat16)
    mixed = jnp.dot(weight, values, preferred_element_type=jnp.float32)
    if own is not None:
        own_weight = (own_weight / total).astype(jnp.bfloat16).astype(jnp.float32)
        mixed = mixed + own_weight * new_value.astype(jnp.float32)
    return jnp.sum(jnp.where(mine, mixed, 0.0), axis=0, keepdims=True)


def kernel(
    count,
    cores,
    cache_len,
    finished,
    new_slot,
    hidden,
    token_qkv,
    self_cache,
    ln_gain,
    ln_bias,
    cross_hbm,
    out_proj_hbm,
    query_proj_hbm,
    moved_cache,
    moved_out,
    cross,
    out_proj,
    query_proj,
    updated,
    parcel,
    arrived,
    mark,
    mark_in,
    line,
    line_in,
    part,
    part_in,
    load_sem,
    cache_sems,
    mark_sems,
    line_sems,
    part_sems,
):
    spans, width = hidden.shape
    slots, local = self_cache.shape[2:]
    me = lax.axis_index("batch")
    core = lax.axis_index("mp")
    loads = [
        pltpu.make_async_copy(source, target, load_sem.at[i])
        for i, (source, target) in enumerate(
            [(out_proj_hbm, out_proj), (query_proj_hbm, query_proj), (cross_hbm, cross)]
        )
    ]
    for load in loads:
        load.start()

    barrier = pltpu.get_barrier_semaphore()
    targets = [lax.rem(me + distance + count, count) for distance in DISTANCES]
    for target in targets:
        pl.semaphore_signal(barrier, inc=1, device_id={"batch": target}, device_id_type=MESH)
    others = [lax.rem(core + k, cores) for k in range(1, cores)]
    for other in others:
        pl.semaphore_signal(barrier, inc=1, device_id={"mp": other}, device_id_type=MESH)

    half = count // 2
    alive, offset, place = [], [], []
    for c in range(spans):
        slot = new_slot[c]
        owner = lax.div(slot, spans)
        offset.append(lax.rem(owner - me + half + count, count) - half)
        place.append(lax.rem(slot, spans))
        alive.append(jnp.where(finished[c] == 0, 1, 0))

    position = lax.broadcasted_iota(jnp.int32, (slots, local), 0)
    for c in range(spans):
        length = cache_len[c]
        older = jnp.where(position < length * alive[c], 1.0, 0.0).astype(jnp.bfloat16)
        fresh = jnp.where(position == jnp.where(alive[c] == 1, length, -1), 1.0, 0.0).astype(
            jnp.bfloat16
        )
        for a in range(2):
            updated[a, c] = self_cache[a, c] * older + token_qkv[1 + a, c : c + 1, :] * fresh

    def flag(value, shape):
        return jnp.full(shape, jnp.where(value, 1.0, 0.0), jnp.float32).astype(jnp.bfloat16)

    marker_row = lax.broadcasted_iota(jnp.int32, mark.shape[1:], 0)
    for i, distance in enumerate(DISTANCES):
        marker = jnp.zeros(mark.shape[1:], jnp.float32)
        for c in range(spans):
            at = jnp.where(offset[c] == distance, place[c], -1)
            marker = jnp.where(marker_row == at, 1.0, marker)
        mark[i] = marker.astype(jnp.bfloat16)

    def send(source, target, sems, i, distance):
        return pltpu.make_async_remote_copy(
            src_ref=source,
            dst_ref=target,
            send_sem=sems.at[0, i],
            recv_sem=sems.at[1, i],
            device_id={"batch": targets[i]},
            device_id_type=MESH,
        )

    pl.semaphore_wait(barrier, len(targets) + len(others))
    mark_copies, cache_copies = [], []
    for i, distance in enumerate(DISTANCES):
        copy = send(mark.at[i], mark_in.at[i], mark_sems, i, distance)
        copy.start()
        mark_copies.append(copy)
    for i, distance in enumerate(DISTANCES):
        for a in range(2):
            total = updated[a, 0] * flag(offset[0] == distance, (1, local))
            for c in range(1, spans):
                total = total + updated[a, c] * flag(offset[c] == distance, (1, local))
            parcel[i, a] = total
        copy = send(parcel.at[i], arrived.at[i], cache_sems, i, distance)
        copy.start()
        cache_copies.append(copy)

    for l in range(spans):
        for a in range(2):
            total = updated[a, 0] * flag((offset[0] == 0) & (place[0] == l), (1, local))
            for c in range(1, spans):
                keep = flag((offset[c] == 0) & (place[c] == l), (1, local))
                total = total + updated[a, c] * keep
            moved_cache[a, l] = total

    contexts = []
    for c in range(spans):
        query, key, value = (token_qkv[k, c : c + 1, :] for k in range(3))
        contexts.append(
            attend(query, self_cache[0, c], self_cache[1, c], cache_len[c], (key, value))
        )
    pad = part.shape[0] - spans
    context = jnp.concatenate(contexts + [jnp.zeros((pad, local), jnp.float32)], 0)
    context = context.astype(jnp.bfloat16)
    loads[0].wait()
    part[...] = jnp.dot(context, out_proj[...], preferred_element_type=jnp.float32)
    part_copies = []
    for k, other in enumerate(others):
        copy = pltpu.make_async_remote_copy(
            src_ref=part,
            dst_ref=part_in.at[k],
            send_sem=part_sems.at[0, k],
            recv_sem=part_sems.at[1, k],
            device_id={"mp": other},
            device_id_type=MESH,
        )
        copy.start()
        part_copies.append(copy)
    loads[1].wait()
    loads[2].wait()
    for copy in part_copies:
        copy.wait()
    summed = part[...]
    for k in range(len(others)):
        summed = summed + part_in[k]
    resid = hidden[...].astype(jnp.float32) + summed[:spans]
    centre = jnp.mean(resid, axis=-1, keepdims=True)
    spread = jnp.mean((resid - centre) ** 2, axis=-1, keepdims=True)
    gain = ln_gain[...].reshape(1, width)
    bias = ln_bias[...].reshape(1, width)
    normed = (resid - centre) * lax.rsqrt(spread + 1e-05) * gain + bias
    normed = jnp.concatenate([normed, jnp.zeros((pad, width), jnp.float32)], 0)
    query = jnp.dot(
        normed.astype(jnp.bfloat16), query_proj[...], preferred_element_type=jnp.float32
    ).astype(jnp.bfloat16).astype(jnp.float32)
    decoded = []
    for c in range(spans):
        mixed = attend(query[c : c + 1], cross[0, c], cross[1, c], None, None)
        decoded.append(mixed * jnp.where(alive[c] == 1, 1.0, 0.0))

    line_copies = []
    blank = jnp.zeros((line.shape[1] - 1, local), jnp.float32)
    for i, distance in enumerate(DISTANCES):
        row = jnp.zeros((1, local), jnp.float32)
        for c in range(spans):
            row = row + decoded[c] * jnp.where(offset[c] == distance, 1.0, 0.0)
        line[i] = jnp.concatenate([row, blank], 0).astype(jnp.bfloat16)
        copy = send(line.at[i], line_in.at[i], line_sems, i, distance)
        copy.start()
        line_copies.append(copy)

    rows = []
    for l in range(spans):
        row = jnp.zeros((1, local), jnp.float32)
        for c in range(spans):
            keep = (offset[c] == 0) & (place[c] == l)
            row = row + decoded[c] * jnp.where(keep, 1.0, 0.0)
        rows.append(row)
    for i in range(len(DISTANCES)):
        mark_copies[i].wait()
        cache_copies[i].wait()
        for l in range(spans):
            taken = mark_in[i, l : l + 1, :]
            for a in range(2):
                moved_cache[a, l] = moved_cache[a, l] + arrived[i, a] * taken
    for i in range(len(DISTANCES)):
        line_copies[i].wait()
        for l in range(spans):
            taken = mark_in[i, l : l + 1, :].astype(jnp.float32)
            rows[l] = rows[l] + line_in[i, 0:1, :].astype(jnp.float32) * taken
    moved_out[...] = jnp.concatenate(rows, 0).astype(jnp.bfloat16)


def relay_kernel(
    count,
    cores,
    cache_len_hbm,
    finished_hbm,
    new_slot_hbm,
    hidden_hbm,
    token_qkv_hbm,
    cache_hbm,
    ln_gain_hbm,
    ln_bias_hbm,
    cross_hbm,
    out_proj_hbm,
    query_proj_hbm,
    moved_cache,
    moved_out,
    cache_len,
    finished,
    new_slot,
    hidden,
    token_qkv,
    ln_gain,
    ln_bias,
    self_cache,
    cross,
    out_proj,
    query_proj,
    own,
    raw_in,
    cross_out,
    cross_in,
    kept,
    final_out,
    final_in,
    final_far,
    pick,
    label,
    label_in,
    line,
    line_in,
    line_kept,
    line_out,
    line_cross,
    line_last,
    line_final,
    part,
    part_in,
    load_sem,
    send_sems,
    mate_recv,
    second_recv,
    whole_recv,
    cross_recv,
    final_recv,
    far_recv,
    half_recv,
    label_send,
    label_recv,
    line_send,
    line_recv,
    line_hops,
    part_sems,
    core_sem,
):
    spans, width = hidden.shape
    slots, local = self_cache.shape[2:]
    steps, _, rows_per, _ = own.shape
    per = steps // 2
    me = lax.axis_index("batch")
    core = lax.axis_index("mp")
    level, column = lax.div(me, 2), lax.rem(me, 2)
    inner = (level == 1) | (level == REACH - 1)
    outer = jnp.logical_not(inner)
    barrier = pltpu.get_barrier_semaphore()

    def greet(where):
        pl.semaphore_signal(barrier, inc=1, device_id=where, device_id_type=MESH)

    mate_level = jnp.where(level == 0, 1, jnp.where(level == 1, 0, jnp.where(level == 2, 3, 2)))
    mate = mate_level * 2 + column
    mate_aside = mate_level * 2 + 1 - column
    aside = level * 2 + 1 - column
    across = (REACH - level) * 2 + column
    beyond = (REACH - mate_level) * 2 + column
    others = [lax.rem(core + k, cores) for k in range(1, cores)]
    for node in (mate, aside):
        greet({"batch": node})

    @pl.when(inner)
    def _():
        greet({"batch": across})

    @pl.when(core == 0)
    def _():
        greet({"mp": 1})

    loads = [
        pltpu.make_async_copy(source, target, load_sem.at[i])
        for i, (source, target) in enumerate(
            [
                (out_proj_hbm, out_proj),
                (query_proj_hbm, query_proj),
                (cross_hbm, cross),
                (cache_hbm.at[0], self_cache.at[0]),
                (cache_hbm.at[1], self_cache.at[1]),
                (cache_len_hbm, cache_len),
                (finished_hbm, finished),
                (new_slot_hbm, new_slot),
                (hidden_hbm, hidden),
                (token_qkv_hbm, token_qkv),
                (ln_gain_hbm, ln_gain),
                (ln_bias_hbm, ln_bias),
            ]
        )
    ]
    for i in [3, *range(5, len(loads)), 4, 0, 1, 2]:
        loads[i].start()
    for load in loads[5:]:
        load.wait()

    alive = [jnp.where(finished[c] == 0, 1, 0) for c in range(spans)]

    def to(node, source, target, sent, received):
        return pltpu.make_async_remote_copy(
            src_ref=source,
            dst_ref=target,
            send_sem=sent,
            recv_sem=received,
            device_id={"batch": node},
            device_id_type=MESH,
        )

    own_send, aside_send, pass_send, far_send, cross_send, joined_send, final_send = (
        send_sems.at[i] for i in range(7)
    )

    def mate_copy(k):
        return to(mate, own.at[k], raw_in.at[0, k], own_send, mate_recv.at[k])

    def across_copy(k):
        return to(across, own.at[k], raw_in.at[1, k], own_send, whole_recv.at[0])

    def aside_copy(k):
        return to(aside, own.at[k], raw_in.at[2, k], aside_send, second_recv.at[k])

    def pass_copy(k):
        return to(across, raw_in.at[0, k], raw_in.at[2, k], pass_send, second_recv.at[k])

    def outer_pass_copy(k):
        return to(mate, raw_in.at[2, k], raw_in.at[1, k], pass_send, mate_recv.at[k])

    def arrive(blocks, sem):
        pltpu.make_async_copy(blocks, blocks, sem).wait()

    def far_copy(k):
        return to(
            beyond,
            cross_out.at[k, pl.ds(spans, spans)],
            final_far.at[k],
            far_send,
            far_recv.at[k - JOINED + 1],
        )

    def half_copy(k):
        return to(
            across,
            cross_out.at[k, pl.ds(spans, spans)],
            cross_in.at[k, pl.ds(spans, spans)],
            far_send,
            half_recv.at[k - SPLIT],
        )

    def turn_copy(k):
        return to(
            mate,
            cross_out.at[k, pl.ds(spans, spans)],
            raw_in.at[2, k],
            far_send,
            second_recv.at[k],
        )

    def turned_copy(k):
        return to(aside, raw_in.at[2, k], final_far.at[k], far_send, far_recv.at[0])

    def cross_copy(k, node, count, sent, slot=None):
        return to(
            node,
            cross_out.at[k, pl.ds(0, count)],
            cross_in.at[k, pl.ds(0, count)],
            sent,
            cross_recv.at[k - TURNED + 1 if slot is None else slot],
        )

    def final_copy(k, slot):
        return to(mate, final_out.at[k], final_in.at[k], final_send, final_recv.at[slot])

    def last_copy(k):
        return final_copy(k, k - SPLIT + 2)

    def label_copy(node, lane, way):
        return to(node, label, label_in.at[way], label_send.at[0], label_recv.at[way])

    def line_copy(node, lane, way):
        return to(node, line, line_in.at[way], line_send.at[0], line_recv.at[way])

    def label_pass_copy(node, here, there):
        return to(node, label_in.at[here], label_in.at[there], label_send.at[0], label_recv.at[there])

    def line_pass_copy():
        return to(mate, line_in.at[1], line_in.at[1], line_send.at[0], line_recv.at[1])

    def line_cross_copy():
        return to(across, line_out, line_cross, line_hops.at[0], line_hops.at[1])

    def line_final_copy():
        return to(mate, line_last, line_final, line_hops.at[2], line_hops.at[3])

    label_row = lax.broadcasted_iota(jnp.int32, label.shape, 0)
    labels = jnp.zeros(label.shape, jnp.int32)
    for c in range(spans):
        labels = jnp.where(label_row == c, new_slot[c], labels)
    label[...] = labels.astype(jnp.float32)

    @pl.when(inner)
    def _():
        pl.semaphore_wait(barrier, 3 + core)

    @pl.when(outer)
    def _():
        pl.semaphore_wait(barrier, 2 + core)

    @pl.when(core == 1)
    def _():
        pl.semaphore_signal(core_sem, inc=1, device_id={"mp": 0}, device_id_type=MESH)

    position = lax.broadcasted_iota(jnp.int32, (rows_per, local), 0)
    ends = [cache_len[c] * alive[c] for c in range(spans)]
    fresh_at = [jnp.where(alive[c] == 1, cache_len[c], -1) for c in range(spans)]

    def grow(k, _):
        a, r = lax.div(k, per), lax.rem(k, per)
        start = pl.multiple_of(r * rows_per, rows_per)
        at = position + start
        for c in range(spans):
            older = jnp.where(at < ends[c], 1.0, 0.0).astype(jnp.bfloat16)
            fresh = jnp.where(at == fresh_at[c], 1.0, 0.0).astype(jnp.bfloat16)
            new = jnp.where(a == 0, token_qkv[1, c : c + 1, :].astype(jnp.float32),
                            token_qkv[2, c : c + 1, :].astype(jnp.float32)).astype(jnp.bfloat16)
            own[k, c] = self_cache[a, c, pl.ds(start, rows_per), :] * older + new * fresh

        return 0

    def pass_whole(k, _):
        grow(k, 0)

        @pl.when(outer)
        def _():
            mate_copy(k).start()

        @pl.when(inner)
        def _():
            across_copy(k).start()

        return 0

    def pass_on(k, _):
        aside_copy(k).start()
        return 0

    @pl.when(outer)
    def _():
        label_copy(mate, 0, 0).start()
        label_copy(aside, 1, 1).start()

    @pl.when(inner)
    def _():
        label_copy(aside, 0, 2).start()
        label_copy(across, 1, 3).start()

    loads[3].wait()
    lax.fori_loop(0, WHOLE, pass_whole, 0)
    lax.fori_loop(WHOLE, per, grow, 0)
    loads[4].wait()
    lax.fori_loop(per, steps, grow, 0)

    @pl.when(inner)
    def _():
        lax.fori_loop(JOINED, steps, pass_on, 0)
        lax.fori_loop(WHOLE, WHOLE + AHEAD, pass_on, 0)

    @pl.when(outer)
    def _():
        lax.fori_loop(WHOLE, steps, pass_on, 0)


    def self_part():
        contexts = []
        for c in range(spans):
            query, key, value = (token_qkv[k, c : c + 1, :] for k in range(3))
            contexts.append(
                attend(query, self_cache[0, c], self_cache[1, c], cache_len[c], (key, value))
            )
        context = jnp.concatenate(contexts + [jnp.zeros((pad, local), jnp.float32)], 0)
        context = context.astype(jnp.bfloat16)
        loads[0].wait()
        part[...] = jnp.dot(context, out_proj[...], preferred_element_type=jnp.float32)

    def part_copy(k):
        return pltpu.make_async_remote_copy(
            src_ref=part,
            dst_ref=part_in.at[k],
            send_sem=part_sems.at[0, k],
            recv_sem=part_sems.at[1, k],
            device_id={"mp": others[k]},
            device_id_type=MESH,
        )

    pad = part.shape[0] - spans
    self_part()

    @pl.when(core == 0)
    def _():
        pl.semaphore_wait(core_sem, 1)

    for k in range(len(others)):
        part_copy(k).start()

    @pl.when(outer)
    def _():
        label_copy(mate, 0, 1).wait_recv()
        label_pass_copy(mate, 1, 1).start()

    @pl.when(inner)
    def _():
        label_copy(mate, 0, 0).wait_recv()
        label_pass_copy(across, 0, 4).start()

    def choose(p, ways, nodes):
        for s, source in enumerate([label] + [label_in.at[way] for way in ways]):
            for d, node in enumerate(nodes):
                choose_one(p, s, source, d, node)

    def choose_one(p, s, source, d, node):
        for c in range(spans):
            held = jnp.broadcast_to(source[c : c + 1, 0:1], (rows_per, local))
            for l in range(spans):
                wanted = jnp.full((rows_per, local), node * spans + l, jnp.int32)
                pick[p, s * spans + c, d * spans + l] = jnp.where(
                    held == wanted.astype(jnp.float32), 1.0, 0.0
                ).astype(jnp.bfloat16)

    def level(k, s, d):
        total = own[k, 0] * pick[0, 0, d]
        for c in range(1, spans):
            total = total + own[k, c] * pick[0, c, d]
        for c in range(spans):
            total = total + raw_in[2, k, c] * pick[0, s * spans + c, d]
        return total

    def hand_early(k, _):
        aside_copy(k).wait_recv()
        for l in range(spans):
            final_out[k, l] = level(k, 3, spans + l)
        last_copy(k).start()
        return 0

    def gather(k, p, cross_done, final_done):
        blocks = [own[k, c] for c in range(spans)]
        for way in range(3):
            blocks += [raw_in[way, k, c] for c in range(spans)]

        def gathered(d):
            total = blocks[0] * pick[p, 0, d]
            for s in range(1, len(blocks)):
                total = total + blocks[s] * pick[p, s, d]
            return total

        for d in range(spans, 2 * spans):
            cross_out[k, d] = gathered(2 * spans + d)
        for d in range(spans):
            cross_out[k, d] = gathered(2 * spans + d)
        cross_done()
        if final_done is not None:
            for d in range(spans):
                final_out[k, d] = gathered(spans + d)
            final_done()
        for d in range(spans):
            kept[k, d] = gathered(d)

    def gathered_in(k):
        arrive(raw_in.at[pl.ds(0, 2), k], mate_recv.at[k])
        aside_copy(k).wait_recv()

    def merge_whole(k, _):
        pass_copy(k).wait_recv()

        def cross_done():
            turn_copy(k).start()
            cross_copy(k, aside, spans, cross_send, 0).start()

        gather(k, 1, cross_done, lambda: final_copy(k, 0).start())
        return 0

    def merge_whole_joined(k, _):
        pass_copy(k).wait_recv()
        gather(k, 1, lambda: cross_copy(k, aside, 2 * spans, joined_send).start(), lambda: None)
        return 0

    def whole(k):
        return (merge_whole if k < TURNED else merge_whole_joined, k)

    def merge_joined(k, _):
        gathered_in(k)
        gather(k, 0, lambda: cross_copy(k, across, 2 * spans, joined_send).start(), lambda: None)
        return 0

    def merge_half(k, _):
        gathered_in(k)
        gather(k, 0, lambda: half_copy(k).start(), lambda: None)
        return 0

    def merge(k, _):
        arrive(raw_in.at[pl.ds(0, 2), k], mate_recv.at[k])
        gather(k, 0, lambda: far_copy(k).start(), None)
        return 0

    def send_rest(k, _):
        cross_copy(k, across, spans, cross_send).start()
        return 0

    def settle(k):
        a, r = lax.div(k, per), lax.rem(k, per)
        start = pl.multiple_of(r * rows_per, rows_per)
        for l in range(spans):
            moved_cache[a, l, pl.ds(start, rows_per), :] = kept[k, l] + cross_in[k, l]

    def finish(k, _):
        cross_copy(k, across, spans, cross_send).wait_recv()
        settle(k)
        return 0

    def hand_on(k, copy):
        for l in range(spans):
            final_out[k, l] = final_out[k, l] + cross_in[k, spans + l]
        copy.start()

    def finish_joined(k, _):
        cross_copy(k, across, 2 * spans, joined_send).wait_recv()
        hand_on(k, final_copy(k, 1))
        settle(k)
        return 0

    def finish_half(k, _):
        half_copy(k).wait_recv()
        hand_on(k, last_copy(k))
        return 0

    loads[1].wait()
    loads[2].wait()
    for k in range(len(others)):
        part_copy(k).wait()
    summed = part[...]
    for k in range(len(others)):
        summed = summed + part_in[k]
    resid = hidden[...].astype(jnp.float32) + summed[:spans]
    centre = jnp.mean(resid, axis=-1, keepdims=True)
    spread = jnp.mean((resid - centre) ** 2, axis=-1, keepdims=True)
    gain = ln_gain[...].reshape(1, width)
    bias = ln_bias[...].reshape(1, width)
    normed = (resid - centre) * lax.rsqrt(spread + 1e-05) * gain + bias
    normed = jnp.concatenate([normed, jnp.zeros((pad, width), jnp.float32)], 0)
    query = jnp.dot(
        normed.astype(jnp.bfloat16), query_proj[...], preferred_element_type=jnp.float32
    ).astype(jnp.bfloat16).astype(jnp.float32)

    decoded = []
    for c in range(spans):
        mixed = attend(query[c : c + 1], cross[0, c], cross[1, c], None, None)
        decoded.append(mixed * jnp.where(alive[c] == 1, 1.0, 0.0))

    line[...] = jnp.concatenate(decoded, 0).astype(jnp.bfloat16)

    @pl.when(outer)
    def _():
        line_copy(mate, 0, 0).start()
        line_copy(aside, 1, 1).start()

    @pl.when(inner)
    def _():
        line_copy(aside, 0, 2).start()

    def turn(k, _):
        turn_copy(k).wait_recv()
        turned_copy(k).start()
        return 0

    def outer_forward(k, _):
        mate_copy(k).start()
        aside_copy(k).wait_recv()
        outer_pass_copy(k).start()
        return 0

    @pl.when(outer)
    def _():
        lax.fori_loop(WHOLE, WHOLE + AHEAD, outer_forward, 0)
        line_copy(mate, 0, 1).wait_recv()
        line_pass_copy().start()
        lax.fori_loop(WHOLE + AHEAD, steps, outer_forward, 0)
        lax.fori_loop(0, TURNED, turn, 0)

    @pl.when(inner)
    def _():
        lax.fori_loop(WHOLE + AHEAD, JOINED, pass_on, 0)

    def forward(k, _):
        mate_copy(k).wait_recv()
        pass_copy(k).start()
        return 0

    def gather_lines():
        for way in range(3):
            line_copy(mate, 0, way).wait_recv()
        blocks = []
        for held in [line] + [line_in.at[way] for way in range(3)]:
            blocks += [held[c : c + 1, :].astype(jnp.float32) for c in range(spans)]
        rows = []
        for d in range(4 * spans):
            total = blocks[0] * pick[0, 0, d, 0:1, :].astype(jnp.float32)
            for s in range(1, len(blocks)):
                total = total + blocks[s] * pick[0, s, d, 0:1, :].astype(jnp.float32)
            rows.append(total)
        line_out[...] = jnp.concatenate(rows[2 * spans :], 0).astype(jnp.bfloat16)
        line_cross_copy().start()
        line_kept[...] = jnp.concatenate(rows[: 2 * spans], 0)

    def send_lines():
        line_cross_copy().wait_recv()
        total = line_kept[...] + line_cross[...].astype(jnp.float32)
        line_last[...] = total[spans:].astype(jnp.bfloat16)
        line_final_copy().start()
        moved_out[...] = total[:spans].astype(jnp.bfloat16)

    def run(groups):
        while groups:
            ops, starts = [op for op, _ in groups[0]], [k for _, k in groups[0]]
            size = 1
            while size < len(groups) and groups[size] == [(op, k + size) for op, k in groups[0]]:
                size += 1

            def step(i, _, ops=ops, starts=starts):
                for op, k in zip(ops, starts):
                    op(i + k, 0)
                return 0

            if size > 1:
                lax.fori_loop(0, size, step, 0)
            else:
                step(0, 0)
            groups = groups[size:]

    def groups(low, high):
        found = []
        for k in range(low, high):
            group = []
            if k < steps:
                group.append(
                    (merge_joined if k < SPLIT else merge_half if k < JOINED else merge, k)
                )
            if SPLIT <= k - DEFER < steps and k < steps:
                group.append((send_rest, k - DEFER))
            if k == steps - 1:
                group += [(send_rest, j) for j in range(steps - DEFER, steps)]
            if WHOLE <= k - LAG < JOINED:
                group.append((finish_joined if k - LAG < SPLIT else finish_half, k - LAG))
            if k < WHOLE + BEHIND:
                group.append(whole(k - BEHIND))
            if TURNED <= k - WHOLE - WAIT + TURNED < WHOLE:
                group.append((finish_joined, k - WHOLE - WAIT + TURNED))
            found.append(group)
        return found

    @pl.when(inner)
    def _():
        label_copy(mate, 0, 2).wait_recv()
        choose_one(0, 0, label, 1, mate)
        choose_one(0, 3, label_in.at[2], 1, mate)
        lax.fori_loop(JOINED, steps, hand_early, 0)
        lax.fori_loop(0, WHOLE, forward, 0)
        for way in (1, 3, 4):
            label_copy(mate, 0, way).wait_recv()
        choose(1, (0, 3, 4), (me, mate, aside, mate_aside))
        choose(0, (0, 1, 2), (me, mate, across, beyond))
        arrive(raw_in.at[1, pl.ds(0, WHOLE)], whole_recv.at[0])
        run([[whole(k)] for k in range(WHOLE - BEHIND)])
        run(groups(WHOLE, LINES))
        gather_lines()
        run(groups(LINES, steps + LAG))
        send_lines()

    def place(k, value):
        a, r = lax.div(k, per), lax.rem(k, per)
        start = pl.multiple_of(r * rows_per, rows_per)
        for l in range(spans):
            moved_cache[a, l, pl.ds(start, rows_per), :] = value(l)

    def land_turned(k, _):
        place(k, lambda l: final_in[k, l] + final_far[k, l])
        return 0

    def land_ready(k, _):
        place(k, lambda l: final_in[k, l])
        return 0

    def land_joined(k, _):
        last_copy(k).wait_recv()
        return land_ready(k, 0)

    def land(k, _):
        last_copy(k).wait_recv()
        far_copy(k).wait_recv()
        place(k, lambda l: final_in[k, l] + final_far[k, l] + level(k, 1, l))
        return 0

    def settle_turned(k, _):
        settle(k)
        return 0

    rest = steps - WHOLE

    @pl.when(inner)
    def _():
        arrive(kept.at[pl.ds(0, TURNED)], cross_recv.at[0])
        lax.fori_loop(0, TURNED, settle_turned, 0)
        lax.fori_loop(SPLIT, steps, finish, 0)
        arrive(label_in.at[pl.ds(0, 3)], label_send.at[0])
        line_copy(aside, 0, 2).wait_send()
        line_cross_copy().wait_send()
        line_final_copy().wait_send()
        arrive(own.at[pl.ds(0, WHOLE)], own_send)
        arrive(own.at[pl.ds(0, rest)], aside_send)
        arrive(own.at[pl.ds(0, WHOLE)], pass_send)
        arrive(own.at[pl.ds(0, TURNED + steps - SPLIT)], far_send)
        arrive(own.at[pl.ds(0, TURNED + steps - SPLIT)], cross_send)
        arrive(cross_out.at[pl.ds(0, SPLIT - TURNED)], joined_send)
        arrive(own, final_send)

    @pl.when(outer)
    def _():
        choose_one(0, 0, label, 0, me)
        choose_one(0, 1, label_in.at[1], 0, me)
        arrive(final_in.at[pl.ds(0, TURNED)], final_recv.at[0])
        arrive(final_far.at[pl.ds(0, TURNED)], far_recv.at[0])
        lax.fori_loop(0, TURNED, land_turned, 0)
        arrive(final_in.at[pl.ds(TURNED, SPLIT - TURNED)], final_recv.at[1])
        lax.fori_loop(TURNED, SPLIT, land_ready, 0)
        lax.fori_loop(SPLIT, JOINED, land_joined, 0)
        lax.fori_loop(JOINED, steps, land, 0)
        arrive(label_in.at[pl.ds(0, 3)], label_send.at[0])
        arrive(line_in, line_send.at[0])
        line_final_copy().wait_recv()
        moved_out[...] = line_final[...]
        arrive(own, own_send)
        arrive(own.at[pl.ds(0, rest)], aside_send)
        arrive(own.at[pl.ds(0, rest)], pass_send)
        arrive(own.at[pl.ds(0, TURNED)], far_send)


def store_kernel(cache, out, cache_hbm, out_hbm, sems):
    copies = [pltpu.make_async_copy(out, out_hbm, sems.at[0])] + [
        pltpu.make_async_copy(cache.at[a], cache_hbm.at[a], sems.at[1 + a]) for a in range(2)
    ]
    for copy in copies:
        copy.start()
    for copy in copies:
        copy.wait()


def body(
    hidden,
    token_qkv,
    self_cache,
    cross_kv,
    cache_len,
    finished,
    new_slot,
    out_proj,
    ln_gain,
    ln_bias,
    query_proj,
):
    count, cores = lax.axis_size("batch"), lax.axis_size("mp")
    spans, width = hidden.shape
    slots, local = self_cache.shape[2:]
    moves = len(DISTANCES)
    smem = pl.BlockSpec(memory_space=pltpu.SMEM)
    vmem = pl.BlockSpec(memory_space=pltpu.VMEM)
    away = pl.BlockSpec(memory_space=pl.ANY)
    bf16, f32 = jnp.bfloat16, jnp.float32
    operands = (
        cache_len,
        finished,
        new_slot,
        hidden,
        token_qkv,
        self_cache,
        ln_gain,
        ln_bias,
        cross_kv,
        out_proj,
        query_proj,
    )
    parcels = pltpu.VMEM((moves, 2, slots, local), bf16)
    tiles = pltpu.VMEM((moves, 16, local), bf16)
    dma = pltpu.SemaphoreType.DMA
    inputs = [pltpu.VMEM(array.shape, bf16) for array in (cross_kv, out_proj, query_proj)]
    parts = [pltpu.VMEM((8, width), f32), pltpu.VMEM((cores - 1, 8, width), f32)]
    steps = 2 * slots // ROWS
    if count == 2 * (REACH + 1) and cores == 2:
        function, specs = relay_kernel, [away] * 8

        def blocks(*lead):
            return pltpu.VMEM(lead + (ROWS, local), bf16)

        small = [pltpu.SMEM((spans,), jnp.int32)] * 3 + [
            pltpu.VMEM(hidden.shape, bf16),
            pltpu.VMEM(token_qkv.shape, bf16),
            pltpu.VMEM(ln_gain.shape, f32),
            pltpu.VMEM(ln_bias.shape, f32),
        ]
        scratch = small + [pltpu.VMEM(self_cache.shape, bf16)] + inputs + [
            blocks(steps, spans),
            blocks(3, steps, spans),
            blocks(steps, 2 * spans),
            blocks(steps, 2 * spans),
            blocks(steps, spans),
            blocks(steps, spans),
            blocks(steps, spans),
            blocks(steps, spans),
            blocks(2, 4 * spans, 4 * spans),
            pltpu.VMEM((8, 128), f32),
            pltpu.VMEM((5, 8, 128), f32),
            pltpu.VMEM((spans, local), bf16),
            pltpu.VMEM((3, spans, local), bf16),
            pltpu.VMEM((2 * spans, local), f32),
            pltpu.VMEM((2 * spans, local), bf16),
            pltpu.VMEM((2 * spans, local), bf16),
            pltpu.VMEM((spans, local), bf16),
            pltpu.VMEM((spans, local), bf16),
            *parts,
            dma((12,)),
            dma((7,)),
            dma((steps,)),
            dma((steps,)),
            dma((1,)),
            dma((steps - TURNED + 1,)),
            dma((steps - SPLIT + 2,)),
            dma((steps - JOINED + 1,)),
            dma((JOINED - SPLIT,)),
            dma((1,)),
            dma((5,)),
            dma((1,)),
            dma((3,)),
            dma((4,)),
            dma((2, cores - 1)),
            pltpu.SemaphoreType.REGULAR,
        ]
    else:
        function, specs = kernel, [smem] * 3 + [vmem] * 5
        scratch = inputs + [
            pltpu.VMEM(self_cache.shape, bf16),
            parcels,
            parcels,
            tiles,
            tiles,
            tiles,
            tiles,
            *parts,
            dma((3,)),
            dma((2, moves)),
            dma((2, moves)),
            dma((2, moves)),
            dma((2, cores - 1)),
        ]
    moved = pl.pallas_call(
        functools.partial(function, count, cores),
        out_shape=(
            pltpu.VMEM(self_cache.shape, bf16),
            pltpu.VMEM((spans, local), bf16),
        ),
        in_specs=specs + [away] * 3,
        out_specs=(vmem, vmem),
        scratch_shapes=scratch,
        compiler_params=pltpu.CompilerParams(collective_id=0, has_side_effects=True),
    )(*operands)
    return pl.pallas_call(
        store_kernel,
        out_shape=tuple(jax.ShapeDtypeStruct(array.shape, bf16) for array in moved),
        in_specs=[vmem, vmem],
        out_specs=(away, away),
        scratch_shapes=[dma((3,))],
    )(*(pltpu.with_memory_space_constraint(a, pltpu.VMEM) for a in moved))


def solution(mesh):
    placed = (
        P(("groups", "batch"), None),
        P(None, ("groups", "batch"), "mp"),
        P(None, ("groups", "batch"), None, "mp"),
        P(None, ("groups", "batch"), None, "mp"),
        P(("groups", "batch")),
        P(("groups", "batch")),
        P(("groups", "batch")),
        P("mp", None),
        P(),
        P(),
        P(None, "mp"),
    )
    return jax.shard_map(
        body,
        mesh=mesh,
        in_specs=placed,
        out_specs=(P(None, ("groups", "batch"), None, "mp"), P(("groups", "batch"), "mp")),
        check_vma=False,
    )
```

```python
import functools

import jax
import jax.numpy as jnp
from jax import lax
from jax.experimental import pallas as pl
from jax.experimental.pallas import tpu as pltpu
from jax.sharding import PartitionSpec as P

HEAD_DIM = 64
REACH = 3
MESH = pl.DeviceIdType.MESH
DISTANCES = [3, -3, 2, -2, 1, -1]
ROWS = 16
WHOLE = 7
SPLIT = 10
JOINED = 14
AHEAD = 5
LAG = 3
BEHIND = 3
TURNED = 4
WAIT = 4
DEFER = 1
DEFER_ONE = 6
LINES = 10


def attend(query, keys, values, length, own):
    slots, width = keys.shape
    heads = width // HEAD_DIM
    rows = -(-heads // 16) * 16
    row = lax.broadcasted_iota(jnp.int32, (rows, width), 0)
    column = lax.broadcasted_iota(jnp.int32, (rows, width), 1)
    low = row * HEAD_DIM
    mine = (column >= low) & (column < low + HEAD_DIM)
    spread = jnp.where(mine, query.astype(jnp.float32), 0.0)
    factor = HEAD_DIM ** (-0.5)
    scores = (
        lax.dot_general(
            spread.astype(jnp.bfloat16),
            keys,
            (((1,), (1,)), ((), ())),
            preferred_element_type=jnp.float32,
        )
        * factor
    )
    if length is not None:
        usable = lax.broadcasted_iota(jnp.int32, (rows, slots), 1) < length
        scores = jnp.where(usable, scores, -1e30)
    highest = jnp.max(scores, axis=-1, keepdims=True)
    if own is not None:
        new_key, new_value = own
        own_score = jnp.sum(spread * new_key.astype(jnp.float32), axis=-1, keepdims=True) * factor
        highest = jnp.maximum(highest, own_score)
    weight = jnp.exp(scores - highest)
    if length is not None:
        weight = jnp.where(usable, weight, 0.0)
    total = jnp.sum(weight, axis=-1, keepdims=True)
    if own is not None:
        own_weight = jnp.exp(own_score - highest)
        total = total + own_weight
    weight = (weight / total).astype(jnp.bfloat16)
    mixed = jnp.dot(weight, values, preferred_element_type=jnp.float32)
    if own is not None:
        own_weight = (own_weight / total).astype(jnp.bfloat16).astype(jnp.float32)
        mixed = mixed + own_weight * new_value.astype(jnp.float32)
    return jnp.sum(jnp.where(mine, mixed, 0.0), axis=0, keepdims=True)


def kernel(
    count,
    cores,
    cache_len,
    finished,
    new_slot,
    hidden,
    token_qkv,
    self_cache,
    ln_gain,
    ln_bias,
    cross_hbm,
    out_proj_hbm,
    query_proj_hbm,
    moved_cache,
    moved_out,
    cross,
    out_proj,
    query_proj,
    updated,
    parcel,
    arrived,
    mark,
    mark_in,
    line,
    line_in,
    part,
    part_in,
    load_sem,
    cache_sems,
    mark_sems,
    line_sems,
    part_sems,
):
    spans, width = hidden.shape
    slots, local = self_cache.shape[2:]
    me = lax.axis_index("batch")
    core = lax.axis_index("mp")
    loads = [
        pltpu.make_async_copy(source, target, load_sem.at[i])
        for i, (source, target) in enumerate(
            [(out_proj_hbm, out_proj), (query_proj_hbm, query_proj), (cross_hbm, cross)]
        )
    ]
    for load in loads:
        load.start()

    barrier = pltpu.get_barrier_semaphore()
    targets = [lax.rem(me + distance + count, count) for distance in DISTANCES]
    for target in targets:
        pl.semaphore_signal(barrier, inc=1, device_id={"batch": target}, device_id_type=MESH)
    others = [lax.rem(core + k, cores) for k in range(1, cores)]
    for other in others:
        pl.semaphore_signal(barrier, inc=1, device_id={"mp": other}, device_id_type=MESH)

    half = count // 2
    alive, offset, place = [], [], []
    for c in range(spans):
        slot = new_slot[c]
        owner = lax.div(slot, spans)
        offset.append(lax.rem(owner - me + half + count, count) - half)
        place.append(lax.rem(slot, spans))
        alive.append(jnp.where(finished[c] == 0, 1, 0))

    position = lax.broadcasted_iota(jnp.int32, (slots, local), 0)
    for c in range(spans):
        length = cache_len[c]
        older = jnp.where(position < length * alive[c], 1.0, 0.0).astype(jnp.bfloat16)
        fresh = jnp.where(position == jnp.where(alive[c] == 1, length, -1), 1.0, 0.0).astype(
            jnp.bfloat16
        )
        for a in range(2):
            updated[a, c] = self_cache[a, c] * older + token_qkv[1 + a, c : c + 1, :] * fresh

    def flag(value, shape):
        return jnp.full(shape, jnp.where(value, 1.0, 0.0), jnp.float32).astype(jnp.bfloat16)

    marker_row = lax.broadcasted_iota(jnp.int32, mark.shape[1:], 0)
    for i, distance in enumerate(DISTANCES):
        marker = jnp.zeros(mark.shape[1:], jnp.float32)
        for c in range(spans):
            at = jnp.where(offset[c] == distance, place[c], -1)
            marker = jnp.where(marker_row == at, 1.0, marker)
        mark[i] = marker.astype(jnp.bfloat16)

    def send(source, target, sems, i, distance):
        return pltpu.make_async_remote_copy(
            src_ref=source,
            dst_ref=target,
            send_sem=sems.at[0, i],
            recv_sem=sems.at[1, i],
            device_id={"batch": targets[i]},
            device_id_type=MESH,
        )

    pl.semaphore_wait(barrier, len(targets) + len(others))
    mark_copies, cache_copies = [], []
    for i, distance in enumerate(DISTANCES):
        copy = send(mark.at[i], mark_in.at[i], mark_sems, i, distance)
        copy.start()
        mark_copies.append(copy)
    for i, distance in enumerate(DISTANCES):
        for a in range(2):
            total = updated[a, 0] * flag(offset[0] == distance, (1, local))
            for c in range(1, spans):
                total = total + updated[a, c] * flag(offset[c] == distance, (1, local))
            parcel[i, a] = total
        copy = send(parcel.at[i], arrived.at[i], cache_sems, i, distance)
        copy.start()
        cache_copies.append(copy)

    for l in range(spans):
        for a in range(2):
            total = updated[a, 0] * flag((offset[0] == 0) & (place[0] == l), (1, local))
            for c in range(1, spans):
                keep = flag((offset[c] == 0) & (place[c] == l), (1, local))
                total = total + updated[a, c] * keep
            moved_cache[a, l] = total

    contexts = []
    for c in range(spans):
        query, key, value = (token_qkv[k, c : c + 1, :] for k in range(3))
        contexts.append(
            attend(query, self_cache[0, c], self_cache[1, c], cache_len[c], (key, value))
        )
    pad = part.shape[0] - spans
    context = jnp.concatenate(contexts + [jnp.zeros((pad, local), jnp.float32)], 0)
    context = context.astype(jnp.bfloat16)
    loads[0].wait()
    part[...] = jnp.dot(context, out_proj[...], preferred_element_type=jnp.float32)
    part_copies = []
    for k, other in enumerate(others):
        copy = pltpu.make_async_remote_copy(
            src_ref=part,
            dst_ref=part_in.at[k],
            send_sem=part_sems.at[0, k],
            recv_sem=part_sems.at[1, k],
            device_id={"mp": other},
            device_id_type=MESH,
        )
        copy.start()
        part_copies.append(copy)
    loads[1].wait()
    loads[2].wait()
    for copy in part_copies:
        copy.wait()
    summed = part[...]
    for k in range(len(others)):
        summed = summed + part_in[k]
    resid = hidden[...].astype(jnp.float32) + summed[:spans]
    centre = jnp.mean(resid, axis=-1, keepdims=True)
    spread = jnp.mean((resid - centre) ** 2, axis=-1, keepdims=True)
    gain = ln_gain[...].reshape(1, width)
    bias = ln_bias[...].reshape(1, width)
    normed = (resid - centre) * lax.rsqrt(spread + 1e-05) * gain + bias
    normed = jnp.concatenate([normed, jnp.zeros((pad, width), jnp.float32)], 0)
    query = jnp.dot(
        normed.astype(jnp.bfloat16), query_proj[...], preferred_element_type=jnp.float32
    ).astype(jnp.bfloat16).astype(jnp.float32)
    decoded = []
    for c in range(spans):
        mixed = attend(query[c : c + 1], cross[0, c], cross[1, c], None, None)
        decoded.append(mixed * jnp.where(alive[c] == 1, 1.0, 0.0))

    line_copies = []
    blank = jnp.zeros((line.shape[1] - 1, local), jnp.float32)
    for i, distance in enumerate(DISTANCES):
        row = jnp.zeros((1, local), jnp.float32)
        for c in range(spans):
            row = row + decoded[c] * jnp.where(offset[c] == distance, 1.0, 0.0)
        line[i] = jnp.concatenate([row, blank], 0).astype(jnp.bfloat16)
        copy = send(line.at[i], line_in.at[i], line_sems, i, distance)
        copy.start()
        line_copies.append(copy)

    rows = []
    for l in range(spans):
        row = jnp.zeros((1, local), jnp.float32)
        for c in range(spans):
            keep = (offset[c] == 0) & (place[c] == l)
            row = row + decoded[c] * jnp.where(keep, 1.0, 0.0)
        rows.append(row)
    for i in range(len(DISTANCES)):
        mark_copies[i].wait()
        cache_copies[i].wait()
        for l in range(spans):
            taken = mark_in[i, l : l + 1, :]
            for a in range(2):
                moved_cache[a, l] = moved_cache[a, l] + arrived[i, a] * taken
    for i in range(len(DISTANCES)):
        line_copies[i].wait()
        for l in range(spans):
            taken = mark_in[i, l : l + 1, :].astype(jnp.float32)
            rows[l] = rows[l] + line_in[i, 0:1, :].astype(jnp.float32) * taken
    moved_out[...] = jnp.concatenate(rows, 0).astype(jnp.bfloat16)


def relay_kernel(
    count,
    cores,
    cache_len_hbm,
    finished_hbm,
    new_slot_hbm,
    hidden_hbm,
    token_qkv_hbm,
    cache_hbm,
    ln_gain_hbm,
    ln_bias_hbm,
    cross_hbm,
    out_proj_hbm,
    query_proj_hbm,
    moved_cache,
    moved_out,
    cache_len,
    finished,
    new_slot,
    hidden,
    token_qkv,
    ln_gain,
    ln_bias,
    self_cache,
    cross,
    out_proj,
    query_proj,
    own,
    raw_in,
    cross_out,
    cross_in,
    kept,
    final_out,
    final_in,
    final_far,
    pick,
    label,
    label_in,
    line,
    line_in,
    line_kept,
    line_out,
    line_cross,
    line_last,
    line_final,
    part,
    part_in,
    load_sem,
    send_sems,
    mate_recv,
    second_recv,
    whole_recv,
    cross_recv,
    final_recv,
    far_recv,
    half_recv,
    label_send,
    label_recv,
    line_send,
    line_recv,
    line_hops,
    part_sems,
    core_sem,
):
    spans, width = hidden.shape
    slots, local = self_cache.shape[2:]
    steps, _, rows_per, _ = own.shape
    per = steps // 2
    me = lax.axis_index("batch")
    core = lax.axis_index("mp")
    level, column = lax.div(me, 2), lax.rem(me, 2)
    inner = (level == 1) | (level == REACH - 1)
    outer = jnp.logical_not(inner)
    barrier = pltpu.get_barrier_semaphore()

    def greet(where):
        pl.semaphore_signal(barrier, inc=1, device_id=where, device_id_type=MESH)

    mate_level = jnp.where(level == 0, 1, jnp.where(level == 1, 0, jnp.where(level == 2, 3, 2)))
    mate = mate_level * 2 + column
    mate_aside = mate_level * 2 + 1 - column
    aside = level * 2 + 1 - column
    across = (REACH - level) * 2 + column
    beyond = (REACH - mate_level) * 2 + column
    others = [lax.rem(core + k, cores) for k in range(1, cores)]
    for node in (mate, aside):
        greet({"batch": node})

    @pl.when(inner)
    def _():
        greet({"batch": across})

    @pl.when(core == 0)
    def _():
        greet({"mp": 1})

    loads = [
        pltpu.make_async_copy(source, target, load_sem.at[i])
        for i, (source, target) in enumerate(
            [
                (out_proj_hbm, out_proj),
                (query_proj_hbm, query_proj),
                (cross_hbm, cross),
                (cache_hbm.at[0], self_cache.at[0]),
                (cache_hbm.at[1], self_cache.at[1]),
                (cache_len_hbm, cache_len),
                (finished_hbm, finished),
                (new_slot_hbm, new_slot),
                (hidden_hbm, hidden),
                (token_qkv_hbm, token_qkv),
                (ln_gain_hbm, ln_gain),
                (ln_bias_hbm, ln_bias),
            ]
        )
    ]
    for i in [3, *range(5, len(loads)), 4, 0, 1, 2]:
        loads[i].start()
    for load in loads[5:]:
        load.wait()

    alive = [jnp.where(finished[c] == 0, 1, 0) for c in range(spans)]

    def to(node, source, target, sent, received):
        return pltpu.make_async_remote_copy(
            src_ref=source,
            dst_ref=target,
            send_sem=sent,
            recv_sem=received,
            device_id={"batch": node},
            device_id_type=MESH,
        )

    own_send, aside_send, pass_send, far_send, cross_send, joined_send, final_send = (
        send_sems.at[i] for i in range(7)
    )

    def mate_copy(k):
        return to(mate, own.at[k], raw_in.at[0, k], own_send, mate_recv.at[k])

    def across_copy(k):
        return to(across, own.at[k], raw_in.at[1, k], own_send, whole_recv.at[0])

    def aside_copy(k):
        return to(aside, own.at[k], raw_in.at[2, k], aside_send, second_recv.at[k])

    def pass_copy(k):
        return to(across, raw_in.at[0, k], raw_in.at[2, k], pass_send, second_recv.at[k])

    def outer_pass_copy(k):
        return to(mate, raw_in.at[2, k], raw_in.at[1, k], pass_send, mate_recv.at[k])

    def arrive(blocks, sem):
        pltpu.make_async_copy(blocks, blocks, sem).wait()

    def far_copy(k):
        return to(
            beyond,
            cross_out.at[k, pl.ds(spans, spans)],
            final_far.at[k],
            far_send,
            far_recv.at[k - JOINED + 1],
        )

    def half_copy(k):
        return to(
            across,
            cross_out.at[k, pl.ds(spans, spans)],
            cross_in.at[k, pl.ds(spans, spans)],
            far_send,
            half_recv.at[k - SPLIT],
        )

    def turn_copy(k):
        return to(
            mate,
            cross_out.at[k, pl.ds(spans, spans)],
            raw_in.at[2, k],
            far_send,
            second_recv.at[k],
        )

    def turned_copy(k):
        return to(aside, raw_in.at[2, k], final_far.at[k], far_send, far_recv.at[0])

    def cross_copy(k, node, count, sent, slot=None):
        return to(
            node,
            cross_out.at[k, pl.ds(0, count)],
            cross_in.at[k, pl.ds(0, count)],
            sent,
            cross_recv.at[k - TURNED + 1 if slot is None else slot],
        )

    def final_copy(k, slot):
        return to(mate, final_out.at[k], final_in.at[k], final_send, final_recv.at[slot])

    def last_copy(k):
        return final_copy(k, k - SPLIT + 2)

    def label_copy(node, lane, way):
        return to(node, label, label_in.at[way], label_send.at[0], label_recv.at[way])

    def line_copy(node, lane, way):
        return to(node, line, line_in.at[way], line_send.at[0], line_recv.at[way])

    def label_pass_copy(node, here, there):
        return to(node, label_in.at[here], label_in.at[there], label_send.at[0], label_recv.at[there])

    def line_pass_copy():
        return to(mate, line_in.at[1], line_in.at[1], line_send.at[0], line_recv.at[1])

    def line_cross_copy():
        return to(across, line_out, line_cross, line_hops.at[0], line_hops.at[1])

    def line_final_copy():
        return to(mate, line_last, line_final, line_hops.at[2], line_hops.at[3])

    label_row = lax.broadcasted_iota(jnp.int32, label.shape, 0)
    labels = jnp.zeros(label.shape, jnp.int32)
    for c in range(spans):
        labels = jnp.where(label_row == c, new_slot[c], labels)
    label[...] = labels.astype(jnp.float32)

    @pl.when(inner)
    def _():
        pl.semaphore_wait(barrier, 3 + core)

    @pl.when(outer)
    def _():
        pl.semaphore_wait(barrier, 2 + core)

    @pl.when(core == 1)
    def _():
        pl.semaphore_signal(core_sem, inc=1, device_id={"mp": 0}, device_id_type=MESH)

    position = lax.broadcasted_iota(jnp.int32, (rows_per, local), 0)
    ends = [cache_len[c] * alive[c] for c in range(spans)]
    fresh_at = [jnp.where(alive[c] == 1, cache_len[c], -1) for c in range(spans)]

    def grow(k, _):
        a, r = lax.div(k, per), lax.rem(k, per)
        start = pl.multiple_of(r * rows_per, rows_per)
        at = position + start
        for c in range(spans):
            older = jnp.where(at < ends[c], 1.0, 0.0).astype(jnp.bfloat16)
            fresh = jnp.where(at == fresh_at[c], 1.0, 0.0).astype(jnp.bfloat16)
            new = jnp.where(a == 0, token_qkv[1, c : c + 1, :].astype(jnp.float32),
                            token_qkv[2, c : c + 1, :].astype(jnp.float32)).astype(jnp.bfloat16)
            own[k, c] = self_cache[a, c, pl.ds(start, rows_per), :] * older + new * fresh

        return 0

    def pass_whole(k, _):
        grow(k, 0)

        @pl.when(outer)
        def _():
            mate_copy(k).start()

        @pl.when(inner)
        def _():
            across_copy(k).start()

        return 0

    def pass_on(k, _):
        aside_copy(k).start()
        return 0

    @pl.when(outer)
    def _():
        label_copy(mate, 0, 0).start()
        label_copy(aside, 1, 1).start()

    @pl.when(inner)
    def _():
        label_copy(aside, 0, 2).start()
        label_copy(across, 1, 3).start()

    loads[3].wait()
    lax.fori_loop(0, WHOLE, pass_whole, 0)
    lax.fori_loop(WHOLE, per, grow, 0)
    loads[4].wait()
    lax.fori_loop(per, steps, grow, 0)

    @pl.when(inner)
    def _():
        lax.fori_loop(JOINED, steps, pass_on, 0)
        lax.fori_loop(WHOLE, WHOLE + AHEAD, pass_on, 0)

    @pl.when(outer)
    def _():
        lax.fori_loop(WHOLE, steps, pass_on, 0)


    def self_part():
        contexts = []
        for c in range(spans):
            query, key, value = (token_qkv[k, c : c + 1, :] for k in range(3))
            contexts.append(
                attend(query, self_cache[0, c], self_cache[1, c], cache_len[c], (key, value))
            )
        context = jnp.concatenate(contexts + [jnp.zeros((pad, local), jnp.float32)], 0)
        context = context.astype(jnp.bfloat16)
        loads[0].wait()
        part[...] = jnp.dot(context, out_proj[...], preferred_element_type=jnp.float32)

    def part_copy(k):
        return pltpu.make_async_remote_copy(
            src_ref=part,
            dst_ref=part_in.at[k],
            send_sem=part_sems.at[0, k],
            recv_sem=part_sems.at[1, k],
            device_id={"mp": others[k]},
            device_id_type=MESH,
        )

    pad = part.shape[0] - spans
    self_part()

    @pl.when(core == 0)
    def _():
        pl.semaphore_wait(core_sem, 1)

    for k in range(len(others)):
        part_copy(k).start()

    @pl.when(outer)
    def _():
        label_copy(mate, 0, 1).wait_recv()
        label_pass_copy(mate, 1, 1).start()

    @pl.when(inner)
    def _():
        label_copy(mate, 0, 0).wait_recv()
        label_pass_copy(across, 0, 4).start()

    def choose(p, ways, nodes):
        for s, source in enumerate([label] + [label_in.at[way] for way in ways]):
            for d, node in enumerate(nodes):
                choose_one(p, s, source, d, node)

    def choose_one(p, s, source, d, node):
        for c in range(spans):
            held = jnp.broadcast_to(source[c : c + 1, 0:1], (rows_per, local))
            for l in range(spans):
                wanted = jnp.full((rows_per, local), node * spans + l, jnp.int32)
                pick[p, s * spans + c, d * spans + l] = jnp.where(
                    held == wanted.astype(jnp.float32), 1.0, 0.0
                ).astype(jnp.bfloat16)

    def level(k, s, d):
        total = own[k, 0] * pick[0, 0, d]
        for c in range(1, spans):
            total = total + own[k, c] * pick[0, c, d]
        for c in range(spans):
            total = total + raw_in[2, k, c] * pick[0, s * spans + c, d]
        return total

    def hand_early(k, _):
        aside_copy(k).wait_recv()
        for l in range(spans):
            final_out[k, l] = level(k, 3, spans + l)
        last_copy(k).start()
        return 0

    def gather(k, p, cross_done, final_done):
        blocks = [own[k, c] for c in range(spans)]
        for way in range(3):
            blocks += [raw_in[way, k, c] for c in range(spans)]

        def gathered(d):
            total = blocks[0] * pick[p, 0, d]
            for s in range(1, len(blocks)):
                total = total + blocks[s] * pick[p, s, d]
            return total

        for d in range(spans, 2 * spans):
            cross_out[k, d] = gathered(2 * spans + d)
        for d in range(spans):
            cross_out[k, d] = gathered(2 * spans + d)
        cross_done()
        if final_done is not None:
            for d in range(spans):
                final_out[k, d] = gathered(spans + d)
            final_done()
        for d in range(spans):
            kept[k, d] = gathered(d)

    def gathered_in(k):
        arrive(raw_in.at[pl.ds(0, 2), k], mate_recv.at[k])
        aside_copy(k).wait_recv()

    def merge_whole(k, _):
        pass_copy(k).wait_recv()

        def cross_done():
            turn_copy(k).start()
            cross_copy(k, aside, spans, cross_send, 0).start()

        gather(k, 1, cross_done, lambda: final_copy(k, 0).start())
        return 0

    def merge_whole_joined(k, _):
        pass_copy(k).wait_recv()
        gather(k, 1, lambda: cross_copy(k, aside, 2 * spans, joined_send).start(), lambda: None)
        return 0

    def whole(k):
        return (merge_whole if k < TURNED else merge_whole_joined, k)

    def merge_joined(k, _):
        gathered_in(k)
        gather(k, 0, lambda: cross_copy(k, across, 2 * spans, joined_send).start(), lambda: None)
        return 0

    def merge_half(k, _):
        gathered_in(k)
        gather(k, 0, lambda: half_copy(k).start(), lambda: None)
        return 0

    def merge(k, _):
        arrive(raw_in.at[pl.ds(0, 2), k], mate_recv.at[k])
        gather(k, 0, lambda: far_copy(k).start(), None)
        return 0

    def send_rest(k, _):
        cross_copy(k, across, spans, cross_send).start()
        return 0

    def settle(k):
        a, r = lax.div(k, per), lax.rem(k, per)
        start = pl.multiple_of(r * rows_per, rows_per)
        for l in range(spans):
            moved_cache[a, l, pl.ds(start, rows_per), :] = kept[k, l] + cross_in[k, l]

    def finish(k, _):
        cross_copy(k, across, spans, cross_send).wait_recv()
        settle(k)
        return 0

    def hand_on(k, copy):
        for l in range(spans):
            final_out[k, l] = final_out[k, l] + cross_in[k, spans + l]
        copy.start()

    def finish_joined(k, _):
        cross_copy(k, across, 2 * spans, joined_send).wait_recv()
        hand_on(k, final_copy(k, 1))
        settle(k)
        return 0

    def finish_half(k, _):
        half_copy(k).wait_recv()
        hand_on(k, last_copy(k))
        return 0

    loads[1].wait()
    loads[2].wait()
    for k in range(len(others)):
        part_copy(k).wait()
    summed = part[...]
    for k in range(len(others)):
        summed = summed + part_in[k]
    resid = hidden[...].astype(jnp.float32) + summed[:spans]
    centre = jnp.mean(resid, axis=-1, keepdims=True)
    spread = jnp.mean((resid - centre) ** 2, axis=-1, keepdims=True)
    gain = ln_gain[...].reshape(1, width)
    bias = ln_bias[...].reshape(1, width)
    normed = (resid - centre) * lax.rsqrt(spread + 1e-05) * gain + bias
    normed = jnp.concatenate([normed, jnp.zeros((pad, width), jnp.float32)], 0)
    query = jnp.dot(
        normed.astype(jnp.bfloat16), query_proj[...], preferred_element_type=jnp.float32
    ).astype(jnp.bfloat16).astype(jnp.float32)

    decoded = []
    for c in range(spans):
        mixed = attend(query[c : c + 1], cross[0, c], cross[1, c], None, None)
        decoded.append(mixed * jnp.where(alive[c] == 1, 1.0, 0.0))

    line[...] = jnp.concatenate(decoded, 0).astype(jnp.bfloat16)

    @pl.when(outer)
    def _():
        line_copy(mate, 0, 0).start()
        line_copy(aside, 1, 1).start()

    @pl.when(inner)
    def _():
        line_copy(aside, 0, 2).start()

    def turn(k, _):
        turn_copy(k).wait_recv()
        turned_copy(k).start()
        return 0

    def outer_forward(k, _):
        mate_copy(k).start()
        aside_copy(k).wait_recv()
        outer_pass_copy(k).start()
        return 0

    @pl.when(outer)
    def _():
        lax.fori_loop(WHOLE, WHOLE + AHEAD, outer_forward, 0)
        line_copy(mate, 0, 1).wait_recv()
        line_pass_copy().start()
        lax.fori_loop(WHOLE + AHEAD, steps, outer_forward, 0)
        lax.fori_loop(0, TURNED, turn, 0)

    @pl.when(inner)
    def _():
        lax.fori_loop(WHOLE + AHEAD, JOINED, pass_on, 0)

    def forward(k, _):
        mate_copy(k).wait_recv()
        pass_copy(k).start()
        return 0

    def gather_lines():
        for way in range(3):
            line_copy(mate, 0, way).wait_recv()
        blocks = []
        for held in [line] + [line_in.at[way] for way in range(3)]:
            blocks += [held[c : c + 1, :].astype(jnp.float32) for c in range(spans)]
        rows = []
        for d in range(4 * spans):
            total = blocks[0] * pick[0, 0, d, 0:1, :].astype(jnp.float32)
            for s in range(1, len(blocks)):
                total = total + blocks[s] * pick[0, s, d, 0:1, :].astype(jnp.float32)
            rows.append(total)
        line_out[...] = jnp.concatenate(rows[2 * spans :], 0).astype(jnp.bfloat16)
        line_cross_copy().start()
        line_kept[...] = jnp.concatenate(rows[: 2 * spans], 0)

    def send_lines():
        line_cross_copy().wait_recv()
        total = line_kept[...] + line_cross[...].astype(jnp.float32)
        line_last[...] = total[spans:].astype(jnp.bfloat16)
        line_final_copy().start()
        moved_out[...] = total[:spans].astype(jnp.bfloat16)

    def run(groups):
        while groups:
            ops, starts = [op for op, _ in groups[0]], [k for _, k in groups[0]]
            size = 1
            while size < len(groups) and groups[size] == [(op, k + size) for op, k in groups[0]]:
                size += 1

            def step(i, _, ops=ops, starts=starts):
                for op, k in zip(ops, starts):
                    op(i + k, 0)
                return 0

            if size > 1:
                lax.fori_loop(0, size, step, 0)
            else:
                step(0, 0)
            groups = groups[size:]

    def groups(low, high, defer):
        found = []
        for k in range(low, high):
            group = []
            if k < steps:
                group.append(
                    (merge_joined if k < SPLIT else merge_half if k < JOINED else merge, k)
                )
            if SPLIT <= k - defer < steps and k < steps:
                group.append((send_rest, k - defer))
            if k == steps - 1:
                group += [(send_rest, j) for j in range(steps - defer, steps)]
            if WHOLE <= k - LAG < JOINED:
                group.append((finish_joined if k - LAG < SPLIT else finish_half, k - LAG))
            if k < WHOLE + BEHIND:
                group.append(whole(k - BEHIND))
            if TURNED <= k - WHOLE - WAIT + TURNED < WHOLE:
                group.append((finish_joined, k - WHOLE - WAIT + TURNED))
            found.append(group)
        return found

    @pl.when(inner)
    def _():
        label_copy(mate, 0, 2).wait_recv()
        choose_one(0, 0, label, 1, mate)
        choose_one(0, 3, label_in.at[2], 1, mate)
        lax.fori_loop(JOINED, steps, hand_early, 0)
        lax.fori_loop(0, WHOLE, forward, 0)
        for way in (1, 3, 4):
            label_copy(mate, 0, way).wait_recv()
        choose(1, (0, 3, 4), (me, mate, aside, mate_aside))
        choose(0, (0, 1, 2), (me, mate, across, beyond))
        arrive(raw_in.at[1, pl.ds(0, WHOLE)], whole_recv.at[0])
        run([[whole(k)] for k in range(WHOLE - BEHIND)])
        run(groups(WHOLE, LINES, DEFER))
        gather_lines()

        @pl.when(core == 0)
        def _():
            run(groups(LINES, steps + LAG, DEFER))

        @pl.when(core != 0)
        def _():
            run(groups(LINES, steps + LAG, DEFER_ONE))

        send_lines()

    def place(k, value):
        a, r = lax.div(k, per), lax.rem(k, per)
        start = pl.multiple_of(r * rows_per, rows_per)
        for l in range(spans):
            moved_cache[a, l, pl.ds(start, rows_per), :] = value(l)

    def land_turned(k, _):
        place(k, lambda l: final_in[k, l] + final_far[k, l])
        return 0

    def land_ready(k, _):
        place(k, lambda l: final_in[k, l])
        return 0

    def land_joined(k, _):
        last_copy(k).wait_recv()
        return land_ready(k, 0)

    def land(k, _):
        last_copy(k).wait_recv()
        far_copy(k).wait_recv()
        place(k, lambda l: final_in[k, l] + final_far[k, l] + level(k, 1, l))
        return 0

    def settle_turned(k, _):
        settle(k)
        return 0

    rest = steps - WHOLE

    @pl.when(inner)
    def _():
        arrive(kept.at[pl.ds(0, TURNED)], cross_recv.at[0])
        lax.fori_loop(0, TURNED, settle_turned, 0)
        lax.fori_loop(SPLIT, steps, finish, 0)
        arrive(label_in.at[pl.ds(0, 3)], label_send.at[0])
        line_copy(aside, 0, 2).wait_send()
        line_cross_copy().wait_send()
        line_final_copy().wait_send()
        arrive(own.at[pl.ds(0, WHOLE)], own_send)
        arrive(own.at[pl.ds(0, rest)], aside_send)
        arrive(own.at[pl.ds(0, WHOLE)], pass_send)
        arrive(own.at[pl.ds(0, TURNED + steps - SPLIT)], far_send)
        arrive(own.at[pl.ds(0, TURNED + steps - SPLIT)], cross_send)
        arrive(cross_out.at[pl.ds(0, SPLIT - TURNED)], joined_send)
        arrive(own, final_send)

    @pl.when(outer)
    def _():
        choose_one(0, 0, label, 0, me)
        choose_one(0, 1, label_in.at[1], 0, me)
        arrive(final_in.at[pl.ds(0, TURNED)], final_recv.at[0])
        arrive(final_far.at[pl.ds(0, TURNED)], far_recv.at[0])
        lax.fori_loop(0, TURNED, land_turned, 0)
        arrive(final_in.at[pl.ds(TURNED, SPLIT - TURNED)], final_recv.at[1])
        lax.fori_loop(TURNED, SPLIT, land_ready, 0)
        lax.fori_loop(SPLIT, JOINED, land_joined, 0)
        lax.fori_loop(JOINED, steps, land, 0)
        arrive(label_in.at[pl.ds(0, 3)], label_send.at[0])
        arrive(line_in, line_send.at[0])
        line_final_copy().wait_recv()
        moved_out[...] = line_final[...]
        arrive(own, own_send)
        arrive(own.at[pl.ds(0, rest)], aside_send)
        arrive(own.at[pl.ds(0, rest)], pass_send)
        arrive(own.at[pl.ds(0, TURNED)], far_send)


def store_kernel(cache, out, cache_hbm, out_hbm, sems):
    copies = [pltpu.make_async_copy(out, out_hbm, sems.at[0])] + [
        pltpu.make_async_copy(cache.at[a], cache_hbm.at[a], sems.at[1 + a]) for a in range(2)
    ]
    for copy in copies:
        copy.start()
    for copy in copies:
        copy.wait()


def body(
    hidden,
    token_qkv,
    self_cache,
    cross_kv,
    cache_len,
    finished,
    new_slot,
    out_proj,
    ln_gain,
    ln_bias,
    query_proj,
):
    count, cores = lax.axis_size("batch"), lax.axis_size("mp")
    spans, width = hidden.shape
    slots, local = self_cache.shape[2:]
    moves = len(DISTANCES)
    smem = pl.BlockSpec(memory_space=pltpu.SMEM)
    vmem = pl.BlockSpec(memory_space=pltpu.VMEM)
    away = pl.BlockSpec(memory_space=pl.ANY)
    bf16, f32 = jnp.bfloat16, jnp.float32
    operands = (
        cache_len,
        finished,
        new_slot,
        hidden,
        token_qkv,
        self_cache,
        ln_gain,
        ln_bias,
        cross_kv,
        out_proj,
        query_proj,
    )
    parcels = pltpu.VMEM((moves, 2, slots, local), bf16)
    tiles = pltpu.VMEM((moves, 16, local), bf16)
    dma = pltpu.SemaphoreType.DMA
    inputs = [pltpu.VMEM(array.shape, bf16) for array in (cross_kv, out_proj, query_proj)]
    parts = [pltpu.VMEM((8, width), f32), pltpu.VMEM((cores - 1, 8, width), f32)]
    steps = 2 * slots // ROWS
    if count == 2 * (REACH + 1) and cores == 2:
        function, specs = relay_kernel, [away] * 8

        def blocks(*lead):
            return pltpu.VMEM(lead + (ROWS, local), bf16)

        small = [pltpu.SMEM((spans,), jnp.int32)] * 3 + [
            pltpu.VMEM(hidden.shape, bf16),
            pltpu.VMEM(token_qkv.shape, bf16),
            pltpu.VMEM(ln_gain.shape, f32),
            pltpu.VMEM(ln_bias.shape, f32),
        ]
        scratch = small + [pltpu.VMEM(self_cache.shape, bf16)] + inputs + [
            blocks(steps, spans),
            blocks(3, steps, spans),
            blocks(steps, 2 * spans),
            blocks(steps, 2 * spans),
            blocks(steps, spans),
            blocks(steps, spans),
            blocks(steps, spans),
            blocks(steps, spans),
            blocks(2, 4 * spans, 4 * spans),
            pltpu.VMEM((8, 128), f32),
            pltpu.VMEM((5, 8, 128), f32),
            pltpu.VMEM((spans, local), bf16),
            pltpu.VMEM((3, spans, local), bf16),
            pltpu.VMEM((2 * spans, local), f32),
            pltpu.VMEM((2 * spans, local), bf16),
            pltpu.VMEM((2 * spans, local), bf16),
            pltpu.VMEM((spans, local), bf16),
            pltpu.VMEM((spans, local), bf16),
            *parts,
            dma((12,)),
            dma((7,)),
            dma((steps,)),
            dma((steps,)),
            dma((1,)),
            dma((steps - TURNED + 1,)),
            dma((steps - SPLIT + 2,)),
            dma((steps - JOINED + 1,)),
            dma((JOINED - SPLIT,)),
            dma((1,)),
            dma((5,)),
            dma((1,)),
            dma((3,)),
            dma((4,)),
            dma((2, cores - 1)),
            pltpu.SemaphoreType.REGULAR,
        ]
    else:
        function, specs = kernel, [smem] * 3 + [vmem] * 5
        scratch = inputs + [
            pltpu.VMEM(self_cache.shape, bf16),
            parcels,
            parcels,
            tiles,
            tiles,
            tiles,
            tiles,
            *parts,
            dma((3,)),
            dma((2, moves)),
            dma((2, moves)),
            dma((2, moves)),
            dma((2, cores - 1)),
        ]
    moved = pl.pallas_call(
        functools.partial(function, count, cores),
        out_shape=(
            pltpu.VMEM(self_cache.shape, bf16),
            pltpu.VMEM((spans, local), bf16),
        ),
        in_specs=specs + [away] * 3,
        out_specs=(vmem, vmem),
        scratch_shapes=scratch,
        compiler_params=pltpu.CompilerParams(collective_id=0, has_side_effects=True),
    )(*operands)
    return pl.pallas_call(
        store_kernel,
        out_shape=tuple(jax.ShapeDtypeStruct(array.shape, bf16) for array in moved),
        in_specs=[vmem, vmem],
        out_specs=(away, away),
        scratch_shapes=[dma((3,))],
    )(*(pltpu.with_memory_space_constraint(a, pltpu.VMEM) for a in moved))


def solution(mesh):
    placed = (
        P(("groups", "batch"), None),
        P(None, ("groups", "batch"), "mp"),
        P(None, ("groups", "batch"), None, "mp"),
        P(None, ("groups", "batch"), None, "mp"),
        P(("groups", "batch")),
        P(("groups", "batch")),
        P(("groups", "batch")),
        P("mp", None),
        P(),
        P(),
        P(None, "mp"),
    )
    return jax.shard_map(
        body,
        mesh=mesh,
        in_specs=placed,
        out_specs=(P(None, ("groups", "batch"), None, "mp"), P(("groups", "batch"), "mp")),
        check_vma=False,
    )
```

```python
import functools

import jax
import jax.numpy as jnp
from jax import lax
from jax.experimental import pallas as pl
from jax.experimental.pallas import tpu as pltpu
from jax.sharding import PartitionSpec as P

HEAD_DIM = 64
REACH = 3
MESH = pl.DeviceIdType.MESH
DISTANCES = [3, -3, 2, -2, 1, -1]
ROWS = 16
WHOLE = 7
SPLIT = 10
JOINED = 14
AHEAD = 5
LAG = 3
BEHIND = 3
TURNED = 5
WAIT = 4
DEFER = 1
DEFER_ONE = 6
LINES = 10


def attend(query, keys, values, length, own):
    slots, width = keys.shape
    heads = width // HEAD_DIM
    rows = -(-heads // 16) * 16
    row = lax.broadcasted_iota(jnp.int32, (rows, width), 0)
    column = lax.broadcasted_iota(jnp.int32, (rows, width), 1)
    low = row * HEAD_DIM
    mine = (column >= low) & (column < low + HEAD_DIM)
    spread = jnp.where(mine, query.astype(jnp.float32), 0.0)
    factor = HEAD_DIM ** (-0.5)
    scores = (
        lax.dot_general(
            spread.astype(jnp.bfloat16),
            keys,
            (((1,), (1,)), ((), ())),
            preferred_element_type=jnp.float32,
        )
        * factor
    )
    if length is not None:
        usable = lax.broadcasted_iota(jnp.int32, (rows, slots), 1) < length
        scores = jnp.where(usable, scores, -1e30)
    highest = jnp.max(scores, axis=-1, keepdims=True)
    if own is not None:
        new_key, new_value = own
        own_score = jnp.sum(spread * new_key.astype(jnp.float32), axis=-1, keepdims=True) * factor
        highest = jnp.maximum(highest, own_score)
    weight = jnp.exp(scores - highest)
    if length is not None:
        weight = jnp.where(usable, weight, 0.0)
    total = jnp.sum(weight, axis=-1, keepdims=True)
    if own is not None:
        own_weight = jnp.exp(own_score - highest)
        total = total + own_weight
    weight = (weight / total).astype(jnp.bfloat16)
    mixed = jnp.dot(weight, values, preferred_element_type=jnp.float32)
    if own is not None:
        own_weight = (own_weight / total).astype(jnp.bfloat16).astype(jnp.float32)
        mixed = mixed + own_weight * new_value.astype(jnp.float32)
    return jnp.sum(jnp.where(mine, mixed, 0.0), axis=0, keepdims=True)


def kernel(
    count,
    cores,
    cache_len,
    finished,
    new_slot,
    hidden,
    token_qkv,
    self_cache,
    ln_gain,
    ln_bias,
    cross_hbm,
    out_proj_hbm,
    query_proj_hbm,
    moved_cache,
    moved_out,
    cross,
    out_proj,
    query_proj,
    updated,
    parcel,
    arrived,
    mark,
    mark_in,
    line,
    line_in,
    part,
    part_in,
    load_sem,
    cache_sems,
    mark_sems,
    line_sems,
    part_sems,
):
    spans, width = hidden.shape
    slots, local = self_cache.shape[2:]
    me = lax.axis_index("batch")
    core = lax.axis_index("mp")
    loads = [
        pltpu.make_async_copy(source, target, load_sem.at[i])
        for i, (source, target) in enumerate(
            [(out_proj_hbm, out_proj), (query_proj_hbm, query_proj), (cross_hbm, cross)]
        )
    ]
    for load in loads:
        load.start()

    barrier = pltpu.get_barrier_semaphore()
    targets = [lax.rem(me + distance + count, count) for distance in DISTANCES]
    for target in targets:
        pl.semaphore_signal(barrier, inc=1, device_id={"batch": target}, device_id_type=MESH)
    others = [lax.rem(core + k, cores) for k in range(1, cores)]
    for other in others:
        pl.semaphore_signal(barrier, inc=1, device_id={"mp": other}, device_id_type=MESH)

    half = count // 2
    alive, offset, place = [], [], []
    for c in range(spans):
        slot = new_slot[c]
        owner = lax.div(slot, spans)
        offset.append(lax.rem(owner - me + half + count, count) - half)
        place.append(lax.rem(slot, spans))
        alive.append(jnp.where(finished[c] == 0, 1, 0))

    position = lax.broadcasted_iota(jnp.int32, (slots, local), 0)
    for c in range(spans):
        length = cache_len[c]
        older = jnp.where(position < length * alive[c], 1.0, 0.0).astype(jnp.bfloat16)
        fresh = jnp.where(position == jnp.where(alive[c] == 1, length, -1), 1.0, 0.0).astype(
            jnp.bfloat16
        )
        for a in range(2):
            updated[a, c] = self_cache[a, c] * older + token_qkv[1 + a, c : c + 1, :] * fresh

    def flag(value, shape):
        return jnp.full(shape, jnp.where(value, 1.0, 0.0), jnp.float32).astype(jnp.bfloat16)

    marker_row = lax.broadcasted_iota(jnp.int32, mark.shape[1:], 0)
    for i, distance in enumerate(DISTANCES):
        marker = jnp.zeros(mark.shape[1:], jnp.float32)
        for c in range(spans):
            at = jnp.where(offset[c] == distance, place[c], -1)
            marker = jnp.where(marker_row == at, 1.0, marker)
        mark[i] = marker.astype(jnp.bfloat16)

    def send(source, target, sems, i, distance):
        return pltpu.make_async_remote_copy(
            src_ref=source,
            dst_ref=target,
            send_sem=sems.at[0, i],
            recv_sem=sems.at[1, i],
            device_id={"batch": targets[i]},
            device_id_type=MESH,
        )

    pl.semaphore_wait(barrier, len(targets) + len(others))
    mark_copies, cache_copies = [], []
    for i, distance in enumerate(DISTANCES):
        copy = send(mark.at[i], mark_in.at[i], mark_sems, i, distance)
        copy.start()
        mark_copies.append(copy)
    for i, distance in enumerate(DISTANCES):
        for a in range(2):
            total = updated[a, 0] * flag(offset[0] == distance, (1, local))
            for c in range(1, spans):
                total = total + updated[a, c] * flag(offset[c] == distance, (1, local))
            parcel[i, a] = total
        copy = send(parcel.at[i], arrived.at[i], cache_sems, i, distance)
        copy.start()
        cache_copies.append(copy)

    for l in range(spans):
        for a in range(2):
            total = updated[a, 0] * flag((offset[0] == 0) & (place[0] == l), (1, local))
            for c in range(1, spans):
                keep = flag((offset[c] == 0) & (place[c] == l), (1, local))
                total = total + updated[a, c] * keep
            moved_cache[a, l] = total

    contexts = []
    for c in range(spans):
        query, key, value = (token_qkv[k, c : c + 1, :] for k in range(3))
        contexts.append(
            attend(query, self_cache[0, c], self_cache[1, c], cache_len[c], (key, value))
        )
    pad = part.shape[0] - spans
    context = jnp.concatenate(contexts + [jnp.zeros((pad, local), jnp.float32)], 0)
    context = context.astype(jnp.bfloat16)
    loads[0].wait()
    part[...] = jnp.dot(context, out_proj[...], preferred_element_type=jnp.float32)
    part_copies = []
    for k, other in enumerate(others):
        copy = pltpu.make_async_remote_copy(
            src_ref=part,
            dst_ref=part_in.at[k],
            send_sem=part_sems.at[0, k],
            recv_sem=part_sems.at[1, k],
            device_id={"mp": other},
            device_id_type=MESH,
        )
        copy.start()
        part_copies.append(copy)
    loads[1].wait()
    loads[2].wait()
    for copy in part_copies:
        copy.wait()
    summed = part[...]
    for k in range(len(others)):
        summed = summed + part_in[k]
    resid = hidden[...].astype(jnp.float32) + summed[:spans]
    centre = jnp.mean(resid, axis=-1, keepdims=True)
    spread = jnp.mean((resid - centre) ** 2, axis=-1, keepdims=True)
    gain = ln_gain[...].reshape(1, width)
    bias = ln_bias[...].reshape(1, width)
    normed = (resid - centre) * lax.rsqrt(spread + 1e-05) * gain + bias
    normed = jnp.concatenate([normed, jnp.zeros((pad, width), jnp.float32)], 0)
    query = jnp.dot(
        normed.astype(jnp.bfloat16), query_proj[...], preferred_element_type=jnp.float32
    ).astype(jnp.bfloat16).astype(jnp.float32)
    decoded = []
    for c in range(spans):
        mixed = attend(query[c : c + 1], cross[0, c], cross[1, c], None, None)
        decoded.append(mixed * jnp.where(alive[c] == 1, 1.0, 0.0))

    line_copies = []
    blank = jnp.zeros((line.shape[1] - 1, local), jnp.float32)
    for i, distance in enumerate(DISTANCES):
        row = jnp.zeros((1, local), jnp.float32)
        for c in range(spans):
            row = row + decoded[c] * jnp.where(offset[c] == distance, 1.0, 0.0)
        line[i] = jnp.concatenate([row, blank], 0).astype(jnp.bfloat16)
        copy = send(line.at[i], line_in.at[i], line_sems, i, distance)
        copy.start()
        line_copies.append(copy)

    rows = []
    for l in range(spans):
        row = jnp.zeros((1, local), jnp.float32)
        for c in range(spans):
            keep = (offset[c] == 0) & (place[c] == l)
            row = row + decoded[c] * jnp.where(keep, 1.0, 0.0)
        rows.append(row)
    for i in range(len(DISTANCES)):
        mark_copies[i].wait()
        cache_copies[i].wait()
        for l in range(spans):
            taken = mark_in[i, l : l + 1, :]
            for a in range(2):
                moved_cache[a, l] = moved_cache[a, l] + arrived[i, a] * taken
    for i in range(len(DISTANCES)):
        line_copies[i].wait()
        for l in range(spans):
            taken = mark_in[i, l : l + 1, :].astype(jnp.float32)
            rows[l] = rows[l] + line_in[i, 0:1, :].astype(jnp.float32) * taken
    moved_out[...] = jnp.concatenate(rows, 0).astype(jnp.bfloat16)


def relay_kernel(
    count,
    cores,
    cache_len_hbm,
    finished_hbm,
    new_slot_hbm,
    hidden_hbm,
    token_qkv_hbm,
    cache_hbm,
    ln_gain_hbm,
    ln_bias_hbm,
    cross_hbm,
    out_proj_hbm,
    query_proj_hbm,
    moved_cache,
    moved_out,
    cache_len,
    finished,
    new_slot,
    hidden,
    token_qkv,
    ln_gain,
    ln_bias,
    self_cache,
    cross,
    out_proj,
    query_proj,
    own,
    raw_in,
    cross_out,
    cross_in,
    kept,
    final_out,
    final_in,
    final_far,
    pick,
    label,
    label_in,
    line,
    line_in,
    line_kept,
    line_out,
    line_cross,
    line_last,
    line_final,
    part,
    part_in,
    load_sem,
    send_sems,
    mate_recv,
    second_recv,
    whole_recv,
    cross_recv,
    final_recv,
    far_recv,
    half_recv,
    label_send,
    label_recv,
    line_send,
    line_recv,
    line_hops,
    part_sems,
    core_sem,
):
    spans, width = hidden.shape
    slots, local = self_cache.shape[2:]
    steps, _, rows_per, _ = own.shape
    per = steps // 2
    me = lax.axis_index("batch")
    core = lax.axis_index("mp")
    level, column = lax.div(me, 2), lax.rem(me, 2)
    inner = (level == 1) | (level == REACH - 1)
    outer = jnp.logical_not(inner)
    barrier = pltpu.get_barrier_semaphore()

    def greet(where):
        pl.semaphore_signal(barrier, inc=1, device_id=where, device_id_type=MESH)

    mate_level = jnp.where(level == 0, 1, jnp.where(level == 1, 0, jnp.where(level == 2, 3, 2)))
    mate = mate_level * 2 + column
    mate_aside = mate_level * 2 + 1 - column
    aside = level * 2 + 1 - column
    across = (REACH - level) * 2 + column
    beyond = (REACH - mate_level) * 2 + column
    others = [lax.rem(core + k, cores) for k in range(1, cores)]
    for node in (mate, aside):
        greet({"batch": node})

    @pl.when(inner)
    def _():
        greet({"batch": across})

    @pl.when(core == 0)
    def _():
        greet({"mp": 1})

    loads = [
        pltpu.make_async_copy(source, target, load_sem.at[i])
        for i, (source, target) in enumerate(
            [
                (out_proj_hbm, out_proj),
                (query_proj_hbm, query_proj),
                (cross_hbm, cross),
                (cache_hbm.at[0], self_cache.at[0]),
                (cache_hbm.at[1], self_cache.at[1]),
                (cache_len_hbm, cache_len),
                (finished_hbm, finished),
                (new_slot_hbm, new_slot),
                (hidden_hbm, hidden),
                (token_qkv_hbm, token_qkv),
                (ln_gain_hbm, ln_gain),
                (ln_bias_hbm, ln_bias),
            ]
        )
    ]
    for i in [3, *range(5, len(loads)), 4, 0, 1, 2]:
        loads[i].start()
    for load in loads[5:]:
        load.wait()

    alive = [jnp.where(finished[c] == 0, 1, 0) for c in range(spans)]

    def to(node, source, target, sent, received):
        return pltpu.make_async_remote_copy(
            src_ref=source,
            dst_ref=target,
            send_sem=sent,
            recv_sem=received,
            device_id={"batch": node},
            device_id_type=MESH,
        )

    own_send, aside_send, pass_send, far_send, cross_send, joined_send, final_send = (
        send_sems.at[i] for i in range(7)
    )

    def mate_copy(k):
        return to(mate, own.at[k], raw_in.at[0, k], own_send, mate_recv.at[k])

    def across_copy(k):
        return to(across, own.at[k], raw_in.at[1, k], own_send, whole_recv.at[0])

    def aside_copy(k):
        return to(aside, own.at[k], raw_in.at[2, k], aside_send, second_recv.at[k])

    def pass_copy(k):
        return to(across, raw_in.at[0, k], raw_in.at[2, k], pass_send, second_recv.at[k])

    def outer_pass_copy(k):
        return to(mate, raw_in.at[2, k], raw_in.at[1, k], pass_send, mate_recv.at[k])

    def arrive(blocks, sem):
        pltpu.make_async_copy(blocks, blocks, sem).wait()

    def far_copy(k):
        return to(
            beyond,
            cross_out.at[k, pl.ds(spans, spans)],
            final_far.at[k],
            far_send,
            far_recv.at[k - JOINED + 1],
        )

    def half_copy(k):
        return to(
            across,
            cross_out.at[k, pl.ds(spans, spans)],
            cross_in.at[k, pl.ds(spans, spans)],
            far_send,
            half_recv.at[k - SPLIT],
        )

    def turn_copy(k):
        return to(
            mate,
            cross_out.at[k, pl.ds(spans, spans)],
            raw_in.at[2, k],
            far_send,
            second_recv.at[k],
        )

    def turned_copy(k):
        return to(aside, raw_in.at[2, k], final_far.at[k], far_send, far_recv.at[0])

    def cross_copy(k, node, count, sent, slot=None):
        return to(
            node,
            cross_out.at[k, pl.ds(0, count)],
            cross_in.at[k, pl.ds(0, count)],
            sent,
            cross_recv.at[k - TURNED + 1 if slot is None else slot],
        )

    def final_copy(k, slot):
        return to(mate, final_out.at[k], final_in.at[k], final_send, final_recv.at[slot])

    def last_copy(k):
        return final_copy(k, k - SPLIT + 2)

    def label_copy(node, lane, way):
        return to(node, label, label_in.at[way], label_send.at[0], label_recv.at[way])

    def line_copy(node, lane, way):
        return to(node, line, line_in.at[way], line_send.at[0], line_recv.at[way])

    def label_pass_copy(node, here, there):
        return to(node, label_in.at[here], label_in.at[there], label_send.at[0], label_recv.at[there])

    def line_pass_copy():
        return to(mate, line_in.at[1], line_in.at[1], line_send.at[0], line_recv.at[1])

    def line_cross_copy():
        return to(across, line_out, line_cross, line_hops.at[0], line_hops.at[1])

    def line_final_copy():
        return to(mate, line_last, line_final, line_hops.at[2], line_hops.at[3])

    label_row = lax.broadcasted_iota(jnp.int32, label.shape, 0)
    labels = jnp.zeros(label.shape, jnp.int32)
    for c in range(spans):
        labels = jnp.where(label_row == c, new_slot[c], labels)
    label[...] = labels.astype(jnp.float32)

    @pl.when(inner)
    def _():
        pl.semaphore_wait(barrier, 3 + core)

    @pl.when(outer)
    def _():
        pl.semaphore_wait(barrier, 2 + core)

    @pl.when(core == 1)
    def _():
        pl.semaphore_signal(core_sem, inc=1, device_id={"mp": 0}, device_id_type=MESH)

    position = lax.broadcasted_iota(jnp.int32, (rows_per, local), 0)
    ends = [cache_len[c] * alive[c] for c in range(spans)]
    fresh_at = [jnp.where(alive[c] == 1, cache_len[c], -1) for c in range(spans)]

    def grow(k, _):
        a, r = lax.div(k, per), lax.rem(k, per)
        start = pl.multiple_of(r * rows_per, rows_per)
        at = position + start
        for c in range(spans):
            older = jnp.where(at < ends[c], 1.0, 0.0).astype(jnp.bfloat16)
            fresh = jnp.where(at == fresh_at[c], 1.0, 0.0).astype(jnp.bfloat16)
            new = jnp.where(a == 0, token_qkv[1, c : c + 1, :].astype(jnp.float32),
                            token_qkv[2, c : c + 1, :].astype(jnp.float32)).astype(jnp.bfloat16)
            own[k, c] = self_cache[a, c, pl.ds(start, rows_per), :] * older + new * fresh

        return 0

    def pass_whole(k, _):
        grow(k, 0)

        @pl.when(outer)
        def _():
            mate_copy(k).start()

        @pl.when(inner)
        def _():
            across_copy(k).start()

        return 0

    def pass_on(k, _):
        aside_copy(k).start()
        return 0

    @pl.when(outer)
    def _():
        label_copy(mate, 0, 0).start()
        label_copy(aside, 1, 1).start()

    @pl.when(inner)
    def _():
        label_copy(aside, 0, 2).start()
        label_copy(across, 1, 3).start()

    loads[3].wait()
    lax.fori_loop(0, WHOLE, pass_whole, 0)
    lax.fori_loop(WHOLE, per, grow, 0)
    loads[4].wait()
    lax.fori_loop(per, steps, grow, 0)

    @pl.when(inner)
    def _():
        lax.fori_loop(JOINED, steps, pass_on, 0)
        lax.fori_loop(WHOLE, WHOLE + AHEAD, pass_on, 0)

    @pl.when(outer)
    def _():
        lax.fori_loop(WHOLE, steps, pass_on, 0)


    def self_part():
        contexts = []
        for c in range(spans):
            query, key, value = (token_qkv[k, c : c + 1, :] for k in range(3))
            contexts.append(
                attend(query, self_cache[0, c], self_cache[1, c], cache_len[c], (key, value))
            )
        context = jnp.concatenate(contexts + [jnp.zeros((pad, local), jnp.float32)], 0)
        context = context.astype(jnp.bfloat16)
        loads[0].wait()
        part[...] = jnp.dot(context, out_proj[...], preferred_element_type=jnp.float32)

    def part_copy(k):
        return pltpu.make_async_remote_copy(
            src_ref=part,
            dst_ref=part_in.at[k],
            send_sem=part_sems.at[0, k],
            recv_sem=part_sems.at[1, k],
            device_id={"mp": others[k]},
            device_id_type=MESH,
        )

    pad = part.shape[0] - spans
    self_part()

    @pl.when(core == 0)
    def _():
        pl.semaphore_wait(core_sem, 1)

    for k in range(len(others)):
        part_copy(k).start()

    @pl.when(outer)
    def _():
        label_copy(mate, 0, 1).wait_recv()
        label_pass_copy(mate, 1, 1).start()

    @pl.when(inner)
    def _():
        label_copy(mate, 0, 0).wait_recv()
        label_pass_copy(across, 0, 4).start()

    def choose(p, ways, nodes):
        for s, source in enumerate([label] + [label_in.at[way] for way in ways]):
            for d, node in enumerate(nodes):
                choose_one(p, s, source, d, node)

    def choose_one(p, s, source, d, node):
        for c in range(spans):
            held = jnp.broadcast_to(source[c : c + 1, 0:1], (rows_per, local))
            for l in range(spans):
                wanted = jnp.full((rows_per, local), node * spans + l, jnp.int32)
                pick[p, s * spans + c, d * spans + l] = jnp.where(
                    held == wanted.astype(jnp.float32), 1.0, 0.0
                ).astype(jnp.bfloat16)

    def level(k, s, d):
        total = own[k, 0] * pick[0, 0, d]
        for c in range(1, spans):
            total = total + own[k, c] * pick[0, c, d]
        for c in range(spans):
            total = total + raw_in[2, k, c] * pick[0, s * spans + c, d]
        return total

    def hand_early(k, _):
        aside_copy(k).wait_recv()
        for l in range(spans):
            final_out[k, l] = level(k, 3, spans + l)
        last_copy(k).start()
        return 0

    def gather(k, p, cross_done, final_done):
        blocks = [own[k, c] for c in range(spans)]
        for way in range(3):
            blocks += [raw_in[way, k, c] for c in range(spans)]

        def gathered(d):
            total = blocks[0] * pick[p, 0, d]
            for s in range(1, len(blocks)):
                total = total + blocks[s] * pick[p, s, d]
            return total

        for d in range(spans, 2 * spans):
            cross_out[k, d] = gathered(2 * spans + d)
        for d in range(spans):
            cross_out[k, d] = gathered(2 * spans + d)
        cross_done()
        if final_done is not None:
            for d in range(spans):
                final_out[k, d] = gathered(spans + d)
            final_done()
        for d in range(spans):
            kept[k, d] = gathered(d)

    def gathered_in(k):
        arrive(raw_in.at[pl.ds(0, 2), k], mate_recv.at[k])
        aside_copy(k).wait_recv()

    def merge_whole(k, _):
        pass_copy(k).wait_recv()

        def cross_done():
            turn_copy(k).start()
            cross_copy(k, aside, spans, cross_send, 0).start()

        gather(k, 1, cross_done, lambda: final_copy(k, 0).start())
        return 0

    def merge_whole_joined(k, _):
        pass_copy(k).wait_recv()
        gather(k, 1, lambda: cross_copy(k, aside, 2 * spans, joined_send).start(), lambda: None)
        return 0

    def whole(k):
        return (merge_whole if k < TURNED else merge_whole_joined, k)

    def merge_joined(k, _):
        gathered_in(k)
        gather(k, 0, lambda: cross_copy(k, across, 2 * spans, joined_send).start(), lambda: None)
        return 0

    def merge_half(k, _):
        gathered_in(k)
        gather(k, 0, lambda: half_copy(k).start(), lambda: None)
        return 0

    def merge(k, _):
        arrive(raw_in.at[pl.ds(0, 2), k], mate_recv.at[k])
        gather(k, 0, lambda: far_copy(k).start(), None)
        return 0

    def send_rest(k, _):
        cross_copy(k, across, spans, cross_send).start()
        return 0

    def settle(k):
        a, r = lax.div(k, per), lax.rem(k, per)
        start = pl.multiple_of(r * rows_per, rows_per)
        for l in range(spans):
            moved_cache[a, l, pl.ds(start, rows_per), :] = kept[k, l] + cross_in[k, l]

    def finish(k, _):
        cross_copy(k, across, spans, cross_send).wait_recv()
        settle(k)
        return 0

    def hand_on(k, copy):
        for l in range(spans):
            final_out[k, l] = final_out[k, l] + cross_in[k, spans + l]
        copy.start()

    def finish_joined(k, _):
        cross_copy(k, across, 2 * spans, joined_send).wait_recv()
        hand_on(k, final_copy(k, 1))
        settle(k)
        return 0

    def finish_half(k, _):
        half_copy(k).wait_recv()
        hand_on(k, last_copy(k))
        return 0

    loads[1].wait()
    loads[2].wait()
    for k in range(len(others)):
        part_copy(k).wait()
    summed = part[...]
    for k in range(len(others)):
        summed = summed + part_in[k]
    resid = hidden[...].astype(jnp.float32) + summed[:spans]
    centre = jnp.mean(resid, axis=-1, keepdims=True)
    spread = jnp.mean((resid - centre) ** 2, axis=-1, keepdims=True)
    gain = ln_gain[...].reshape(1, width)
    bias = ln_bias[...].reshape(1, width)
    normed = (resid - centre) * lax.rsqrt(spread + 1e-05) * gain + bias
    normed = jnp.concatenate([normed, jnp.zeros((pad, width), jnp.float32)], 0)
    query = jnp.dot(
        normed.astype(jnp.bfloat16), query_proj[...], preferred_element_type=jnp.float32
    ).astype(jnp.bfloat16).astype(jnp.float32)

    decoded = []
    for c in range(spans):
        mixed = attend(query[c : c + 1], cross[0, c], cross[1, c], None, None)
        decoded.append(mixed * jnp.where(alive[c] == 1, 1.0, 0.0))

    line[...] = jnp.concatenate(decoded, 0).astype(jnp.bfloat16)

    @pl.when(outer)
    def _():
        line_copy(mate, 0, 0).start()
        line_copy(aside, 1, 1).start()

    @pl.when(inner)
    def _():
        line_copy(aside, 0, 2).start()

    def turn(k, _):
        turn_copy(k).wait_recv()
        turned_copy(k).start()
        return 0

    def outer_forward(k, _):
        mate_copy(k).start()
        aside_copy(k).wait_recv()
        outer_pass_copy(k).start()
        return 0

    @pl.when(outer)
    def _():
        lax.fori_loop(WHOLE, WHOLE + AHEAD, outer_forward, 0)
        line_copy(mate, 0, 1).wait_recv()
        line_pass_copy().start()
        lax.fori_loop(WHOLE + AHEAD, steps, outer_forward, 0)
        lax.fori_loop(0, TURNED, turn, 0)

    @pl.when(inner)
    def _():
        lax.fori_loop(WHOLE + AHEAD, JOINED, pass_on, 0)

    def forward(k, _):
        mate_copy(k).wait_recv()
        pass_copy(k).start()
        return 0

    def gather_lines():
        for way in range(3):
            line_copy(mate, 0, way).wait_recv()
        blocks = []
        for held in [line] + [line_in.at[way] for way in range(3)]:
            blocks += [held[c : c + 1, :].astype(jnp.float32) for c in range(spans)]
        rows = []
        for d in range(4 * spans):
            total = blocks[0] * pick[0, 0, d, 0:1, :].astype(jnp.float32)
            for s in range(1, len(blocks)):
                total = total + blocks[s] * pick[0, s, d, 0:1, :].astype(jnp.float32)
            rows.append(total)
        line_out[...] = jnp.concatenate(rows[2 * spans :], 0).astype(jnp.bfloat16)
        line_cross_copy().start()
        line_kept[...] = jnp.concatenate(rows[: 2 * spans], 0)

    def send_lines():
        line_cross_copy().wait_recv()
        total = line_kept[...] + line_cross[...].astype(jnp.float32)
        line_last[...] = total[spans:].astype(jnp.bfloat16)
        line_final_copy().start()
        moved_out[...] = total[:spans].astype(jnp.bfloat16)

    def run(groups):
        while groups:
            ops, starts = [op for op, _ in groups[0]], [k for _, k in groups[0]]
            size = 1
            while size < len(groups) and groups[size] == [(op, k + size) for op, k in groups[0]]:
                size += 1

            def step(i, _, ops=ops, starts=starts):
                for op, k in zip(ops, starts):
                    op(i + k, 0)
                return 0

            if size > 1:
                lax.fori_loop(0, size, step, 0)
            else:
                step(0, 0)
            groups = groups[size:]

    def groups(low, high, defer):
        found = []
        for k in range(low, high):
            group = []
            if k < steps:
                group.append(
                    (merge_joined if k < SPLIT else merge_half if k < JOINED else merge, k)
                )
            if SPLIT <= k - defer < steps and k < steps:
                group.append((send_rest, k - defer))
            if k == steps - 1:
                group += [(send_rest, j) for j in range(steps - defer, steps)]
            if WHOLE <= k - LAG < JOINED:
                group.append((finish_joined if k - LAG < SPLIT else finish_half, k - LAG))
            if k < WHOLE + BEHIND:
                group.append(whole(k - BEHIND))
            if TURNED <= k - WHOLE - WAIT + TURNED < WHOLE:
                group.append((finish_joined, k - WHOLE - WAIT + TURNED))
            found.append(group)
        return found

    @pl.when(inner)
    def _():
        label_copy(mate, 0, 2).wait_recv()
        choose_one(0, 0, label, 1, mate)
        choose_one(0, 3, label_in.at[2], 1, mate)
        lax.fori_loop(JOINED, steps, hand_early, 0)
        lax.fori_loop(0, WHOLE, forward, 0)
        for way in (1, 3, 4):
            label_copy(mate, 0, way).wait_recv()
        choose(1, (0, 3, 4), (me, mate, aside, mate_aside))
        choose(0, (0, 1, 2), (me, mate, across, beyond))
        arrive(raw_in.at[1, pl.ds(0, WHOLE)], whole_recv.at[0])
        run([[whole(k)] for k in range(WHOLE - BEHIND)])
        run(groups(WHOLE, LINES, DEFER))
        gather_lines()

        @pl.when(core == 0)
        def _():
            run(groups(LINES, steps + LAG, DEFER))

        @pl.when(core != 0)
        def _():
            run(groups(LINES, steps + LAG, DEFER_ONE))

        send_lines()

    def place(k, value):
        a, r = lax.div(k, per), lax.rem(k, per)
        start = pl.multiple_of(r * rows_per, rows_per)
        for l in range(spans):
            moved_cache[a, l, pl.ds(start, rows_per), :] = value(l)

    def land_turned(k, _):
        place(k, lambda l: final_in[k, l] + final_far[k, l])
        return 0

    def land_ready(k, _):
        place(k, lambda l: final_in[k, l])
        return 0

    def land_joined(k, _):
        last_copy(k).wait_recv()
        return land_ready(k, 0)

    def land(k, _):
        last_copy(k).wait_recv()
        far_copy(k).wait_recv()
        place(k, lambda l: final_in[k, l] + final_far[k, l] + level(k, 1, l))
        return 0

    def settle_turned(k, _):
        settle(k)
        return 0

    rest = steps - WHOLE

    @pl.when(inner)
    def _():
        arrive(kept.at[pl.ds(0, TURNED)], cross_recv.at[0])
        lax.fori_loop(0, TURNED, settle_turned, 0)
        lax.fori_loop(SPLIT, steps, finish, 0)
        arrive(label_in.at[pl.ds(0, 3)], label_send.at[0])
        line_copy(aside, 0, 2).wait_send()
        line_cross_copy().wait_send()
        line_final_copy().wait_send()
        arrive(own.at[pl.ds(0, WHOLE)], own_send)
        arrive(own.at[pl.ds(0, rest)], aside_send)
        arrive(own.at[pl.ds(0, WHOLE)], pass_send)
        arrive(own.at[pl.ds(0, TURNED + steps - SPLIT)], far_send)
        arrive(own.at[pl.ds(0, TURNED + steps - SPLIT)], cross_send)
        arrive(cross_out.at[pl.ds(0, SPLIT - TURNED)], joined_send)
        arrive(own, final_send)

    @pl.when(outer)
    def _():
        choose_one(0, 0, label, 0, me)
        choose_one(0, 1, label_in.at[1], 0, me)
        arrive(final_in.at[pl.ds(0, TURNED)], final_recv.at[0])
        arrive(final_far.at[pl.ds(0, TURNED)], far_recv.at[0])
        lax.fori_loop(0, TURNED, land_turned, 0)
        arrive(final_in.at[pl.ds(TURNED, SPLIT - TURNED)], final_recv.at[1])
        lax.fori_loop(TURNED, SPLIT, land_ready, 0)
        lax.fori_loop(SPLIT, JOINED, land_joined, 0)
        lax.fori_loop(JOINED, steps, land, 0)
        arrive(label_in.at[pl.ds(0, 3)], label_send.at[0])
        arrive(line_in, line_send.at[0])
        line_final_copy().wait_recv()
        moved_out[...] = line_final[...]
        arrive(own, own_send)
        arrive(own.at[pl.ds(0, rest)], aside_send)
        arrive(own.at[pl.ds(0, rest)], pass_send)
        arrive(own.at[pl.ds(0, TURNED)], far_send)


def store_kernel(cache, out, cache_hbm, out_hbm, sems):
    copies = [pltpu.make_async_copy(out, out_hbm, sems.at[0])] + [
        pltpu.make_async_copy(cache.at[a], cache_hbm.at[a], sems.at[1 + a]) for a in range(2)
    ]
    for copy in copies:
        copy.start()
    for copy in copies:
        copy.wait()


def body(
    hidden,
    token_qkv,
    self_cache,
    cross_kv,
    cache_len,
    finished,
    new_slot,
    out_proj,
    ln_gain,
    ln_bias,
    query_proj,
):
    count, cores = lax.axis_size("batch"), lax.axis_size("mp")
    spans, width = hidden.shape
    slots, local = self_cache.shape[2:]
    moves = len(DISTANCES)
    smem = pl.BlockSpec(memory_space=pltpu.SMEM)
    vmem = pl.BlockSpec(memory_space=pltpu.VMEM)
    away = pl.BlockSpec(memory_space=pl.ANY)
    bf16, f32 = jnp.bfloat16, jnp.float32
    operands = (
        cache_len,
        finished,
        new_slot,
        hidden,
        token_qkv,
        self_cache,
        ln_gain,
        ln_bias,
        cross_kv,
        out_proj,
        query_proj,
    )
    parcels = pltpu.VMEM((moves, 2, slots, local), bf16)
    tiles = pltpu.VMEM((moves, 16, local), bf16)
    dma = pltpu.SemaphoreType.DMA
    inputs = [pltpu.VMEM(array.shape, bf16) for array in (cross_kv, out_proj, query_proj)]
    parts = [pltpu.VMEM((8, width), f32), pltpu.VMEM((cores - 1, 8, width), f32)]
    steps = 2 * slots // ROWS
    if count == 2 * (REACH + 1) and cores == 2:
        function, specs = relay_kernel, [away] * 8

        def blocks(*lead):
            return pltpu.VMEM(lead + (ROWS, local), bf16)

        small = [pltpu.SMEM((spans,), jnp.int32)] * 3 + [
            pltpu.VMEM(hidden.shape, bf16),
            pltpu.VMEM(token_qkv.shape, bf16),
            pltpu.VMEM(ln_gain.shape, f32),
            pltpu.VMEM(ln_bias.shape, f32),
        ]
        scratch = small + [pltpu.VMEM(self_cache.shape, bf16)] + inputs + [
            blocks(steps, spans),
            blocks(3, steps, spans),
            blocks(steps, 2 * spans),
            blocks(steps, 2 * spans),
            blocks(steps, spans),
            blocks(steps, spans),
            blocks(steps, spans),
            blocks(steps, spans),
            blocks(2, 4 * spans, 4 * spans),
            pltpu.VMEM((8, 128), f32),
            pltpu.VMEM((5, 8, 128), f32),
            pltpu.VMEM((spans, local), bf16),
            pltpu.VMEM((3, spans, local), bf16),
            pltpu.VMEM((2 * spans, local), f32),
            pltpu.VMEM((2 * spans, local), bf16),
            pltpu.VMEM((2 * spans, local), bf16),
            pltpu.VMEM((spans, local), bf16),
            pltpu.VMEM((spans, local), bf16),
            *parts,
            dma((12,)),
            dma((7,)),
            dma((steps,)),
            dma((steps,)),
            dma((1,)),
            dma((steps - TURNED + 1,)),
            dma((steps - SPLIT + 2,)),
            dma((steps - JOINED + 1,)),
            dma((JOINED - SPLIT,)),
            dma((1,)),
            dma((5,)),
            dma((1,)),
            dma((3,)),
            dma((4,)),
            dma((2, cores - 1)),
            pltpu.SemaphoreType.REGULAR,
        ]
    else:
        function, specs = kernel, [smem] * 3 + [vmem] * 5
        scratch = inputs + [
            pltpu.VMEM(self_cache.shape, bf16),
            parcels,
            parcels,
            tiles,
            tiles,
            tiles,
            tiles,
            *parts,
            dma((3,)),
            dma((2, moves)),
            dma((2, moves)),
            dma((2, moves)),
            dma((2, cores - 1)),
        ]
    moved = pl.pallas_call(
        functools.partial(function, count, cores),
        out_shape=(
            pltpu.VMEM(self_cache.shape, bf16),
            pltpu.VMEM((spans, local), bf16),
        ),
        in_specs=specs + [away] * 3,
        out_specs=(vmem, vmem),
        scratch_shapes=scratch,
        compiler_params=pltpu.CompilerParams(collective_id=0, has_side_effects=True),
    )(*operands)
    return pl.pallas_call(
        store_kernel,
        out_shape=tuple(jax.ShapeDtypeStruct(array.shape, bf16) for array in moved),
        in_specs=[vmem, vmem],
        out_specs=(away, away),
        scratch_shapes=[dma((3,))],
    )(*(pltpu.with_memory_space_constraint(a, pltpu.VMEM) for a in moved))


def solution(mesh):
    placed = (
        P(("groups", "batch"), None),
        P(None, ("groups", "batch"), "mp"),
        P(None, ("groups", "batch"), None, "mp"),
        P(None, ("groups", "batch"), None, "mp"),
        P(("groups", "batch")),
        P(("groups", "batch")),
        P(("groups", "batch")),
        P("mp", None),
        P(),
        P(),
        P(None, "mp"),
    )
    return jax.shard_map(
        body,
        mesh=mesh,
        in_specs=placed,
        out_specs=(P(None, ("groups", "batch"), None, "mp"), P(("groups", "batch"), "mp")),
        check_vma=False,
    )
```
